128 devices in a mesh: ctx: 32 (over y, z, x_hi), tp: 4 (over x_lo, core).
Axes of the slice: x: 4 (x_hi: 2, x_lo: 2; x = x_hi * 2 + x_lo), y: 4, z: 4, core: 2. Of those that a mesh axis runs over, the one named last changes fastest.
Arguments:
- tokens: bfloat16 [8192, 5376], P('ctx', 'tp'), as said below
- out_grad: bfloat16 [8192, 5376], P('ctx', 'tp'), may hold values from -6 to 6
- in_gain: float32 [5376], replicated, may hold values from 0.5 to 1.5
- query_gain: float32 [128], replicated, may hold values from 0.25 to 1.75
- key_gain: float32 [128], replicated, may hold values from 0.25 to 1.75
- post_gain: float32 [5376], replicated, may hold values from 0.5 to 1.5
- q_codes: int32 [5376, 2048], P('ctx', 'tp'), may hold values from 0 to 15
- q_scodes: int32 [5376, 32], P('ctx', 'tp'), may hold values from 0 to 255
- q_second: float32 [21, 32], P(None, 'tp'), as said below
- kv_codes: int32 [2, 5376, 1024], P(None, 'ctx', 'tp'), may hold values from 0 to 15
- kv_scodes: int32 [2, 5376, 16], P(None, 'ctx', 'tp'), may hold values from 0 to 255
- kv_second: float32 [2, 21, 16], P(None, None, 'tp'), as said below
- o_codes: int32 [5376, 2048], P('ctx', 'tp'), may hold values from 0 to 15
- o_scodes: int32 [5376, 32], P('ctx', 'tp'), may hold values from 0 to 255
- o_second: float32 [21, 32], P(None, 'tp'), as said below
- q_down: bfloat16 [5376, 16], replicated, may hold values from -0.078125 to 0.078125
- query_up: bfloat16 [16, 2048], P(None, 'tp'), may hold values from -0.23925781 to 0.23925781
- kv_down: bfloat16 [2, 5376, 16], replicated, may hold values from -0.078125 to 0.078125
- key_value_up: bfloat16 [2, 16, 1024], P(None, None, 'tp'), may hold values from -0.23925781 to 0.23925781
- output_down: bfloat16 [2048, 16], P('tp'), may hold values from -0.125 to 0.125
- output_up: bfloat16 [16, 5376], replicated, may hold values from -0.23925781 to 0.23925781
Outputs:
- mixed: bfloat16 [8192, 5376], P('ctx', 'tp')
- tokens_grad: float32 [8192, 5376], P('ctx', 'tp')
- query_down_gradient: float32 [5376, 16], replicated
- query_up_gradient: float32 [16, 2048], P(None, 'tp')
- key_value_down_gradient: float32 [2, 5376, 16], replicated
- key_value_up_gradient: float32 [2, 16, 1024], P(None, None, 'tp')
- output_down_gradient: float32 [2048, 16], P('tp')
- output_up_gradient: float32 [16, 5376], replicated
- in_projection: float32 [8192, 1], P('ctx')
The draws below stay inside these ranges and needn't reach their ends.
Inputs may be any that keep to these rules, and one draw needn't show every extreme that they name: `q_second`: positive, between one and eight over the square root of 5376. `kv_second`: positive, between one and eight over the square root of 5376. `o_second`: positive, between one and eight over the square root of 2048. `tokens`: real-valued activations of magnitude up to some tens.
All inputs are finite; a program needn't handle non-finite values.
Results may differ from the reference program's by a relative error of at most 0.015.
Values may be sent and summed in bfloat16 or wider, within the bound.
No kernel may reach another device: no remote copies, remote signals or barrier semaphores. Data moves between devices by JAX's collectives and lax.ppermute only.
A program may use at most 128 MiB of HBM per device.

```python
import jax
import jax.numpy as jnp
from jax import lax

D = 5376
HEAD_SIZE = 128
HQ = 16
KEY_VALUE_HEADS = 8
RANK = 16
WINDOW_TOKENS = 1024
QBLOCK = 64
QGROUP = 256
SLAB_TOKENS = 8192
FQ = 2048
FK = 1024


def spread_log(key, shape, lowest, highest):
    return jnp.exp(jax.random.uniform(key, shape, jnp.float32, jnp.log(lowest), jnp.log(highest)))


def draw_tokens(key, part):
    streams = jax.random.split(jax.random.fold_in(key, 11), 4)
    row_scales = spread_log(streams[0], (SLAB_TOKENS, 1), 0.3, 3.0)
    column_scales = spread_log(streams[1], (1, D), 0.3, 3.0)
    values = jax.random.normal(streams[3], (SLAB_TOKENS, D), jnp.float32)
    return (values * row_scales * column_scales).astype(jnp.bfloat16)


def scale_table(key, shape, fan_in):
    root = float(fan_in) ** 0.5
    return spread_log(key, shape, 2.0 / root, 5.0 / root)


def draw_q_second(key, part):
    return scale_table(jax.random.fold_in(key, 21), (D // QGROUP, FQ // QBLOCK), D)


def draw_kv_second(key, part):
    return scale_table(jax.random.fold_in(key, 22), (2, D // QGROUP, FK // QBLOCK), D)


def draw_o_second(key, part):
    return scale_table(jax.random.fold_in(key, 23), (D // QGROUP, FQ // QBLOCK), FQ)


def with_ends(array, rng, low, top_value):
    longest = array.shape.index(max(array.shape))
    spots = []
    for shift in (0, 1):
        where = [jax.random.randint(jax.random.fold_in(rng, axis), (), 0, length) for axis, length in enumerate(array.shape)]
        where[longest] = (where[longest] + shift) % array.shape[longest]
        spots.append(tuple(where))
    return array.at[spots[0]].set(low).at[spots[1]].set(top_value)


def block_scale(rng, shape, cuts, smallest, top_value):
    level, own = 1.0, jax.random.fold_in(rng, 6)
    for position, blocks in cuts:
        steps = jnp.exp(jax.random.uniform(jax.random.fold_in(own, position), (blocks,), jnp.float32, smallest / len(cuts), top_value / len(cuts)))
        level = level * jnp.repeat(steps, shape[position] // blocks).reshape([-1 if axis == position else 1 for axis in range(len(shape))])
    return level


def centred(key, dims, scale, reach, cuts=(), kind=jnp.bfloat16):
    level = block_scale(key, dims, cuts, -0.22, 0.18) if cuts else 1.0
    result = jax.random.normal(key, dims, jnp.float32) * scale * level
    return jnp.minimum(jnp.maximum(result, -reach), reach).astype(kind)


def setup_inputs(seed: int = 0) -> dict:
    splits = jax.random.split(jax.random.key(seed), 22)
    return {
        "tokens": draw_tokens(jax.random.fold_in(splits[21], 71), 0),
        "out_grad": centred(splits[1], (SLAB_TOKENS, D), 1.0, 6.0, ((0, 32), (1, 4))),
        "in_gain": jnp.clip(1.0 + 0.1 * jax.random.normal(splits[2], (D,), jnp.float32), 0.5, 1.5),
        "query_gain": jnp.clip(1.0 + 0.15 * jax.random.normal(splits[3], (HEAD_SIZE,), jnp.float32), 0.25, 1.75),
        "key_gain": jnp.clip(1.0 + 0.15 * jax.random.normal(splits[4], (HEAD_SIZE,), jnp.float32), 0.25, 1.75),
        "post_gain": jnp.clip(1.0 + 0.1 * jax.random.normal(splits[5], (D,), jnp.float32), 0.5, 1.5),
        "q_codes": with_ends(jax.random.randint(splits[6], (D, FQ), 0, 16), jax.random.fold_in(splits[6], 1), 0, 15).astype(jnp.int32),
        "q_scodes": with_ends(jax.random.randint(splits[7], (D, FQ // QBLOCK), 0, 256), jax.random.fold_in(splits[7], 1), 0, 255).astype(jnp.int32),
        "q_second": draw_q_second(jax.random.fold_in(splits[21], 71), 0),
        "kv_codes": with_ends(jax.random.randint(splits[9], (2, D, FK), 0, 16), jax.random.fold_in(splits[9], 1), 0, 15).astype(jnp.int32),
        "kv_scodes": with_ends(jax.random.randint(splits[10], (2, D, FK // QBLOCK), 0, 256), jax.random.fold_in(splits[10], 1), 0, 255).astype(jnp.int32),
        "kv_second": draw_kv_second(jax.random.fold_in(splits[21], 71), 0),
        "o_codes": with_ends(jax.random.randint(splits[12], (D, FQ), 0, 16), jax.random.fold_in(splits[12], 1), 0, 15).astype(jnp.int32),
        "o_scodes": with_ends(jax.random.randint(splits[13], (D, FQ // QBLOCK), 0, 256), jax.random.fold_in(splits[13], 1), 0, 255).astype(jnp.int32),
        "o_second": draw_o_second(jax.random.fold_in(splits[21], 71), 0),
        "q_down": centred(splits[15], (D, RANK), D ** -0.5, 0.078125),
        "query_up": centred(splits[16], (RANK, FQ), 0.04, 0.23925781, ((1, 4),)),
        "kv_down": centred(splits[17], (2, D, RANK), D ** -0.5, 0.078125),
        "key_value_up": centred(splits[18], (2, RANK, FK), 0.04, 0.23925781, ((2, 4),)),
        "output_down": centred(splits[19], (FQ, RANK), FQ ** -0.5, 0.125, ((0, 4),)),
        "output_up": centred(splits[20], (RANK, D), 0.04, 0.23925781),
    }


NORMAL_FLOAT = (-1.0, -0.6961928009986877, -0.5250730514526367, -0.39491748809814453, -0.28444138169288635, -0.18477343022823334, -0.09105003625154495, 0.0, 0.07958029955625534, 0.16093020141124725, 0.24611230194568634, 0.33791524171829224, 0.44070982933044434, 0.5626170039176941, 0.7229568362236023, 1.0)
EPSILON = 1e-06
ADAPTER_SCALE = 2.0
SCORE_SCALE = 168.0 ** (-0.5)
ROPE_BASE = 10000.0

def widen(value_rows):
    return lax.optimization_barrier(value_rows).astype(jnp.float32)

def dequantize(codes, scodes, second):
    height, width = codes.shape
    levels = jnp.zeros(codes.shape, jnp.float32)
    for level in range(16):
        levels = jnp.where(codes == level, jnp.float32(NORMAL_FLOAT[level]), levels)
    second_rows = jnp.repeat(second, QGROUP, axis=0)
    absmax = second_rows * ((scodes.astype(jnp.float32) + 1.0) / 256.0)
    scaled = levels.reshape(height, width // QBLOCK, QBLOCK) * absmax[:, :, None]
    return scaled.reshape(height, width).astype(jnp.bfloat16)

def rope_tables(positions):
    half = HEAD_SIZE // 2
    exponent = jnp.arange(half, dtype=jnp.float32) * (2.0 / HEAD_SIZE)
    frequency = jnp.power(jnp.float32(ROPE_BASE), -exponent)
    angle = positions.astype(jnp.float32)[:, None] * frequency[None, :]
    return (jnp.cos(angle), jnp.sin(angle))

def rotate(heads, cosine, sine):
    half = heads.shape[-1] // 2
    first = heads[..., :half]
    second = heads[..., half:]
    across = cosine[:, None, :]
    along = sine[:, None, :]
    return jnp.concatenate([first * across - second * along, second * across + first * along], axis=-1)

def unrotate(grad, cosine, sine):
    half = grad.shape[-1] // 2
    first = grad[..., :half]
    second = grad[..., half:]
    across = cosine[:, None, :]
    along = sine[:, None, :]
    return jnp.concatenate([first * across + second * along, second * across - first * along], axis=-1)

def head_norm(heads, gain):
    scale = lax.rsqrt(lax.optimization_barrier(jnp.mean(heads * heads, axis=-1, keepdims=True)) + EPSILON)
    return (heads * scale * gain, scale)

def head_norm_back(heads, scale, gain, grad):
    weighted = grad * gain
    inner = lax.optimization_barrier(jnp.mean(weighted * heads, axis=-1, keepdims=True))
    return scale * weighted - scale ** 3 * heads * inner

def probabilities(q_rot, keys, query_pos, key_pos):
    count, q_heads, width = q_rot.shape
    kv_heads = keys.shape[1]
    grouped = q_rot.reshape(count, kv_heads, q_heads // kv_heads, width)
    scores = jnp.einsum('tkgd,lkd->kgtl', widen(grouped), widen(keys)) * SCORE_SCALE
    gap = query_pos[:, None] - key_pos[None, :]
    allowed = (gap >= 0) & (gap < WINDOW_TOKENS) & (key_pos[None, :] >= 0)
    weights = jnp.where(allowed, jnp.exp(scores), 0.0)
    return (weights / lax.optimization_barrier(jnp.sum(weights, axis=-1, keepdims=True)), grouped)

def attention_forward(q_rot, keys, values, query_pos, key_pos):
    count, q_heads, width = q_rot.shape
    probability, grouped = probabilities(q_rot, keys, query_pos, key_pos)
    prob_low = probability.astype(jnp.bfloat16)
    mixed = jnp.einsum('kgtl,lkd->tkgd', widen(prob_low), widen(values))
    return mixed.reshape(count, q_heads * width).astype(jnp.bfloat16)

def attention_backward(q_rot, keys, values, output_gradient, query_pos, key_pos):
    count, q_heads, width = q_rot.shape
    kv_heads = keys.shape[1]
    probability, grouped = probabilities(q_rot, keys, query_pos, key_pos)
    prob_low = probability.astype(jnp.bfloat16)
    grad_grouped = output_gradient.reshape(count, kv_heads, q_heads // kv_heads, width)
    grad_prob = jnp.einsum('tkgd,lkd->kgtl', widen(grad_grouped), widen(values))
    grad_values = jnp.einsum('kgtl,tkgd->lkd', widen(prob_low), widen(grad_grouped))
    inner = lax.optimization_barrier(jnp.sum(probability * grad_prob, axis=-1, keepdims=True))
    grad_scores = (probability * (grad_prob - inner) * SCORE_SCALE).astype(jnp.bfloat16)
    grad_query = jnp.einsum('kgtl,lkd->tkgd', widen(grad_scores), widen(keys)).reshape(count, q_heads, width)
    grad_keys = jnp.einsum('kgtl,tkgd->lkd', widen(grad_scores), widen(grouped))
    return (grad_query, grad_keys, grad_values)

def reference(tokens, out_grad, in_gain, query_gain, key_gain, post_gain, q_codes, q_scodes, q_second, kv_codes, kv_scodes, kv_second, o_codes, o_scodes, o_second, q_down, query_up, kv_down, key_value_up, output_down, output_up):
    query_matrix = dequantize(q_codes, q_scodes, q_second)
    key_matrix = dequantize(kv_codes[0], kv_scodes[0], kv_second[0])
    value_matrix = dequantize(kv_codes[1], kv_scodes[1], kv_second[1])
    output_matrix = dequantize(o_codes, o_scodes, o_second)
    wide = tokens.astype(jnp.float32)
    row_scale = lax.rsqrt(lax.optimization_barrier(jnp.mean(wide * wide, axis=1, keepdims=True)) + EPSILON)
    normalized_input = (wide * row_scale * in_gain).astype(jnp.bfloat16)
    query_lowrank = jnp.dot(normalized_input, q_down, preferred_element_type=jnp.float32).astype(jnp.bfloat16)
    key_lowrank = jnp.dot(normalized_input, kv_down[0], preferred_element_type=jnp.float32).astype(jnp.bfloat16)
    value_lowrank = jnp.dot(normalized_input, kv_down[1], preferred_element_type=jnp.float32).astype(jnp.bfloat16)
    query_rows = jnp.dot(normalized_input, query_matrix, preferred_element_type=jnp.float32) + ADAPTER_SCALE * jnp.dot(query_lowrank, query_up, preferred_element_type=jnp.float32)
    key = jnp.dot(normalized_input, key_matrix, preferred_element_type=jnp.float32) + ADAPTER_SCALE * jnp.dot(key_lowrank, key_value_up[0], preferred_element_type=jnp.float32)
    value_total = jnp.dot(normalized_input, value_matrix, preferred_element_type=jnp.float32) + ADAPTER_SCALE * jnp.dot(value_lowrank, key_value_up[1], preferred_element_type=jnp.float32)
    value_rows = value_total.astype(jnp.bfloat16).reshape(SLAB_TOKENS, KEY_VALUE_HEADS, HEAD_SIZE)
    positions = jnp.arange(SLAB_TOKENS, dtype=jnp.int32)
    cosine, sine = rope_tables(positions)
    q_heads = query_rows.reshape(SLAB_TOKENS, HQ, HEAD_SIZE)
    q_normed, q_scale = head_norm(q_heads, query_gain)
    q_rot = rotate(q_normed, cosine, sine).astype(jnp.bfloat16)
    key_head_rows = key.reshape(SLAB_TOKENS, KEY_VALUE_HEADS, HEAD_SIZE)
    k_normed, k_scale = head_norm(key_head_rows, key_gain)
    k_rot = rotate(k_normed, cosine, sine).astype(jnp.bfloat16)
    front_rows = jnp.zeros((WINDOW_TOKENS, KEY_VALUE_HEADS, HEAD_SIZE), jnp.bfloat16)
    key_pad = jnp.concatenate([front_rows, k_rot], axis=0)
    value_pad = jnp.concatenate([front_rows, value_rows], axis=0)
    blocks = SLAB_TOKENS // WINDOW_TOKENS
    block_ids = jnp.arange(blocks, dtype=jnp.int32)

    def block_inputs(index):
        start = index * WINDOW_TOKENS
        q_block = lax.dynamic_slice_in_dim(q_rot, start, WINDOW_TOKENS, 0)
        k_block = lax.dynamic_slice_in_dim(key_pad, start, 2 * WINDOW_TOKENS, 0)
        v_block = lax.dynamic_slice_in_dim(value_pad, start, 2 * WINDOW_TOKENS, 0)
        query_pos = start + jnp.arange(WINDOW_TOKENS, dtype=jnp.int32)
        key_pos = start - WINDOW_TOKENS + jnp.arange(2 * WINDOW_TOKENS, dtype=jnp.int32)
        return (start, q_block, k_block, v_block, query_pos, key_pos)

    def forward_block(index):
        start, q_block, k_block, v_block, query_pos, key_pos = block_inputs(index)
        return attention_forward(q_block, k_block, v_block, query_pos, key_pos)
    attended_rows = lax.map(forward_block, block_ids).reshape(SLAB_TOKENS, FQ)
    output_lowrank = jnp.dot(attended_rows, output_down, preferred_element_type=jnp.float32).astype(jnp.bfloat16)
    output_total_sum = jnp.dot(attended_rows, output_matrix.T, preferred_element_type=jnp.float32) + ADAPTER_SCALE * jnp.dot(output_lowrank, output_up, preferred_element_type=jnp.float32)
    out_scale = lax.rsqrt(lax.optimization_barrier(jnp.mean(output_total_sum * output_total_sum, axis=1, keepdims=True)) + EPSILON)
    mixed = (wide + output_total_sum * out_scale * post_gain).astype(jnp.bfloat16)
    weighted_out = out_grad.astype(jnp.float32) * post_gain
    out_inner = lax.optimization_barrier(jnp.mean(weighted_out * output_total_sum, axis=1, keepdims=True))
    output_gradient = (out_scale * weighted_out - out_scale ** 3 * output_total_sum * out_inner).astype(jnp.bfloat16)
    output_mixture = jnp.dot(output_gradient, output_up.T, preferred_element_type=jnp.float32).astype(jnp.bfloat16)
    output_up_gradient = ADAPTER_SCALE * jnp.dot(output_lowrank.T, output_gradient, preferred_element_type=jnp.float32)
    output_down_gradient = ADAPTER_SCALE * jnp.dot(attended_rows.T, output_mixture, preferred_element_type=jnp.float32)
    attended_gradient = (jnp.dot(output_gradient, output_matrix, preferred_element_type=jnp.float32) + ADAPTER_SCALE * jnp.dot(output_mixture, output_down.T, preferred_element_type=jnp.float32)).astype(jnp.bfloat16)

    def backward_block(carry, index):
        key_grad, value_grad = carry
        start, q_block, k_block, v_block, query_pos, key_pos = block_inputs(index)
        grad_block = lax.dynamic_slice_in_dim(attended_gradient, start, WINDOW_TOKENS, 0)
        grad_query, grad_keys, grad_values = attention_backward(q_block, k_block, v_block, grad_block, query_pos, key_pos)
        key_grad = lax.dynamic_update_slice_in_dim(key_grad, lax.dynamic_slice_in_dim(key_grad, start, 2 * WINDOW_TOKENS, 0) + grad_keys, start, 0)
        value_grad = lax.dynamic_update_slice_in_dim(value_grad, lax.dynamic_slice_in_dim(value_grad, start, 2 * WINDOW_TOKENS, 0) + grad_values, start, 0)
        return ((key_grad, value_grad), grad_query)
    empty_state = jnp.zeros((SLAB_TOKENS + WINDOW_TOKENS, KEY_VALUE_HEADS, HEAD_SIZE), jnp.float32)
    (key_grad, value_grad), query_grad = lax.scan(backward_block, (empty_state, empty_state), block_ids)
    query_grad = query_grad.reshape(SLAB_TOKENS, HQ, HEAD_SIZE)
    key_grad = key_grad[WINDOW_TOKENS:]
    value_grad = value_grad[WINDOW_TOKENS:]
    q_norm_grad = unrotate(query_grad, cosine, sine)
    k_norm_grad = unrotate(key_grad, cosine, sine)
    query_gradient_lowrank = head_norm_back(q_heads, q_scale, query_gain, q_norm_grad).reshape(SLAB_TOKENS, FQ).astype(jnp.bfloat16)
    key_gradient_lowrank = head_norm_back(key_head_rows, k_scale, key_gain, k_norm_grad).reshape(SLAB_TOKENS, FK).astype(jnp.bfloat16)
    value_gradient_lowrank = value_grad.reshape(SLAB_TOKENS, FK).astype(jnp.bfloat16)
    query_mixture = jnp.dot(query_gradient_lowrank, query_up.T, preferred_element_type=jnp.float32).astype(jnp.bfloat16)
    key_mixture = jnp.dot(key_gradient_lowrank, key_value_up[0].T, preferred_element_type=jnp.float32).astype(jnp.bfloat16)
    value_mixture = jnp.dot(value_gradient_lowrank, key_value_up[1].T, preferred_element_type=jnp.float32).astype(jnp.bfloat16)
    normalized_gradient = jnp.dot(query_gradient_lowrank, query_matrix.T, preferred_element_type=jnp.float32)
    normalized_gradient = normalized_gradient + jnp.dot(key_gradient_lowrank, key_matrix.T, preferred_element_type=jnp.float32)
    normalized_gradient = normalized_gradient + jnp.dot(value_gradient_lowrank, value_matrix.T, preferred_element_type=jnp.float32)
    adapter_term = jnp.dot(query_mixture, q_down.T, preferred_element_type=jnp.float32) + jnp.dot(key_mixture, kv_down[0].T, preferred_element_type=jnp.float32) + jnp.dot(value_mixture, kv_down[1].T, preferred_element_type=jnp.float32)
    normalized_gradient = normalized_gradient + ADAPTER_SCALE * adapter_term
    weighted_in = normalized_gradient * in_gain
    in_inner = lax.optimization_barrier(jnp.mean(weighted_in * wide, axis=1, keepdims=True))
    tokens_grad = out_grad.astype(jnp.float32) + row_scale * weighted_in - row_scale ** 3 * wide * in_inner
    in_projection = float(D) ** 0.5 * row_scale * in_inner
    query_down_gradient = ADAPTER_SCALE * jnp.dot(normalized_input.T, query_mixture, preferred_element_type=jnp.float32)
    key_value_down_gradient = jnp.stack([ADAPTER_SCALE * jnp.dot(normalized_input.T, key_mixture, preferred_element_type=jnp.float32), ADAPTER_SCALE * jnp.dot(normalized_input.T, value_mixture, preferred_element_type=jnp.float32)])
    query_up_gradient = ADAPTER_SCALE * jnp.dot(query_lowrank.T, query_gradient_lowrank, preferred_element_type=jnp.float32)
    key_value_up_gradient = jnp.stack([ADAPTER_SCALE * jnp.dot(key_lowrank.T, key_gradient_lowrank, preferred_element_type=jnp.float32), ADAPTER_SCALE * jnp.dot(value_lowrank.T, value_gradient_lowrank, preferred_element_type=jnp.float32)])
    return (mixed, tokens_grad, query_down_gradient, query_up_gradient, key_value_down_gradient, key_value_up_gradient, output_down_gradient, output_up_gradient, in_projection)
```

```python
import jax
import jax.numpy as jnp
from jax import lax
from jax.sharding import Mesh
from jax.sharding import PartitionSpec as P

D = 5376
HEAD_SIZE = 128
WINDOW_TOKENS = 1024
QBLOCK = 64
QGROUP = 256
CTX = ("y", "z", "xh")
TP = ("xl", "c")
NORMAL_FLOAT = (
    -1.0,
    -0.6961928009986877,
    -0.5250730514526367,
    -0.39491748809814453,
    -0.28444138169288635,
    -0.18477343022823334,
    -0.09105003625154495,
    0.0,
    0.07958029955625534,
    0.16093020141124725,
    0.24611230194568634,
    0.33791524171829224,
    0.44070982933044434,
    0.5626170039176941,
    0.7229568362236023,
    1.0,
)
EPSILON = 1e-06
ADAPTER_SCALE = 2.0
SCORE_SCALE = 168.0 ** (-0.5)
ROPE_BASE = 10000.0
BF = jnp.bfloat16
F32 = jnp.float32


def swap(x, axis):
    return lax.ppermute(x, axis, [(0, 1), (1, 0)])


def ring(x, axis, by):
    n = lax.axis_size(axis)
    return lax.ppermute(x, axis, [(i, (i + by) % n) for i in range(n)])


def ring_pieces(v, axis):
    h = v.shape[0] // 2
    left = ring(v, axis, 1)
    right = ring(v, axis, -1)
    return [v, left, ring(left[:h], axis, 1), ring(right[h:], axis, -1), right]


def shifted(x, by):
    n = lax.axis_size(CTX)
    return lax.ppermute(x, CTX, [(i, i + by) for i in range(n) if 0 <= i + by < n])


def dot_f32(a, b, ca, cb):
    return lax.dot_general(a, b, (((ca,), (cb,)), ((), ())), preferred_element_type=F32)


def dequantize(codes, scodes, second, row_start):
    height, width = codes.shape
    levels = jnp.zeros(codes.shape, F32)
    for level in range(16):
        levels = jnp.where(codes == level, F32(NORMAL_FLOAT[level]), levels)
    group_ids = (row_start + jnp.arange(height, dtype=jnp.int32)) // QGROUP
    group_list = jnp.arange(second.shape[0], dtype=jnp.int32)
    picker = (group_ids[:, None] == group_list[None, :]).astype(F32)
    second_rows = jnp.dot(picker, second, precision=lax.Precision.HIGHEST)
    absmax = second_rows * ((scodes.astype(F32) + 1.0) / 256.0)
    scaled = levels.reshape(height, width // QBLOCK, QBLOCK) * absmax[:, :, None]
    return scaled.reshape(height, width).astype(BF)


def rope_tables(positions):
    half = HEAD_SIZE // 2
    exponent = jnp.arange(half, dtype=F32) * (2.0 / HEAD_SIZE)
    frequency = jnp.power(F32(ROPE_BASE), -exponent)
    angle = positions.astype(F32)[:, None] * frequency[None, :]
    return (jnp.cos(angle), jnp.sin(angle))


def rotate(heads, cosine, sine):
    half = heads.shape[-1] // 2
    first = heads[..., :half]
    second = heads[..., half:]
    across = cosine[:, None, :]
    along = sine[:, None, :]
    return jnp.concatenate(
        [first * across - second * along, second * across + first * along], axis=-1
    )


def unrotate(grad, cosine, sine):
    return rotate(grad, cosine, -sine)


def head_norm(heads, gain):
    scale = lax.rsqrt(jnp.mean(heads * heads, axis=-1, keepdims=True) + EPSILON)
    return (heads * scale * gain, scale)


def head_norm_back(heads, scale, gain, grad):
    weighted = grad * gain
    inner = jnp.mean(weighted * heads, axis=-1, keepdims=True)
    return scale * weighted - scale**3 * heads * inner


def probabilities(q_rot, keys, query_pos, key_pos):
    count, q_heads, width = q_rot.shape
    kv_heads = keys.shape[1]
    grouped = q_rot.reshape(count, kv_heads, q_heads // kv_heads, width)
    scores = (
        jnp.einsum("tkgd,lkd->kgtl", grouped, keys, preferred_element_type=F32) * SCORE_SCALE
    )
    gap = query_pos[:, None] - key_pos[None, :]
    allowed = (gap >= 0) & (gap < WINDOW_TOKENS) & (key_pos[None, :] >= 0)
    weights = jnp.where(allowed, jnp.exp(scores), 0.0)
    return (weights / jnp.sum(weights, axis=-1, keepdims=True), grouped)


def attention_forward(q_rot, keys, values, query_pos, key_pos):
    count, q_heads, width = q_rot.shape
    probability, grouped = probabilities(q_rot, keys, query_pos, key_pos)
    prob_low = probability.astype(BF)
    mixed = jnp.einsum("kgtl,lkd->tkgd", prob_low, values, preferred_element_type=F32)
    return mixed.reshape(count, q_heads * width).astype(BF)


def attention_backward(q_rot, keys, values, output_gradient, query_pos, key_pos):
    count, q_heads, width = q_rot.shape
    kv_heads = keys.shape[1]
    probability, grouped = probabilities(q_rot, keys, query_pos, key_pos)
    prob_low = probability.astype(BF)
    grad_grouped = output_gradient.reshape(count, kv_heads, q_heads // kv_heads, width)
    grad_prob = jnp.einsum("tkgd,lkd->kgtl", grad_grouped, values, preferred_element_type=F32)
    grad_values = jnp.einsum("kgtl,tkgd->lkd", prob_low, grad_grouped, preferred_element_type=F32)
    inner = jnp.sum(probability * grad_prob, axis=-1, keepdims=True)
    grad_scores = (probability * (grad_prob - inner) * SCORE_SCALE).astype(BF)
    grad_query = jnp.einsum(
        "kgtl,lkd->tkgd", grad_scores, keys, preferred_element_type=F32
    ).reshape(count, q_heads, width)
    grad_keys = jnp.einsum("kgtl,tkgd->lkd", grad_scores, grouped, preferred_element_type=F32)
    return (grad_query, grad_keys, grad_values)


def gathered_pieces(own, xl, c):
    other = swap(own, "xl")
    pair = jnp.stack([jnp.where(xl == 0, own, other), jnp.where(xl == 0, other, own)])
    far = swap(pair, "c")
    return jnp.stack([jnp.where(c == 0, pair, far), jnp.where(c == 0, far, pair)], axis=1)


def on_device(
    tokens,
    out_grad,
    in_gain,
    query_gain,
    key_gain,
    post_gain,
    q_codes,
    q_scodes,
    q_second,
    kv_codes,
    kv_scodes,
    kv_second,
    o_codes,
    o_scodes,
    o_second,
    q_down,
    query_up,
    kv_down,
    key_value_up,
    output_down,
    output_up,
):
    count, share = tokens.shape
    y, z, xh = (lax.axis_index(a) for a in CTX)
    xl, c = (lax.axis_index(a) for a in TP)
    ctx_rank = lax.axis_index(CTX)
    column_start = lax.axis_index(TP) * share
    rows = q_codes.shape[0]
    row_start = ctx_rank * rows
    blocks = share // rows
    ny, nz = lax.axis_size("y"), lax.axis_size("z")
    q_width = query_up.shape[1]
    kv_width = key_value_up.shape[2]
    q_heads_here = q_width // HEAD_SIZE
    kv_heads_here = kv_width // HEAD_SIZE

    q_part = dequantize(q_codes, q_scodes, q_second, row_start)
    k_part = dequantize(kv_codes[0], kv_scodes[0], kv_second[0], row_start)
    v_part = dequantize(kv_codes[1], kv_scodes[1], kv_second[1], row_start)
    kv_part = jnp.concatenate([k_part, v_part], axis=1)
    o_part = dequantize(o_codes, o_scodes, o_second, row_start)
    kv_near = jnp.concatenate(ring_pieces(kv_part, "y"))
    q_near = jnp.concatenate(ring_pieces(q_part, "z"))
    kv_pieces = ring_pieces(kv_near, "z")
    q_pieces = ring_pieces(q_near, "y")

    tokens_t = tokens.T
    mine = tokens_t.reshape(blocks // 2, 2, rows, count)
    keep = lax.dynamic_index_in_dim(mine, xh, 1, False)
    give = lax.dynamic_index_in_dim(mine, 1 - xh, 1, False)
    pair = jnp.concatenate([keep, swap(give, "xh")], axis=-1)
    wide = gathered_pieces(pair, xl, c).reshape(ny, nz, rows, 2 * count).astype(F32)
    partial_sum = jnp.sum(wide * wide, axis=(0, 1, 2))
    other_sum = swap(partial_sum.reshape(4, -1), "xh").reshape(-1)
    square_sum = partial_sum + jnp.roll(other_sum, count)
    pair_scale = lax.rsqrt(square_sum / D + EPSILON)
    gain_parity = lax.dynamic_index_in_dim(in_gain.reshape(ny, nz, 2, rows), xh, 2, False)
    normed = (wide * pair_scale * gain_parity[..., None]).astype(BF)

    def turned(a, axis, at):
        n = a.shape[axis]
        return jnp.concatenate(
            [lax.dynamic_slice_in_dim(a, (at - r) % n, 1, axis) for r in range(n)], axis
        )

    normed = turned(turned(normed, 0, y), 1, z)
    normed_kv = normed.transpose(1, 0, 2, 3).reshape(D // 2, -1)
    normed_q = normed.reshape(D // 2, -1)
    downs = jnp.concatenate([q_down, kv_down[0], kv_down[1]], axis=1)
    downs_parity = lax.dynamic_index_in_dim(downs.reshape(ny, nz, 2, rows, -1), xh, 2, False)
    downs_parity = turned(turned(downs_parity, 0, y), 1, z).reshape(D // 2, -1)

    def by_pieces(acts, pieces):
        total, at = None, 0
        for p in pieces:
            term = dot_f32(acts[at : at + p.shape[0]], p, 0, 0)
            total = term if total is None else total + term
            at += p.shape[0]
        return total

    low_pair = dot_f32(normed_q, downs_parity, 0, 0)
    low_sum = low_pair[:count] + swap(low_pair[count:], "xh")
    low = low_sum.astype(BF)
    rank = q_down.shape[1]
    query_lowrank, key_lowrank, value_lowrank = (
        low[:, i * rank : (i + 1) * rank] for i in range(3)
    )
    kv_pair = by_pieces(normed_kv, kv_pieces)
    kv_sum = kv_pair[:count] + swap(kv_pair[count:].astype(BF), "xh").astype(F32)
    q_pair = by_pieces(normed_q, q_pieces)
    q_sum = q_pair[:count] + swap(q_pair[count:].astype(BF), "xh").astype(F32)
    row_scale = pair_scale[:count]

    key = kv_sum[:, :kv_width] + ADAPTER_SCALE * dot_f32(key_lowrank, key_value_up[0], 1, 0)
    value_total = kv_sum[:, kv_width:] + ADAPTER_SCALE * dot_f32(
        value_lowrank, key_value_up[1], 1, 0
    )
    value_rows = value_total.astype(BF)
    query_rows = q_sum + ADAPTER_SCALE * dot_f32(query_lowrank, query_up, 1, 0)

    query_pos = ctx_rank * count + jnp.arange(count, dtype=jnp.int32)
    key_pos = ctx_rank * count - WINDOW_TOKENS + jnp.arange(WINDOW_TOKENS + count, dtype=jnp.int32)
    cosine, sine = rope_tables(query_pos)
    key_head_rows = key.reshape(count, kv_heads_here, HEAD_SIZE)
    k_normed, k_scale = head_norm(key_head_rows, key_gain)
    k_rot = rotate(k_normed, cosine, sine).astype(BF)
    kv_rows = jnp.concatenate([k_rot.reshape(count, kv_width), value_rows], axis=1)
    steps = WINDOW_TOKENS // count
    window = jnp.concatenate([shifted(kv_rows, s) for s in range(steps, 0, -1)] + [kv_rows])
    window_keys = window[:, :kv_width].reshape(-1, kv_heads_here, HEAD_SIZE)
    window_values = window[:, kv_width:].reshape(-1, kv_heads_here, HEAD_SIZE)
    q_heads = query_rows.reshape(count, q_heads_here, HEAD_SIZE)
    q_normed, q_scale = head_norm(q_heads, query_gain)
    q_rot = rotate(q_normed, cosine, sine).astype(BF)

    o_swapped = swap(o_part, "xh")
    qkv_part = jnp.concatenate([q_part, kv_part], axis=1)
    qkv_swapped = swap(qkv_part, "xh")
    o_both = jnp.concatenate(
        [jnp.where(xh == 0, o_part, o_swapped), jnp.where(xh == 0, o_swapped, o_part)]
    )
    qkv_both = jnp.concatenate(
        [jnp.where(xh == 0, qkv_part, qkv_swapped), jnp.where(xh == 0, qkv_swapped, qkv_part)]
    )
    output_matrix = lax.all_gather(o_both, ("y", "z"), axis=0, tiled=True)
    qkv_matrix = lax.all_gather(qkv_both, ("y", "z"), axis=0, tiled=True)
    out_grad_t = out_grad.T
    out_grad_full = gathered_pieces(out_grad_t, xl, c)

    attended = attention_forward(q_rot, window_keys, window_values, query_pos, key_pos)

    low_out_part = dot_f32(attended, output_down, 1, 0).astype(BF)
    out_rows = output_matrix.reshape(2, 2 * share, q_width)
    up_rows = output_up.T.reshape(2, 2 * share, rank)
    low_rows = low_out_part.T.astype(F32)
    sums, low_total = [], None
    for j in range(2):
        part = dot_f32(out_rows[j], attended, 1, 1) + ADAPTER_SCALE * dot_f32(
            up_rows[j], low_out_part, 1, 1
        )
        part = part.reshape(2, share, count)
        keep = lax.dynamic_index_in_dim(part, c, 0, False)
        give = lax.dynamic_index_in_dim(part, 1 - c, 0, False)
        if j == 0:
            keep = jnp.concatenate([keep, low_rows])
            give = jnp.concatenate([give, low_rows])
        chip = (keep + swap(give.astype(BF), "c").astype(F32)).astype(BF)
        total = (chip.astype(F32) + swap(chip, "xl").astype(F32)).astype(BF)
        if j == 0:
            low_total = total[share:]
            total = total[:share]
        far = swap(total, "c")
        sums.append(jnp.stack([jnp.where(c == 0, total, far), jnp.where(c == 0, far, total)]))
    out_total = jnp.stack(sums).astype(F32)
    output_lowrank = low_total.T
    gain_full = post_gain.reshape(2, 2, share, 1)
    weighted_out = out_grad_full.astype(F32) * gain_full
    out_scale = lax.rsqrt(jnp.sum(out_total * out_total, axis=(0, 1, 2)) / D + EPSILON)
    out_inner = jnp.sum(weighted_out * out_total, axis=(0, 1, 2)) / D
    grad_full = (out_scale * weighted_out - out_scale**3 * out_total * out_inner).astype(BF)
    output_gradient = grad_full.reshape(D, count)
    out_mine = lax.dynamic_slice_in_dim(out_total.reshape(D, count), column_start, share, 0)
    post_mine = lax.dynamic_slice_in_dim(post_gain, column_start, share, 0)[:, None]
    mixed = (tokens_t.astype(F32) + out_mine * out_scale * post_mine).astype(BF)

    output_mixture = dot_f32(output_gradient, output_up, 0, 1).astype(BF)
    grad_mine = lax.dynamic_slice_in_dim(output_gradient, column_start, share, 0)
    output_up_gradient = ADAPTER_SCALE * dot_f32(output_lowrank, grad_mine, 0, 1)
    output_down_gradient = ADAPTER_SCALE * dot_f32(output_mixture, attended, 0, 0)
    attended_gradient = (
        dot_f32(output_gradient, output_matrix, 0, 0)
        + ADAPTER_SCALE * dot_f32(output_mixture, output_down, 1, 1)
    ).astype(BF)
    query_grad, key_window_grad, value_window_grad = attention_backward(
        q_rot, window_keys, window_values, attended_gradient, query_pos, key_pos
    )
    window_grad = jnp.concatenate(
        [key_window_grad.reshape(-1, kv_width), value_window_grad.reshape(-1, kv_width)], axis=1
    )
    own = window_grad[WINDOW_TOKENS:]
    for s in range(steps, 0, -1):
        piece = window_grad[(steps - s) * count : (steps - s + 1) * count].astype(BF)
        own = own + shifted(piece, -s).astype(F32)
    q_norm_grad = unrotate(query_grad, cosine, sine)
    k_norm_grad = unrotate(own[:, :kv_width].reshape(count, kv_heads_here, HEAD_SIZE), cosine, sine)
    query_back = head_norm_back(q_heads, q_scale, query_gain, q_norm_grad)
    query_back = query_back.reshape(count, q_width).astype(BF)
    key_back = head_norm_back(key_head_rows, k_scale, key_gain, k_norm_grad)
    key_back = key_back.reshape(count, kv_width).astype(BF)
    value_back = own[:, kv_width:].astype(BF)

    inner_part = (
        jnp.sum(query_back.astype(F32) * query_rows, axis=1)
        + jnp.sum(key_back.astype(F32) * key, axis=1)
        + jnp.sum(value_back.astype(F32) * value_total, axis=1)
    )
    small = jnp.concatenate(
        [
            dot_f32(query_up, query_back, 1, 1),
            dot_f32(key_value_up[0], key_back, 1, 1),
            dot_f32(key_value_up[1], value_back, 1, 1),
            inner_part[None],
            jnp.zeros((7, count), F32),
        ]
    )
    small = jnp.sum(lax.all_gather(small, TP), axis=0)
    mixes = small[: 3 * rank].astype(BF)
    in_inner = small[3 * rank] / (row_scale * D)

    normed_mine = lax.dynamic_slice_in_dim(in_gain, column_start, share, 0)[:, None]
    in_gain_mine = normed_mine
    tokens_wide = tokens_t.astype(F32)
    normed_mine = (tokens_wide * row_scale * in_gain_mine).astype(BF)
    down_gradients = ADAPTER_SCALE * dot_f32(mixes, normed_mine, 1, 1)
    up_gradients = ADAPTER_SCALE * jnp.concatenate(
        [
            dot_f32(query_lowrank, query_back, 0, 0),
            dot_f32(key_lowrank, key_back, 0, 0),
            dot_f32(value_lowrank, value_back, 0, 0),
        ],
        axis=1,
    )
    everything = jnp.concatenate(
        [
            down_gradients.reshape(-1),
            output_up_gradient.reshape(-1),
            up_gradients.reshape(-1),
            output_down_gradient.reshape(-1),
        ]
    )
    devices = lax.axis_size(CTX)
    parts = everything.reshape(devices, -1, 128)
    arrived = lax.all_to_all(parts, CTX, 0, 0, tiled=True)
    chunk = jnp.sum(arrived, axis=0)
    spread = jnp.broadcast_to(chunk[None], (devices, *chunk.shape))
    summed = lax.all_to_all(spread, CTX, 0, 0, tiled=True).reshape(-1)
    cut = 4 * rank * share
    wide_sums = gathered_pieces(summed[:cut].reshape(4 * rank, share), xl, c)
    wide_sums = jnp.moveaxis(wide_sums.reshape(4, 4 * rank, share), 0, 1).reshape(4 * rank, D)
    narrow = summed[cut : cut + up_gradients.size].reshape(up_gradients.shape)
    output_down_gradient = summed[cut + up_gradients.size :].reshape(rank, q_width).T

    grads = jnp.concatenate([query_back, key_back, value_back], axis=1)
    into_part = dot_f32(qkv_matrix, grads, 1, 1).reshape(2, 2, share, count)
    keep = lax.dynamic_index_in_dim(into_part, c, 1, False)
    give = lax.dynamic_index_in_dim(into_part, 1 - c, 1, False)
    chip = keep + swap(give.astype(BF), "c").astype(F32)
    keep = lax.dynamic_index_in_dim(chip, xl, 0, False)
    give = lax.dynamic_index_in_dim(chip, 1 - xl, 0, False)
    into_mine = keep + swap(give.astype(BF), "xl").astype(F32)
    downs_mine = lax.dynamic_slice_in_dim(downs, column_start, share, 0)
    normalized_gradient = into_mine + ADAPTER_SCALE * dot_f32(downs_mine, mixes, 1, 0)
    weighted_in = normalized_gradient * in_gain_mine
    tokens_grad = (
        out_grad_t.astype(F32)
        + row_scale * weighted_in
        - row_scale**3 * tokens_wide * in_inner
    )
    in_projection = (float(D) ** 0.5 * row_scale * in_inner)[:, None]
    return (
        mixed.T,
        tokens_grad.T,
        wide_sums[:rank].T,
        narrow[:, :q_width],
        jnp.stack([wide_sums[rank : 2 * rank].T, wide_sums[2 * rank : 3 * rank].T]),
        jnp.stack([narrow[:, q_width : q_width + kv_width], narrow[:, q_width + kv_width :]]),
        output_down_gradient,
        wide_sums[3 * rank :],
        in_projection,
    )


def solution(mesh):
    torus = Mesh(mesh.devices.reshape(4, 4, 2, 2, 2), (*CTX, *TP))
    return jax.shard_map(
        on_device,
        mesh=torus,
        in_specs=(
            P(CTX, TP),
            P(CTX, TP),
            P(),
            P(),
            P(),
            P(),
            P(CTX, TP),
            P(CTX, TP),
            P(None, TP),
            P(None, CTX, TP),
            P(None, CTX, TP),
            P(None, None, TP),
            P(CTX, TP),
            P(CTX, TP),
            P(None, TP),
            P(),
            P(None, TP),
            P(),
            P(None, None, TP),
            P(TP, None),
            P(),
        ),
        out_specs=(
            P(CTX, TP),
            P(CTX, TP),
            P(),
            P(None, TP),
            P(),
            P(None, None, TP),
            P(TP, None),
            P(),
            P(CTX, None),
        ),
        check_vma=False,
    )
```

```python
import jax
import jax.numpy as jnp
from jax import lax
from jax.sharding import Mesh
from jax.sharding import PartitionSpec as P

D = 5376
HEAD_SIZE = 128
WINDOW_TOKENS = 1024
QBLOCK = 64
QGROUP = 256
CTX = ("y", "z", "xh")
TP = ("xl", "c")
NORMAL_FLOAT = (
    -1.0,
    -0.6961928009986877,
    -0.5250730514526367,
    -0.39491748809814453,
    -0.28444138169288635,
    -0.18477343022823334,
    -0.09105003625154495,
    0.0,
    0.07958029955625534,
    0.16093020141124725,
    0.24611230194568634,
    0.33791524171829224,
    0.44070982933044434,
    0.5626170039176941,
    0.7229568362236023,
    1.0,
)
EPSILON = 1e-06
ADAPTER_SCALE = 2.0
SCORE_SCALE = 168.0 ** (-0.5)
ROPE_BASE = 10000.0
CUT = 88
BF = jnp.bfloat16
F32 = jnp.float32


def swap(x, axis):
    return lax.ppermute(x, axis, [(0, 1), (1, 0)])


def ring(x, axis, by):
    n = lax.axis_size(axis)
    return lax.ppermute(x, axis, [(i, (i + by) % n) for i in range(n)])


def ring_pieces(v, axis):
    h = v.shape[0] // 16 * 8
    left = ring(v, axis, 1)
    right = ring(v, axis, -1)
    return [v, left, ring(left[:h], axis, 1), ring(right[h:], axis, -1), right]


def two_ways(near, far):
    a, axis_a, b, axis_b = *near, *far
    a = jnp.concatenate(ring_pieces(a, axis_a))
    b = jnp.concatenate(ring_pieces(b, axis_b))
    return ring_pieces(a, axis_b), ring_pieces(b, axis_a)


def after(arrays, *done):
    return lax.optimization_barrier((arrays, done))[0]


def shifted(x, by):
    n = lax.axis_size(CTX)
    return lax.ppermute(x, CTX, [(i, i + by) for i in range(n) if 0 <= i + by < n])


def dot_f32(a, b, ca, cb):
    return lax.dot_general(a, b, (((ca,), (cb,)), ((), ())), preferred_element_type=F32)


def dequantize(codes, scodes, second, row_start):
    height, width = codes.shape
    levels = jnp.zeros(codes.shape, F32)
    for level in range(16):
        levels = jnp.where(codes == level, F32(NORMAL_FLOAT[level]), levels)
    group_ids = (row_start + jnp.arange(height, dtype=jnp.int32)) // QGROUP
    group_list = jnp.arange(second.shape[0], dtype=jnp.int32)
    picker = (group_ids[:, None] == group_list[None, :]).astype(F32)
    second_rows = jnp.dot(picker, second, precision=lax.Precision.HIGHEST)
    absmax = second_rows * ((scodes.astype(F32) + 1.0) / 256.0)
    scaled = levels.reshape(height, width // QBLOCK, QBLOCK) * absmax[:, :, None]
    return scaled.reshape(height, width).astype(BF)


def rope_tables(positions):
    half = HEAD_SIZE // 2
    exponent = jnp.arange(half, dtype=F32) * (2.0 / HEAD_SIZE)
    frequency = jnp.power(F32(ROPE_BASE), -exponent)
    angle = positions.astype(F32)[:, None] * frequency[None, :]
    return (jnp.cos(angle), jnp.sin(angle))


def rotate(heads, cosine, sine):
    half = heads.shape[-1] // 2
    first = heads[..., :half]
    second = heads[..., half:]
    across = cosine[:, None, :]
    along = sine[:, None, :]
    return jnp.concatenate(
        [first * across - second * along, second * across + first * along], axis=-1
    )


def unrotate(grad, cosine, sine):
    return rotate(grad, cosine, -sine)


def head_norm(heads, gain):
    scale = lax.rsqrt(jnp.mean(heads * heads, axis=-1, keepdims=True) + EPSILON)
    return (heads * scale * gain, scale)


def head_norm_back(heads, scale, gain, grad):
    weighted = grad * gain
    inner = jnp.mean(weighted * heads, axis=-1, keepdims=True)
    return scale * weighted - scale**3 * heads * inner


def probabilities(q_rot, keys, query_pos, key_pos):
    count, q_heads, width = q_rot.shape
    kv_heads = keys.shape[1]
    grouped = q_rot.reshape(count, kv_heads, q_heads // kv_heads, width)
    scores = (
        jnp.einsum("tkgd,lkd->kgtl", grouped, keys, preferred_element_type=F32) * SCORE_SCALE
    )
    gap = query_pos[:, None] - key_pos[None, :]
    allowed = (gap >= 0) & (gap < WINDOW_TOKENS) & (key_pos[None, :] >= 0)
    weights = jnp.where(allowed, jnp.exp(scores), 0.0)
    return (weights / jnp.sum(weights, axis=-1, keepdims=True), grouped)


def attention_forward(q_rot, keys, values, query_pos, key_pos):
    count, q_heads, width = q_rot.shape
    probability, grouped = probabilities(q_rot, keys, query_pos, key_pos)
    prob_low = probability.astype(BF)
    mixed = jnp.einsum("kgtl,lkd->tkgd", prob_low, values, preferred_element_type=F32)
    return mixed.reshape(count, q_heads * width).astype(BF)


def attention_backward(q_rot, keys, values, output_gradient, query_pos, key_pos):
    count, q_heads, width = q_rot.shape
    kv_heads = keys.shape[1]
    probability, grouped = probabilities(q_rot, keys, query_pos, key_pos)
    prob_low = probability.astype(BF)
    grad_grouped = output_gradient.reshape(count, kv_heads, q_heads // kv_heads, width)
    grad_prob = jnp.einsum("tkgd,lkd->kgtl", grad_grouped, values, preferred_element_type=F32)
    grad_values = jnp.einsum("kgtl,tkgd->lkd", prob_low, grad_grouped, preferred_element_type=F32)
    inner = jnp.sum(probability * grad_prob, axis=-1, keepdims=True)
    grad_scores = (probability * (grad_prob - inner) * SCORE_SCALE).astype(BF)
    grad_query = jnp.einsum(
        "kgtl,lkd->tkgd", grad_scores, keys, preferred_element_type=F32
    ).reshape(count, q_heads, width)
    grad_keys = jnp.einsum("kgtl,tkgd->lkd", grad_scores, grouped, preferred_element_type=F32)
    return (grad_query, grad_keys, grad_values)


def gathered_pieces(own, xl, c):
    other = swap(own, "xl")
    pair = jnp.stack([jnp.where(xl == 0, own, other), jnp.where(xl == 0, other, own)])
    far = swap(pair, "c")
    return jnp.stack([jnp.where(c == 0, pair, far), jnp.where(c == 0, far, pair)], axis=1)


def on_device(
    tokens,
    out_grad,
    in_gain,
    query_gain,
    key_gain,
    post_gain,
    q_codes,
    q_scodes,
    q_second,
    kv_codes,
    kv_scodes,
    kv_second,
    o_codes,
    o_scodes,
    o_second,
    q_down,
    query_up,
    kv_down,
    key_value_up,
    output_down,
    output_up,
):
    count, share = tokens.shape
    y, z, xh = (lax.axis_index(a) for a in CTX)
    xl, c = (lax.axis_index(a) for a in TP)
    ctx_rank = lax.axis_index(CTX)
    column_start = lax.axis_index(TP) * share
    rows = q_codes.shape[0]
    row_start = ctx_rank * rows
    blocks = share // rows
    ny, nz = lax.axis_size("y"), lax.axis_size("z")
    q_width = query_up.shape[1]
    kv_width = key_value_up.shape[2]
    q_heads_here = q_width // HEAD_SIZE
    kv_heads_here = kv_width // HEAD_SIZE

    def turned(a, axis, at):
        n = a.shape[axis]
        return jnp.concatenate(
            [lax.dynamic_slice_in_dim(a, (at - r) % n, 1, axis) for r in range(n)], axis
        )

    def by_distance(a):
        return turned(turned(a, 0, y), 1, z)

    def parity(a, which):
        return lax.dynamic_index_in_dim(a.reshape(ny, nz, 2, rows, -1), which, 2, False)

    def joined(a, b):
        return (
            a.transpose(1, 0, 2, 3).reshape(-1, a.shape[-1]),
            b.reshape(-1, b.shape[-1]),
        )

    q_part = dequantize(q_codes, q_scodes, q_second, row_start)
    k_part = dequantize(kv_codes[0], kv_scodes[0], kv_second[0], row_start)
    v_part = dequantize(kv_codes[1], kv_scodes[1], kv_second[1], row_start)
    qkv_part = jnp.concatenate([q_part, k_part, v_part], axis=1)
    o_part = dequantize(o_codes, o_scodes, o_second, row_start)
    own_a, own_b = two_ways((qkv_part[:CUT], "y"), (qkv_part[CUT:], "z"))

    tokens_t = tokens.T
    mine = tokens_t.reshape(blocks // 2, 2, rows, count)
    keep = lax.dynamic_index_in_dim(mine, xh, 1, False)
    give = lax.dynamic_index_in_dim(mine, 1 - xh, 1, False)
    pair = jnp.concatenate([keep, swap(give, "xh")], axis=-1)
    wide = gathered_pieces(pair, xl, c).reshape(ny, nz, rows, 2 * count).astype(F32)
    partial_sum = jnp.sum(wide * wide, axis=(0, 1, 2))
    other_sum = swap(partial_sum.reshape(4, -1), "xh").reshape(-1)
    square_sum = partial_sum + jnp.roll(other_sum, count)
    pair_scale = lax.rsqrt(square_sum / D + EPSILON)
    normed = (wide * pair_scale * parity(in_gain, xh)).astype(BF)
    normed = by_distance(normed)
    normed_a, normed_b = joined(normed[:, :, :CUT], normed[:, :, CUT:])
    downs = jnp.concatenate([q_down, kv_down[0], kv_down[1]], axis=1)
    downs_parity = by_distance(parity(downs, xh))
    downs_a, downs_b = joined(downs_parity[:, :, :CUT], downs_parity[:, :, CUT:])

    def by_pieces(acts, pieces, total=None):
        at = 0
        for p in pieces:
            term = dot_f32(acts[at : at + p.shape[0]], p, 0, 0)
            total = term if total is None else total + term
            at += p.shape[0]
        return total

    low_pair = dot_f32(normed_a, downs_a, 0, 0) + dot_f32(normed_b, downs_b, 0, 0)
    low_sum = low_pair[:count] + swap(low_pair[count:], "xh")
    low = low_sum.astype(BF)
    rank = q_down.shape[1]
    query_lowrank, key_lowrank, value_lowrank = (
        low[:, i * rank : (i + 1) * rank] for i in range(3)
    )
    qkv_pair = by_pieces(normed_b, own_b, by_pieces(normed_a, own_a))
    far_kv = swap(qkv_pair[count:, q_width:].astype(BF), "xh")
    kv_sum = qkv_pair[:count, q_width:] + far_kv.astype(F32)
    far_q = swap(after(qkv_pair[count:, :q_width].astype(BF), far_kv), "xh")
    q_sum = qkv_pair[:count, :q_width] + far_q.astype(F32)
    row_scale = pair_scale[:count]

    key = kv_sum[:, :kv_width] + ADAPTER_SCALE * dot_f32(key_lowrank, key_value_up[0], 1, 0)
    value_total = kv_sum[:, kv_width:] + ADAPTER_SCALE * dot_f32(
        value_lowrank, key_value_up[1], 1, 0
    )
    value_rows = value_total.astype(BF)
    query_rows = q_sum + ADAPTER_SCALE * dot_f32(query_lowrank, query_up, 1, 0)

    query_pos = ctx_rank * count + jnp.arange(count, dtype=jnp.int32)
    key_pos = ctx_rank * count - WINDOW_TOKENS + jnp.arange(WINDOW_TOKENS + count, dtype=jnp.int32)
    cosine, sine = rope_tables(query_pos)
    key_head_rows = key.reshape(count, kv_heads_here, HEAD_SIZE)
    k_normed, k_scale = head_norm(key_head_rows, key_gain)
    k_rot = rotate(k_normed, cosine, sine).astype(BF)
    kv_rows = jnp.concatenate([k_rot.reshape(count, kv_width), value_rows], axis=1)
    steps = WINDOW_TOKENS // count
    window = jnp.concatenate([shifted(kv_rows, s) for s in range(steps, 0, -1)] + [kv_rows])
    window_keys = window[:, :kv_width].reshape(-1, kv_heads_here, HEAD_SIZE)
    window_values = window[:, kv_width:].reshape(-1, kv_heads_here, HEAD_SIZE)
    q_heads = query_rows.reshape(count, q_heads_here, HEAD_SIZE)
    q_normed, q_scale = head_norm(q_heads, query_gain)
    q_rot = rotate(q_normed, cosine, sine).astype(BF)

    o_other, qkv_other = swap(after((o_part, qkv_part), normed_a), "xh")
    o_own, o_other = after((o_part, o_other), qkv_pair)
    o_own, o_other = two_ways((o_own, "y"), (o_other, "z"))
    out_grad_t = out_grad.T
    out_grad_full = gathered_pieces(after(out_grad_t, far_q), xl, c)

    attended = attention_forward(q_rot, window_keys, window_values, query_pos, key_pos)

    qkv_other = after(qkv_other, o_own, o_other)
    other_a, other_b = two_ways((qkv_other[:CUT], "y"), (qkv_other[CUT:], "z"))
    low_out_part = dot_f32(attended, output_down, 1, 0).astype(BF)
    low_rows = low_out_part.T.astype(F32)

    def both_orders(a):
        own = by_distance(parity(a, xh)).transpose(1, 0, 2, 3).reshape(D // 2, -1)
        return own, by_distance(parity(a, 1 - xh)).reshape(D // 2, -1)

    ups = both_orders(output_up.T)
    post = both_orders(post_gain)
    cotangent = both_orders(out_grad_full.reshape(D, count))
    sums, low_total = [], None
    for j, pieces in enumerate((o_own, o_other)):
        part = jnp.concatenate([dot_f32(p, attended, 1, 1) for p in pieces])
        part = part + ADAPTER_SCALE * dot_f32(ups[j], low_out_part, 1, 1)
        part = part.reshape(2, share, count)
        keep = lax.dynamic_index_in_dim(part, c, 0, False)
        give = lax.dynamic_index_in_dim(part, 1 - c, 0, False)
        if j == 0:
            keep = jnp.concatenate([keep, low_rows])
            give = jnp.concatenate([give, low_rows])
        chip = (keep + swap(give.astype(BF), "c").astype(F32)).astype(BF)
        total = (chip.astype(F32) + swap(chip, "xl").astype(F32)).astype(BF)
        if j == 0:
            low_total = total[share:]
            total = total[:share]
        far = swap(total, "c")
        sums.append(jnp.concatenate([jnp.where(c == 0, total, far), jnp.where(c == 0, far, total)]))
    output_lowrank = low_total.T
    weighted = [g.astype(F32) * p for g, p in zip(cotangent, post)]
    wide_sums = [s.astype(F32) for s in sums]
    square_sum = sum(jnp.sum(s * s, axis=0) for s in wide_sums)
    out_scale = lax.rsqrt(square_sum / D + EPSILON)
    out_inner = sum(jnp.sum(w * s, axis=0) for w, s in zip(weighted, wide_sums)) / D
    grads = [
        (out_scale * w - out_scale**3 * s * out_inner).astype(BF)
        for w, s in zip(weighted, wide_sums)
    ]
    output_mixture = sum(dot_f32(g, u, 0, 0) for g, u in zip(grads, ups)).astype(BF)
    attended_gradient = ADAPTER_SCALE * dot_f32(output_mixture, output_down, 1, 1)
    for g, pieces in zip(grads, (o_own, o_other)):
        attended_gradient = by_pieces(g, pieces, attended_gradient)
    attended_gradient = attended_gradient.astype(BF)

    piece = lax.axis_index(TP)
    distance = (y - piece) % ny

    def home(own, other):
        halves = []
        for a in (own, other):
            a = lax.dynamic_index_in_dim(a, distance, 0, False)
            halves.append(turned(a, 0, z))
        first = jnp.where(xh == 0, halves[0], halves[1])
        second = jnp.where(xh == 0, halves[1], halves[0])
        return jnp.stack([first, second], axis=1).reshape(share, -1)

    blocked = (ny, nz, rows, count)

    def home_rows(arrays):
        return home(arrays[0].reshape(blocked).transpose(1, 0, 2, 3), arrays[1].reshape(blocked))

    out_mine = home_rows(sums).astype(F32)
    post_mine = lax.dynamic_slice_in_dim(post_gain, column_start, share, 0)[:, None]
    mixed = (tokens_t.astype(F32) + out_mine * out_scale * post_mine).astype(BF)
    grad_mine = home_rows(grads)
    output_up_gradient = ADAPTER_SCALE * dot_f32(output_lowrank, grad_mine, 0, 1)
    output_down_gradient = ADAPTER_SCALE * dot_f32(output_mixture, attended, 0, 0)
    query_grad, key_window_grad, value_window_grad = attention_backward(
        q_rot, window_keys, window_values, attended_gradient, query_pos, key_pos
    )
    window_grad = jnp.concatenate(
        [key_window_grad.reshape(-1, kv_width), value_window_grad.reshape(-1, kv_width)], axis=1
    )
    own = window_grad[WINDOW_TOKENS:]
    for s in range(steps, 0, -1):
        piece = window_grad[(steps - s) * count : (steps - s + 1) * count].astype(BF)
        own = own + shifted(piece, -s).astype(F32)
    q_norm_grad = unrotate(query_grad, cosine, sine)
    k_norm_grad = unrotate(own[:, :kv_width].reshape(count, kv_heads_here, HEAD_SIZE), cosine, sine)
    query_back = head_norm_back(q_heads, q_scale, query_gain, q_norm_grad)
    query_back = query_back.reshape(count, q_width).astype(BF)
    key_back = head_norm_back(key_head_rows, k_scale, key_gain, k_norm_grad)
    key_back = key_back.reshape(count, kv_width).astype(BF)
    value_back = own[:, kv_width:].astype(BF)

    back = jnp.concatenate([query_back, key_back, value_back], axis=1)

    def toward(ps):
        a = jnp.concatenate([dot_f32(p, back, 1, 1) for p in ps[0]])
        b = jnp.concatenate([dot_f32(p, back, 1, 1) for p in ps[1]])
        a = a.reshape(nz, ny, CUT, count).transpose(1, 0, 2, 3)
        return jnp.concatenate([a, b.reshape(ny, nz, rows - CUT, count)], axis=2)

    into = jnp.stack([toward((own_a, own_b)), toward((other_a, other_b))], axis=1)

    def for_piece(far_xl, far_c):
        p = (jnp.where(far_xl, 1 - xl, xl)) * 2 + jnp.where(far_c, 1 - c, c)
        return lax.dynamic_index_in_dim(into, (y - p) % ny, 0, False)

    give = jnp.stack([for_piece(True, True), for_piece(False, True)]).astype(BF)
    arrived = swap(give, "c").astype(F32)
    to_chip = for_piece(True, False) + arrived[0]
    into_mine = for_piece(False, False) + arrived[1]
    far_into = swap(to_chip.astype(BF), "xl")
    into_mine = into_mine + far_into.astype(F32)
    halves = turned(into_mine, 1, z)
    first = jnp.where(xh == 0, halves[0], halves[1])
    second = jnp.where(xh == 0, halves[1], halves[0])
    into_mine = jnp.stack([first, second], axis=1).reshape(share, count)
    inner_part = (
        jnp.sum(query_back.astype(F32) * query_rows, axis=1)
        + jnp.sum(key_back.astype(F32) * key, axis=1)
        + jnp.sum(value_back.astype(F32) * value_total, axis=1)
    )
    small = jnp.concatenate(
        [
            dot_f32(query_up, query_back, 1, 1),
            dot_f32(key_value_up[0], key_back, 1, 1),
            dot_f32(key_value_up[1], value_back, 1, 1),
            inner_part[None],
            jnp.zeros((7, count), F32),
        ]
    )
    small = jnp.sum(lax.all_gather(after(small, to_chip), TP), axis=0)
    mixes = small[: 3 * rank].astype(BF)
    in_inner = small[3 * rank] / (row_scale * D)

    in_gain_mine = lax.dynamic_slice_in_dim(in_gain, column_start, share, 0)[:, None]
    tokens_wide = tokens_t.astype(F32)
    normed_mine = (tokens_wide * row_scale * in_gain_mine).astype(BF)
    down_gradients = ADAPTER_SCALE * dot_f32(mixes, normed_mine, 1, 1)
    up_gradients = ADAPTER_SCALE * jnp.concatenate(
        [
            dot_f32(query_lowrank, query_back, 0, 0),
            dot_f32(key_lowrank, key_back, 0, 0),
            dot_f32(value_lowrank, value_back, 0, 0),
        ],
        axis=1,
    )
    everything = jnp.concatenate(
        [
            down_gradients.reshape(-1),
            output_up_gradient.reshape(-1),
            up_gradients.reshape(-1),
            output_down_gradient.reshape(-1),
        ]
    )
    devices = lax.axis_size(CTX)
    parts = everything.reshape(devices, -1, 128)
    arrived = lax.all_to_all(parts, CTX, 0, 0, tiled=True)
    chunk = jnp.sum(arrived, axis=0)
    spread = jnp.broadcast_to(chunk[None], (devices, *chunk.shape))
    summed = lax.all_to_all(spread, CTX, 0, 0, tiled=True).reshape(-1)
    cut = 4 * rank * share
    adapter_sums = gathered_pieces(summed[:cut].reshape(4 * rank, share), xl, c)
    adapter_sums = jnp.moveaxis(adapter_sums.reshape(4, 4 * rank, share), 0, 1).reshape(4 * rank, D)
    narrow = summed[cut : cut + up_gradients.size].reshape(up_gradients.shape)
    output_down_gradient = summed[cut + up_gradients.size :].reshape(rank, q_width).T

    downs_mine = lax.dynamic_slice_in_dim(downs, column_start, share, 0)
    normalized_gradient = into_mine + ADAPTER_SCALE * dot_f32(downs_mine, mixes, 1, 0)
    weighted_in = normalized_gradient * in_gain_mine
    tokens_grad = (
        out_grad_t.astype(F32)
        + row_scale * weighted_in
        - row_scale**3 * tokens_wide * in_inner
    )
    in_projection = (float(D) ** 0.5 * row_scale * in_inner)[:, None]
    return (
        mixed.T,
        tokens_grad.T,
        adapter_sums[:rank].T,
        narrow[:, :q_width],
        jnp.stack([adapter_sums[rank : 2 * rank].T, adapter_sums[2 * rank : 3 * rank].T]),
        jnp.stack([narrow[:, q_width : q_width + kv_width], narrow[:, q_width + kv_width :]]),
        output_down_gradient,
        adapter_sums[3 * rank :],
        in_projection,
    )


def solution(mesh):
    torus = Mesh(mesh.devices.reshape(4, 4, 2, 2, 2), (*CTX, *TP))
    return jax.shard_map(
        on_device,
        mesh=torus,
        in_specs=(
            P(CTX, TP),
            P(CTX, TP),
            P(),
            P(),
            P(),
            P(),
            P(CTX, TP),
            P(CTX, TP),
            P(None, TP),
            P(None, CTX, TP),
            P(None, CTX, TP),
            P(None, None, TP),
            P(CTX, TP),
            P(CTX, TP),
            P(None, TP),
            P(),
            P(None, TP),
            P(),
            P(None, None, TP),
            P(TP, None),
            P(),
        ),
        out_specs=(
            P(CTX, TP),
            P(CTX, TP),
            P(),
            P(None, TP),
            P(),
            P(None, None, TP),
            P(TP, None),
            P(),
            P(CTX, None),
        ),
        check_vma=False,
    )
```

```python
import jax
import jax.numpy as jnp
from jax import lax
from jax.experimental import pallas as pl
from jax.experimental.pallas import tpu as pltpu
from jax.sharding import Mesh
from jax.sharding import PartitionSpec as P

D = 5376
HEAD_SIZE = 128
WINDOW_TOKENS = 1024
QBLOCK = 64
QGROUP = 256
CTX = ("y", "z", "xh")
TP = ("xl", "c")
NORMAL_FLOAT = (
    -1.0,
    -0.6961928009986877,
    -0.5250730514526367,
    -0.39491748809814453,
    -0.28444138169288635,
    -0.18477343022823334,
    -0.09105003625154495,
    0.0,
    0.07958029955625534,
    0.16093020141124725,
    0.24611230194568634,
    0.33791524171829224,
    0.44070982933044434,
    0.5626170039176941,
    0.7229568362236023,
    1.0,
)
EPSILON = 1e-06
ADAPTER_SCALE = 2.0
SCORE_SCALE = 168.0 ** (-0.5)
ROPE_BASE = 10000.0
BF = jnp.bfloat16
F32 = jnp.float32


def swap(x, axis):
    return lax.ppermute(x, axis, [(0, 1), (1, 0)])


def after(arrays, *done):
    return lax.optimization_barrier((arrays, done))[0]


def shifted(x, by):
    n = lax.axis_size(CTX)
    return lax.ppermute(x, CTX, [(i, i + by) for i in range(n) if 0 <= i + by < n])


def dot_f32(a, b, ca, cb):
    return lax.dot_general(a, b, (((ca,), (cb,)), ((), ())), preferred_element_type=F32)


def levels_of(codes):
    bits = [(codes & (1 << b)) != 0 for b in range(4)]
    table = [F32(v) for v in NORMAL_FLOAT]
    for bit in bits:
        table = [jnp.where(bit, high, low) for low, high in zip(table[::2], table[1::2])]
    return table[0]


def dequantize_kernel(place, q_ref, kv_ref, o_ref, scodes_ref, second_ref, qkv_out, o_out):
    height = q_ref.shape[0]
    first = second_ref[pl.ds(place[0], 1), :]
    last = second_ref[pl.ds(place[1], 1), :]
    row = lax.broadcasted_iota(jnp.int32, scodes_ref.shape, 0)
    second = jnp.where(row < place[2], first, last)
    absmax = second * ((scodes_ref[...].astype(F32) + 1.0) / 256.0)
    lane = lax.broadcasted_iota(jnp.int32, (height, 128), 1)

    def scaled(codes, block):
        scale = jnp.where(lane < QBLOCK, absmax[:, block : block + 1], absmax[:, block + 1 : block + 2])
        return (levels_of(codes) * scale).astype(BF)

    q_width, kv_width = q_ref.shape[1], kv_ref.shape[2]
    for j in range(q_width // 128):
        at = slice(j * 128, (j + 1) * 128)
        qkv_out[:, at] = scaled(q_ref[:, at], 2 * j)
        o_out[:, at] = scaled(o_ref[:, at], (q_width + 2 * kv_width) // QBLOCK + 2 * j)
    for j in range(kv_width // 128):
        for part in range(2):
            to = q_width + (2 * j + part) * 128
            block = (q_width + part * kv_width) // QBLOCK + 2 * j
            qkv_out[:, to : to + 128] = scaled(kv_ref[part, :, j * 128 : (j + 1) * 128], block)


def dequantize(q_codes, kv_codes, o_codes, scodes, second, row_start):
    height, q_width = q_codes.shape
    kv_width = kv_codes.shape[2]
    group = row_start // QGROUP
    last = jnp.minimum(group + 1, second.shape[0] - 1)
    place = jnp.stack([group, last, (group + 1) * QGROUP - row_start]).astype(jnp.int32)
    return pl.pallas_call(
        dequantize_kernel,
        out_shape=(
            jax.ShapeDtypeStruct((height, q_width + 2 * kv_width), BF),
            jax.ShapeDtypeStruct((height, q_width), BF),
        ),
        in_specs=[pl.BlockSpec(memory_space=pltpu.SMEM)]
        + [pl.BlockSpec(memory_space=pltpu.VMEM)] * 5,
        name="dequantize",
    )(place, q_codes, kv_codes, o_codes, scodes, second)


def rope_tables(positions):
    half = HEAD_SIZE // 2
    exponent = jnp.arange(half, dtype=F32) * (2.0 / HEAD_SIZE)
    frequency = jnp.power(F32(ROPE_BASE), -exponent)
    angle = positions.astype(F32)[:, None] * frequency[None, :]
    return (jnp.cos(angle), jnp.sin(angle))


def rotate(heads, cosine, sine):
    half = heads.shape[-1] // 2
    first = heads[..., :half]
    second = heads[..., half:]
    across = cosine[:, None, :]
    along = sine[:, None, :]
    return jnp.concatenate(
        [first * across - second * along, second * across + first * along], axis=-1
    )


def unrotate(grad, cosine, sine):
    return rotate(grad, cosine, -sine)


def head_norm(heads, gain):
    scale = lax.rsqrt(jnp.mean(heads * heads, axis=-1, keepdims=True) + EPSILON)
    return (heads * scale * gain, scale)


def head_norm_back(heads, scale, gain, grad):
    weighted = grad * gain
    inner = jnp.mean(weighted * heads, axis=-1, keepdims=True)
    return scale * weighted - scale**3 * heads * inner


def mxu(a, b, ca, cb):
    return lax.dot_general(a, b, (((ca,), (cb,)), ((), ())), preferred_element_type=F32)


def side_by_side(ref):
    return jnp.concatenate([ref[:HEAD_SIZE, :], ref[HEAD_SIZE:, :]], axis=1)


def weights_of(first_key, blocks, queries):
    weights, total = [], None
    for b, block in enumerate(blocks):
        keys, count = block.shape[0], queries.shape[1] // 2
        scores = mxu(block[:, :HEAD_SIZE], queries, 1, 0) * SCORE_SCALE
        e = jnp.exp(scores)
        key = lax.broadcasted_iota(jnp.int32, e.shape, 0)
        query = lax.broadcasted_iota(jnp.int32, e.shape, 1) % count
        if b == 0:
            e = jnp.where((key > query) & (first_key <= 0), e, 0.0)
        elif b == len(blocks) - 1:
            e = jnp.where(key <= query, e, 0.0)
        else:
            e = jnp.where(key + b * keys >= first_key, e, 0.0)
        part = jnp.sum(e, axis=0, keepdims=True)
        total = part if total is None else total + part
        weights.append(e)
    return weights, total


def forward_kernel(first_key, q_ref, *refs):
    blocks, out = refs[:-1], refs[-1]
    queries = side_by_side(q_ref)
    count = q_ref.shape[1]
    weights, total = weights_of(first_key[0], blocks, queries)
    inverse = 1.0 / total
    mixed = None
    for block, e in zip(blocks, weights):
        term = mxu(block[:, HEAD_SIZE:], (e * inverse).astype(BF), 0, 0)
        mixed = term if mixed is None else mixed + term
    mixed = mixed.astype(BF)
    out[:HEAD_SIZE, :] = mixed[:, :count]
    out[HEAD_SIZE:, :] = mixed[:, count:]


def backward_kernel(first_key, q_ref, grad_ref, *refs):
    n = (len(refs) - 1) // 2
    blocks, q_out, outs = refs[:n], refs[n], refs[n + 1 :]
    queries, grads = side_by_side(q_ref), side_by_side(grad_ref)
    count = q_ref.shape[1]
    weights, total = weights_of(first_key[0], blocks, queries)
    inverse = 1.0 / total
    inner, from_values = None, []
    for block, e in zip(blocks, weights):
        g = mxu(block[:, HEAD_SIZE:], grads, 1, 0)
        part = jnp.sum(e * inverse * g, axis=0, keepdims=True)
        inner = part if inner is None else inner + part
        from_values.append(g)
    q_grad = None
    for block, e, g, out in zip(blocks, weights, from_values, outs):
        p = e * inverse
        score_grad = (p * (g - inner) * SCORE_SCALE).astype(BF)
        out[:, HEAD_SIZE:] = mxu(p.astype(BF), grads, 1, 1).astype(out.dtype)
        out[:, :HEAD_SIZE] = mxu(score_grad, queries, 1, 1).astype(out.dtype)
        term = mxu(block[:, :HEAD_SIZE], score_grad, 0, 0)
        q_grad = term if q_grad is None else q_grad + term
    q_out[:HEAD_SIZE, :] = q_grad[:, :count]
    q_out[HEAD_SIZE:, :] = q_grad[:, count:]


def attention_call(kernel, first_key, transposed, blocks, outs, name):
    count = transposed[0].shape[1]
    row = pl.BlockSpec((2 * HEAD_SIZE, count), lambda g: (g, 0))
    column = pl.BlockSpec((count, 2 * HEAD_SIZE), lambda g: (0, g))
    kinds = [row if o.shape[1] == count else column for o in outs]
    return pl.pallas_call(
        kernel,
        grid=(blocks[0].shape[1] // (2 * HEAD_SIZE),),
        out_shape=outs,
        in_specs=[pl.BlockSpec(memory_space=pltpu.SMEM)]
        + [row] * len(transposed)
        + [column] * len(blocks),
        out_specs=kinds,
        name=name,
    )(first_key, *transposed, *blocks)


def gathered_pieces(own, xl, c):
    other = swap(own, "xl")
    pair = jnp.stack([jnp.where(xl == 0, own, other), jnp.where(xl == 0, other, own)])
    far = swap(pair, "c")
    return jnp.stack([jnp.where(c == 0, pair, far), jnp.where(c == 0, far, pair)], axis=1)


def on_device(
    tokens,
    out_grad,
    in_gain,
    query_gain,
    key_gain,
    post_gain,
    q_codes,
    q_scodes,
    q_second,
    kv_codes,
    kv_scodes,
    kv_second,
    o_codes,
    o_scodes,
    o_second,
    q_down,
    query_up,
    kv_down,
    key_value_up,
    output_down,
    output_up,
):
    count, share = tokens.shape
    y, z, xh = (lax.axis_index(a) for a in CTX)
    xl, c = (lax.axis_index(a) for a in TP)
    ctx_rank = lax.axis_index(CTX)
    column_start = lax.axis_index(TP) * share
    rows = q_codes.shape[0]
    row_start = ctx_rank * rows
    blocks = share // rows
    ny, nz = lax.axis_size("y"), lax.axis_size("z")
    q_width = query_up.shape[1]
    kv_width = key_value_up.shape[2]
    q_heads_here = q_width // HEAD_SIZE
    kv_heads_here = kv_width // HEAD_SIZE

    scodes = jnp.concatenate([q_scodes, kv_scodes[0], kv_scodes[1], o_scodes], axis=1)
    second = jnp.concatenate([q_second, kv_second[0], kv_second[1], o_second], axis=1)
    qkv_part, o_part = dequantize(q_codes, kv_codes, o_codes, scodes, second, row_start)
    own_matrix = lax.all_gather(qkv_part, ("y", "z"), axis=0, tiled=True)

    tokens_t = tokens.T
    mine = tokens_t.reshape(blocks // 2, 2, rows, count)
    keep = lax.dynamic_index_in_dim(mine, xh, 1, False)
    give = lax.dynamic_index_in_dim(mine, 1 - xh, 1, False)
    pair = jnp.concatenate([keep, swap(give, "xh")], axis=-1)
    wide = gathered_pieces(pair, xl, c).reshape(ny, nz, rows, 2 * count).astype(F32)
    partial_sum = jnp.sum(wide * wide, axis=(0, 1, 2))
    other_sum = swap(partial_sum.reshape(4, -1), "xh").reshape(-1)
    square_sum = partial_sum + jnp.roll(other_sum, count)
    pair_scale = lax.rsqrt(square_sum / D + EPSILON)
    def parity(a, which):
        return lax.dynamic_index_in_dim(a.reshape(ny, nz, 2, rows, -1), which, 2, False)

    normed = (wide * pair_scale * parity(in_gain, xh)).astype(BF).reshape(D // 2, -1)
    downs = jnp.concatenate([q_down, kv_down[0], kv_down[1]], axis=1)
    downs_parity = parity(downs, xh).reshape(D // 2, -1)
    low_pair = dot_f32(normed, downs_parity, 0, 0)
    low_sum = low_pair[:count] + swap(low_pair[count:], "xh")
    low = low_sum.astype(BF)
    rank = q_down.shape[1]
    query_lowrank, key_lowrank, value_lowrank = (
        low[:, i * rank : (i + 1) * rank] for i in range(3)
    )
    row_scale = pair_scale[:count]
    qkv_pair = dot_f32(normed, own_matrix, 0, 0)
    far_kv = swap(qkv_pair[count:, q_width:].astype(BF), "xh")
    kv_sum = qkv_pair[:count, q_width:] + far_kv.astype(F32)
    far_q = swap(after(qkv_pair[count:, :q_width].astype(BF), far_kv), "xh")
    q_sum = qkv_pair[:count, :q_width] + far_q.astype(F32)

    def of_heads(both, which):
        return both.reshape(-1, kv_heads_here, 2, HEAD_SIZE)[:, :, which].reshape(-1, kv_width)

    key = of_heads(kv_sum, 0) + ADAPTER_SCALE * dot_f32(key_lowrank, key_value_up[0], 1, 0)
    value_total = of_heads(kv_sum, 1) + ADAPTER_SCALE * dot_f32(
        value_lowrank, key_value_up[1], 1, 0
    )
    value_rows = value_total.astype(BF)
    query_rows = q_sum + ADAPTER_SCALE * dot_f32(query_lowrank, query_up, 1, 0)

    query_pos = ctx_rank * count + jnp.arange(count, dtype=jnp.int32)
    cosine, sine = rope_tables(query_pos)
    key_head_rows = key.reshape(count, kv_heads_here, HEAD_SIZE)
    k_normed, k_scale = head_norm(key_head_rows, key_gain)
    k_rot = rotate(k_normed, cosine, sine).astype(BF)
    kv_rows = jnp.stack([k_rot, value_rows.reshape(k_rot.shape)], axis=2).reshape(count, -1)
    steps = WINDOW_TOKENS // count
    window = [shifted(kv_rows, s) for s in range(steps, 0, -1)] + [kv_rows]
    first_key = (WINDOW_TOKENS - ctx_rank * count).astype(jnp.int32).reshape(1)
    q_heads = query_rows.reshape(count, q_heads_here, HEAD_SIZE)
    q_normed, q_scale = head_norm(q_heads, query_gain)
    q_rot = rotate(q_normed, cosine, sine).astype(BF)

    q_turned = q_rot.reshape(count, q_width).T

    o_swapped, qkv_other = swap(after((o_part, qkv_part), normed), "xh")
    o_both = jnp.concatenate(
        [jnp.where(xh == 0, o_part, o_swapped), jnp.where(xh == 0, o_swapped, o_part)]
    )
    output_matrix = lax.all_gather(after(o_both, own_matrix), ("y", "z"), axis=0, tiled=True)
    other_matrix = lax.all_gather(after(qkv_other, output_matrix), ("y", "z"), axis=0, tiled=True)
    out_grad_t = out_grad.T
    out_grad_full = gathered_pieces(after(out_grad_t, far_q), xl, c)

    (attended,) = attention_call(
        forward_kernel,
        first_key,
        [q_turned],
        window,
        [jax.ShapeDtypeStruct((q_width, count), BF)],
        "attention_forward",
    )

    low_out_part = dot_f32(attended, output_down, 0, 0).astype(BF)
    out_rows = output_matrix.reshape(2, 2 * share, q_width)
    up_rows = output_up.T.reshape(2, 2 * share, rank)
    low_rows = low_out_part.T.astype(F32)
    sums, low_total = [], None
    for j in range(2):
        part = dot_f32(out_rows[j], attended, 1, 0) + ADAPTER_SCALE * dot_f32(
            up_rows[j], low_out_part, 1, 1
        )
        part = part.reshape(2, share, count)
        keep = lax.dynamic_index_in_dim(part, c, 0, False)
        give = lax.dynamic_index_in_dim(part, 1 - c, 0, False)
        if j == 0:
            keep = jnp.concatenate([keep, low_rows])
            give = jnp.concatenate([give, low_rows])
        chip = (keep + swap(give.astype(BF), "c").astype(F32)).astype(BF)
        total = (chip.astype(F32) + swap(chip, "xl").astype(F32)).astype(BF)
        if j == 0:
            low_total = total[share:]
            total = total[:share]
        far = swap(total, "c")
        sums.append(jnp.stack([jnp.where(c == 0, total, far), jnp.where(c == 0, far, total)]))
    out_total = jnp.stack(sums).astype(F32)
    output_lowrank = low_total.T
    gain_full = post_gain.reshape(2, 2, share, 1)
    weighted_out = out_grad_full.astype(F32) * gain_full
    out_scale = lax.rsqrt(jnp.sum(out_total * out_total, axis=(0, 1, 2)) / D + EPSILON)
    out_inner = jnp.sum(weighted_out * out_total, axis=(0, 1, 2)) / D
    grad_full = (out_scale * weighted_out - out_scale**3 * out_total * out_inner).astype(BF)
    output_gradient = grad_full.reshape(D, count)
    out_mine = lax.dynamic_slice_in_dim(out_total.reshape(D, count), column_start, share, 0)
    post_mine = lax.dynamic_slice_in_dim(post_gain, column_start, share, 0)[:, None]
    mixed = (tokens_t.astype(F32) + out_mine * out_scale * post_mine).astype(BF)

    output_mixture = dot_f32(output_gradient, output_up, 0, 1).astype(BF)
    grad_mine = lax.dynamic_slice_in_dim(output_gradient, column_start, share, 0)
    output_up_gradient = ADAPTER_SCALE * dot_f32(output_lowrank, grad_mine, 0, 1)
    output_down_gradient = ADAPTER_SCALE * dot_f32(output_mixture, attended, 0, 1)
    attended_gradient = (
        dot_f32(output_matrix, output_gradient, 0, 0)
        + ADAPTER_SCALE * dot_f32(output_down, output_mixture, 1, 1)
    ).astype(BF)
    query_grad, *window_grad = attention_call(
        backward_kernel,
        first_key,
        [q_turned, attended_gradient],
        window,
        [jax.ShapeDtypeStruct((q_width, count), F32)]
        + [jax.ShapeDtypeStruct((count, 2 * kv_width), BF)] * steps
        + [jax.ShapeDtypeStruct((count, 2 * kv_width), F32)],
        "attention_backward",
    )
    own = window_grad[steps]
    for s in range(steps, 0, -1):
        own = own + shifted(window_grad[steps - s], -s).astype(F32)
    query_grad = query_grad.T.reshape(count, q_heads_here, HEAD_SIZE)
    q_norm_grad = unrotate(query_grad, cosine, sine)
    k_norm_grad = unrotate(of_heads(own, 0).reshape(count, kv_heads_here, HEAD_SIZE), cosine, sine)
    query_back = head_norm_back(q_heads, q_scale, query_gain, q_norm_grad)
    query_back = query_back.reshape(count, q_width).astype(BF)
    key_back = head_norm_back(key_head_rows, k_scale, key_gain, k_norm_grad)
    key_back = key_back.reshape(count, kv_width).astype(BF)
    value_back = of_heads(own, 1).astype(BF)

    heads = (count, kv_heads_here, HEAD_SIZE)
    kv_back = jnp.stack([key_back.reshape(heads), value_back.reshape(heads)], axis=2)
    back = jnp.concatenate([query_back, kv_back.reshape(count, -1)], axis=1)
    into = [
        dot_f32(w, back, 1, 1).reshape(2, 2, share // 2, count) for w in (own_matrix, other_matrix)
    ]

    def piece(a, far_xl, far_c):
        a = lax.dynamic_index_in_dim(a, 1 - xl if far_xl else xl, 0, False)
        return lax.dynamic_index_in_dim(a, 1 - c if far_c else c, 0, False)

    give = [
        jnp.concatenate([piece(a, far, True) for a in into]).astype(BF) for far in (True, False)
    ]
    arrived = [swap(g, "c").astype(F32) for g in give]
    to_chip = jnp.concatenate([piece(a, True, False) for a in into]) + arrived[0]
    far_into = swap(to_chip.astype(BF), "xl")
    into_mine = jnp.concatenate([piece(a, False, False) for a in into]) + arrived[1]
    into_mine = into_mine + far_into.astype(F32)
    halves = into_mine.reshape(2, nz, rows, count)
    first = jnp.where(xh == 0, halves[0], halves[1])
    last = jnp.where(xh == 0, halves[1], halves[0])
    into_mine = jnp.stack([first, last], axis=1).reshape(share, count)

    inner_part = (
        jnp.sum(query_back.astype(F32) * query_rows, axis=1)
        + jnp.sum(key_back.astype(F32) * key, axis=1)
        + jnp.sum(value_back.astype(F32) * value_total, axis=1)
    )
    small = jnp.concatenate(
        [
            dot_f32(query_up, query_back, 1, 1),
            dot_f32(key_value_up[0], key_back, 1, 1),
            dot_f32(key_value_up[1], value_back, 1, 1),
            inner_part[None],
            jnp.zeros((7, count), F32),
        ]
    )
    small = jnp.sum(lax.all_gather(after(small, to_chip), TP), axis=0)
    mixes = small[: 3 * rank].astype(BF)
    in_inner = small[3 * rank] / (row_scale * D)

    in_gain_mine = lax.dynamic_slice_in_dim(in_gain, column_start, share, 0)[:, None]
    tokens_wide = tokens_t.astype(F32)
    normed_mine = (tokens_wide * row_scale * in_gain_mine).astype(BF)
    down_gradients = ADAPTER_SCALE * dot_f32(mixes, normed_mine, 1, 1)
    up_gradients = ADAPTER_SCALE * jnp.concatenate(
        [
            dot_f32(query_lowrank, query_back, 0, 0),
            dot_f32(key_lowrank, key_back, 0, 0),
            dot_f32(value_lowrank, value_back, 0, 0),
        ],
        axis=1,
    )
    everything = jnp.concatenate(
        [
            down_gradients.reshape(-1),
            output_up_gradient.reshape(-1),
            up_gradients.reshape(-1),
            output_down_gradient.reshape(-1),
        ]
    )
    devices = lax.axis_size(CTX)
    parts = everything.reshape(devices, -1, 128)
    arrived = lax.all_to_all(parts, CTX, 0, 0, tiled=True)
    chunk = jnp.sum(arrived, axis=0)
    spread = jnp.broadcast_to(chunk[None], (devices, *chunk.shape))
    summed = lax.all_to_all(spread, CTX, 0, 0, tiled=True).reshape(-1)
    cut = 4 * rank * share
    wide_sums = gathered_pieces(summed[:cut].reshape(4 * rank, share), xl, c)
    wide_sums = jnp.moveaxis(wide_sums.reshape(4, 4 * rank, share), 0, 1).reshape(4 * rank, D)
    narrow = summed[cut : cut + up_gradients.size].reshape(up_gradients.shape)
    output_down_gradient = summed[cut + up_gradients.size :].reshape(rank, q_width).T

    downs_mine = lax.dynamic_slice_in_dim(downs, column_start, share, 0)
    normalized_gradient = into_mine + ADAPTER_SCALE * dot_f32(downs_mine, mixes, 1, 0)
    weighted_in = normalized_gradient * in_gain_mine
    tokens_grad = (
        out_grad_t.astype(F32)
        + row_scale * weighted_in
        - row_scale**3 * tokens_wide * in_inner
    )
    in_projection = (float(D) ** 0.5 * row_scale * in_inner)[:, None]
    return (
        mixed.T,
        tokens_grad.T,
        wide_sums[:rank].T,
        narrow[:, :q_width],
        jnp.stack([wide_sums[rank : 2 * rank].T, wide_sums[2 * rank : 3 * rank].T]),
        jnp.stack([narrow[:, q_width : q_width + kv_width], narrow[:, q_width + kv_width :]]),
        output_down_gradient,
        wide_sums[3 * rank :],
        in_projection,
    )


def solution(mesh):
    torus = Mesh(mesh.devices.reshape(4, 4, 2, 2, 2), (*CTX, *TP))
    return jax.shard_map(
        on_device,
        mesh=torus,
        in_specs=(
            P(CTX, TP),
            P(CTX, TP),
            P(),
            P(),
            P(),
            P(),
            P(CTX, TP),
            P(CTX, TP),
            P(None, TP),
            P(None, CTX, TP),
            P(None, CTX, TP),
            P(None, None, TP),
            P(CTX, TP),
            P(CTX, TP),
            P(None, TP),
            P(),
            P(None, TP),
            P(),
            P(None, None, TP),
            P(TP, None),
            P(),
        ),
        out_specs=(
            P(CTX, TP),
            P(CTX, TP),
            P(),
            P(None, TP),
            P(),
            P(None, None, TP),
            P(TP, None),
            P(),
            P(CTX, None),
        ),
        check_vma=False,
    )
```

```python
import jax
import jax.numpy as jnp
from jax import lax
from jax.experimental import pallas as pl
from jax.experimental.pallas import tpu as pltpu
from jax.sharding import Mesh
from jax.sharding import PartitionSpec as P

D = 5376
HEAD_SIZE = 128
WINDOW_TOKENS = 1024
QBLOCK = 64
QGROUP = 256
CTX = ("y", "z", "xh")
TP = ("xl", "c")
NORMAL_FLOAT = (
    -1.0,
    -0.6961928009986877,
    -0.5250730514526367,
    -0.39491748809814453,
    -0.28444138169288635,
    -0.18477343022823334,
    -0.09105003625154495,
    0.0,
    0.07958029955625534,
    0.16093020141124725,
    0.24611230194568634,
    0.33791524171829224,
    0.44070982933044434,
    0.5626170039176941,
    0.7229568362236023,
    1.0,
)
EPSILON = 1e-06
ADAPTER_SCALE = 2.0
SCORE_SCALE = 168.0 ** (-0.5)
ROPE_BASE = 10000.0
BF = jnp.bfloat16
F32 = jnp.float32


def swap(x, axis):
    return lax.ppermute(x, axis, [(0, 1), (1, 0)])


def after(arrays, *done):
    return lax.optimization_barrier((arrays, done))[0]


def shifted(x, by):
    n = lax.axis_size(CTX)
    return lax.ppermute(x, CTX, [(i, i + by) for i in range(n) if 0 <= i + by < n])


def dot_f32(a, b, ca, cb):
    return lax.dot_general(a, b, (((ca,), (cb,)), ((), ())), preferred_element_type=F32)


def levels_of(codes):
    bits = [(codes & (1 << b)) != 0 for b in range(4)]
    table = [F32(v) for v in NORMAL_FLOAT]
    for bit in bits:
        table = [jnp.where(bit, high, low) for low, high in zip(table[::2], table[1::2])]
    return table[0]


def scales_of(place, scodes, second):
    group = lax.broadcasted_iota(jnp.int32, second.shape, 1)
    first = jnp.sum(jnp.where(group == place[0], second, 0.0), axis=1, keepdims=True)
    last = jnp.sum(jnp.where(group == place[1], second, 0.0), axis=1, keepdims=True)
    row = lax.broadcasted_iota(jnp.int32, scodes.shape, 1)
    return jnp.where(row < place[2], first, last) * ((scodes.astype(F32) + 1.0) / 256.0)


def dequantize_kernel(place, q_ref, kv_ref, o_ref, qs, kvs, os, q2, kv2, o2, qkv_out, o_out):
    height, q_width = q_ref.shape
    kv_width = kv_ref.shape[2]
    parts = [
        scales_of(place, qs[...], q2[...]),
        scales_of(place, kvs[0], kv2[0]),
        scales_of(place, kvs[1], kv2[1]),
        scales_of(place, os[...], o2[...]),
    ]
    parts = [
        p if p.shape[0] % 8 == 0 else jnp.concatenate([p, jnp.zeros((8 - p.shape[0] % 8, height), F32)])
        for p in parts
    ]
    absmax = jnp.concatenate(parts)
    starts = [sum(p.shape[0] for p in parts[:n]) for n in range(4)]
    absmax = absmax.T
    lane = lax.broadcasted_iota(jnp.int32, (height, 128), 1)

    def scaled(codes, block):
        scale = jnp.where(lane < QBLOCK, absmax[:, block : block + 1], absmax[:, block + 1 : block + 2])
        return (levels_of(codes) * scale).astype(BF)

    for j in range(q_width // 128):
        at = slice(j * 128, (j + 1) * 128)
        qkv_out[:, at] = scaled(q_ref[:, at], 2 * j)
        o_out[:, at] = scaled(o_ref[:, at], starts[3] + 2 * j)
    for j in range(kv_width // 128):
        for part in range(2):
            to = q_width + (2 * j + part) * 128
            codes = kv_ref[part, :, j * 128 : (j + 1) * 128]
            qkv_out[:, to : to + 128] = scaled(codes, starts[1 + part] + 2 * j)


def dequantize(codes, scales, row_start):
    q_codes, kv_codes, _ = codes
    height, q_width = q_codes.shape
    kv_width = kv_codes.shape[2]
    group = row_start // QGROUP
    last = jnp.minimum(group + 1, scales[3].shape[1] - 1)
    place = jnp.stack([group, last, (group + 1) * QGROUP - row_start]).astype(jnp.int32)
    return pl.pallas_call(
        dequantize_kernel,
        out_shape=(
            jax.ShapeDtypeStruct((height, q_width + 2 * kv_width), BF),
            jax.ShapeDtypeStruct((height, q_width), BF),
        ),
        in_specs=[pl.BlockSpec(memory_space=pltpu.SMEM)]
        + [pl.BlockSpec(memory_space=pltpu.VMEM)] * 9,
        name="dequantize",
    )(place, *codes, *scales)


def rope_tables(positions):
    half = HEAD_SIZE // 2
    exponent = jnp.arange(half, dtype=F32) * (2.0 / HEAD_SIZE)
    frequency = jnp.power(F32(ROPE_BASE), -exponent)
    angle = positions.astype(F32)[:, None] * frequency[None, :]
    return (jnp.cos(angle), jnp.sin(angle))


def rotate(heads, cosine, sine):
    half = heads.shape[-1] // 2
    first = heads[..., :half]
    second = heads[..., half:]
    across = cosine[:, None, :]
    along = sine[:, None, :]
    return jnp.concatenate(
        [first * across - second * along, second * across + first * along], axis=-1
    )


def unrotate(grad, cosine, sine):
    return rotate(grad, cosine, -sine)


def head_norm(heads, gain):
    scale = lax.rsqrt(jnp.mean(heads * heads, axis=-1, keepdims=True) + EPSILON)
    return (heads * scale * gain, scale)


def head_norm_back(heads, scale, gain, grad):
    weighted = grad * gain
    inner = jnp.mean(weighted * heads, axis=-1, keepdims=True)
    return scale * weighted - scale**3 * heads * inner


def mxu(a, b, ca, cb):
    return lax.dot_general(a, b, (((ca,), (cb,)), ((), ())), preferred_element_type=F32)


def side_by_side(ref):
    return jnp.concatenate([ref[:HEAD_SIZE, :], ref[HEAD_SIZE:, :]], axis=1)


def weights_of(first_key, blocks, queries):
    weights, total = [], None
    for b, block in enumerate(blocks):
        keys, count = block.shape[0], queries.shape[1] // 2
        scores = mxu(block[:, :HEAD_SIZE], queries, 1, 0) * SCORE_SCALE
        e = jnp.exp(scores)
        key = lax.broadcasted_iota(jnp.int32, e.shape, 0)
        query = lax.broadcasted_iota(jnp.int32, e.shape, 1) % count
        if b == 0:
            e = jnp.where((key > query) & (first_key <= 0), e, 0.0)
        elif b == len(blocks) - 1:
            e = jnp.where(key <= query, e, 0.0)
        else:
            e = jnp.where(key + b * keys >= first_key, e, 0.0)
        part = jnp.sum(e, axis=0, keepdims=True)
        total = part if total is None else total + part
        weights.append(e)
    return weights, total


def forward_kernel(first_key, q_ref, *refs):
    blocks, out = refs[:-1], refs[-1]
    queries = side_by_side(q_ref)
    count = q_ref.shape[1]
    weights, total = weights_of(first_key[0], blocks, queries)
    inverse = 1.0 / total
    mixed = None
    for block, e in zip(blocks, weights):
        term = mxu(block[:, HEAD_SIZE:], (e * inverse).astype(BF), 0, 0)
        mixed = term if mixed is None else mixed + term
    mixed = mixed.astype(BF)
    out[:HEAD_SIZE, :] = mixed[:, :count]
    out[HEAD_SIZE:, :] = mixed[:, count:]


def backward_kernel(first_key, q_ref, grad_ref, *refs):
    n = (len(refs) - 1) // 2
    blocks, q_out, outs = refs[:n], refs[n], refs[n + 1 :]
    queries, grads = side_by_side(q_ref), side_by_side(grad_ref)
    count = q_ref.shape[1]
    weights, total = weights_of(first_key[0], blocks, queries)
    inverse = 1.0 / total
    inner, from_values = None, []
    for block, e in zip(blocks, weights):
        g = mxu(block[:, HEAD_SIZE:], grads, 1, 0)
        part = jnp.sum(e * inverse * g, axis=0, keepdims=True)
        inner = part if inner is None else inner + part
        from_values.append(g)
    q_grad = None
    for block, e, g, out in zip(blocks, weights, from_values, outs):
        p = e * inverse
        score_grad = (p * (g - inner) * SCORE_SCALE).astype(BF)
        out[:, HEAD_SIZE:] = mxu(p.astype(BF), grads, 1, 1).astype(out.dtype)
        out[:, :HEAD_SIZE] = mxu(score_grad, queries, 1, 1).astype(out.dtype)
        term = mxu(block[:, :HEAD_SIZE], score_grad, 0, 0)
        q_grad = term if q_grad is None else q_grad + term
    q_out[:HEAD_SIZE, :] = q_grad[:, :count]
    q_out[HEAD_SIZE:, :] = q_grad[:, count:]


def attention_call(kernel, first_key, transposed, blocks, outs):
    count = transposed[0].shape[1]
    row = pl.BlockSpec((2 * HEAD_SIZE, count), lambda g: (g, 0))
    column = pl.BlockSpec((count, 2 * HEAD_SIZE), lambda g: (0, g))
    kinds = [row if o.shape[1] == count else column for o in outs]
    return pl.pallas_call(
        kernel,
        grid=(blocks[0].shape[1] // (2 * HEAD_SIZE),),
        out_shape=outs,
        in_specs=[pl.BlockSpec(memory_space=pltpu.SMEM)]
        + [row] * len(transposed)
        + [column] * len(blocks),
        out_specs=kinds,
    )(first_key, *transposed, *blocks)


def gathered_pieces(own, xl, c):
    other = swap(own, "xl")
    pair = jnp.stack([jnp.where(xl == 0, own, other), jnp.where(xl == 0, other, own)])
    far = swap(pair, "c")
    return jnp.stack([jnp.where(c == 0, pair, far), jnp.where(c == 0, far, pair)], axis=1)


def on_device(
    tokens,
    out_grad,
    in_gain,
    query_gain,
    key_gain,
    post_gain,
    q_codes,
    q_scodes,
    q_second,
    kv_codes,
    kv_scodes,
    kv_second,
    o_codes,
    o_scodes,
    o_second,
    q_down,
    query_up,
    kv_down,
    key_value_up,
    output_down,
    output_up,
):
    count, share = tokens.shape
    _, _, xh = (lax.axis_index(a) for a in CTX)
    xl, c = (lax.axis_index(a) for a in TP)
    ctx_rank = lax.axis_index(CTX)
    column_start = lax.axis_index(TP) * share
    rows = q_codes.shape[0]
    row_start = ctx_rank * rows
    blocks = share // rows
    ny, nz = lax.axis_size("y"), lax.axis_size("z")
    q_width = query_up.shape[1]
    kv_width = key_value_up.shape[2]
    q_heads_here = q_width // HEAD_SIZE
    kv_heads_here = kv_width // HEAD_SIZE

    turned = (0, 2, 1)
    scales = [q_scodes.T, kv_scodes.transpose(turned), o_scodes.T]
    scales += [q_second.T, kv_second.transpose(turned), o_second.T]
    qkv_part, o_part = dequantize([q_codes, kv_codes, o_codes], scales, row_start)
    own_matrix = lax.all_gather(qkv_part, ("y", "z"), axis=0, tiled=True)

    tokens_t = tokens.T
    mine = tokens_t.reshape(blocks // 2, 2, rows, count)
    keep = lax.dynamic_index_in_dim(mine, xh, 1, False)
    give = lax.dynamic_index_in_dim(mine, 1 - xh, 1, False)
    pair = jnp.concatenate([keep, swap(give, "xh")], axis=-1)
    wide = gathered_pieces(pair, xl, c).reshape(ny, nz, rows, 2 * count).astype(F32)
    partial_sum = jnp.sum(wide * wide, axis=(0, 1, 2))
    other_sum = swap(partial_sum.reshape(4, -1), "xh").reshape(-1)
    square_sum = partial_sum + jnp.roll(other_sum, count)
    pair_scale = lax.rsqrt(square_sum / D + EPSILON)

    def parity(a, which):
        return lax.dynamic_index_in_dim(a.reshape(ny, nz, 2, rows, -1), which, 2, False)

    normed = (wide * pair_scale * parity(in_gain, xh)).astype(BF).reshape(D // 2, -1)
    downs = jnp.concatenate([q_down, kv_down[0], kv_down[1]], axis=1)
    downs_parity = parity(downs, xh).reshape(D // 2, -1)
    low_pair = dot_f32(normed, downs_parity, 0, 0)
    low_sum = low_pair[:count] + swap(low_pair[count:], "xh")
    low = low_sum.astype(BF)
    rank = q_down.shape[1]
    query_lowrank, key_lowrank, value_lowrank = (
        low[:, i * rank : (i + 1) * rank] for i in range(3)
    )
    row_scale = pair_scale[:count]
    qkv_pair = dot_f32(normed, own_matrix, 0, 0)
    far_kv = swap(qkv_pair[count:, q_width:].astype(BF), "xh")
    kv_sum = qkv_pair[:count, q_width:] + far_kv.astype(F32)
    far_q = swap(after(qkv_pair[count:, :q_width].astype(BF), far_kv), "xh")
    q_sum = qkv_pair[:count, :q_width] + far_q.astype(F32)

    def of_heads(both, which):
        return both.reshape(-1, kv_heads_here, 2, HEAD_SIZE)[:, :, which].reshape(-1, kv_width)

    key = of_heads(kv_sum, 0) + ADAPTER_SCALE * dot_f32(key_lowrank, key_value_up[0], 1, 0)
    value_total = of_heads(kv_sum, 1) + ADAPTER_SCALE * dot_f32(
        value_lowrank, key_value_up[1], 1, 0
    )
    value_rows = value_total.astype(BF)
    query_rows = q_sum + ADAPTER_SCALE * dot_f32(query_lowrank, query_up, 1, 0)

    query_pos = ctx_rank * count + jnp.arange(count, dtype=jnp.int32)
    cosine, sine = rope_tables(query_pos)
    key_head_rows = key.reshape(count, kv_heads_here, HEAD_SIZE)
    k_normed, k_scale = head_norm(key_head_rows, key_gain)
    k_rot = rotate(k_normed, cosine, sine).astype(BF)
    kv_rows = jnp.stack([k_rot, value_rows.reshape(k_rot.shape)], axis=2).reshape(count, -1)
    steps = WINDOW_TOKENS // count
    window = [shifted(kv_rows, s) for s in range(steps, 0, -1)] + [kv_rows]
    first_key = (WINDOW_TOKENS - ctx_rank * count).astype(jnp.int32).reshape(1)
    q_heads = query_rows.reshape(count, q_heads_here, HEAD_SIZE)
    q_normed, q_scale = head_norm(q_heads, query_gain)
    q_rot = rotate(q_normed, cosine, sine).astype(BF)

    q_turned = q_rot.reshape(count, q_width).T

    o_swapped, qkv_other = swap(after((o_part, qkv_part), low_pair), "xh")
    o_both = jnp.concatenate(
        [jnp.where(xh == 0, o_part, o_swapped), jnp.where(xh == 0, o_swapped, o_part)]
    )
    output_matrix = lax.all_gather(after(o_both, own_matrix), ("y", "z"), axis=0, tiled=True)
    other_matrix = lax.all_gather(after(qkv_other, output_matrix), ("y", "z"), axis=0, tiled=True)
    out_grad_t = out_grad.T
    out_grad_full = gathered_pieces(after(out_grad_t, far_q), xl, c)

    (attended,) = attention_call(
        forward_kernel, first_key, [q_turned], window, [jax.ShapeDtypeStruct((q_width, count), BF)]
    )

    low_out_part = dot_f32(attended, output_down, 0, 0).astype(BF)
    out_rows = output_matrix.reshape(2, 2 * share, q_width)
    up_rows = output_up.T.reshape(2, 2 * share, rank)
    low_rows = low_out_part.T.astype(F32)
    sums, low_total = [], None
    for j in range(2):
        part = dot_f32(out_rows[j], attended, 1, 0) + ADAPTER_SCALE * dot_f32(
            up_rows[j], low_out_part, 1, 1
        )
        part = part.reshape(2, share, count)
        keep = lax.dynamic_index_in_dim(part, c, 0, False)
        give = lax.dynamic_index_in_dim(part, 1 - c, 0, False)
        if j == 0:
            keep = jnp.concatenate([keep, low_rows])
            give = jnp.concatenate([give, low_rows])
        chip = (keep + swap(give.astype(BF), "c").astype(F32)).astype(BF)
        total = (chip.astype(F32) + swap(chip, "xl").astype(F32)).astype(BF)
        if j == 0:
            low_total = total[share:]
            total = total[:share]
        far = swap(total, "c")
        sums.append(jnp.stack([jnp.where(c == 0, total, far), jnp.where(c == 0, far, total)]))
    out_total = jnp.stack(sums).astype(F32)
    output_lowrank = low_total.T
    gain_full = post_gain.reshape(2, 2, share, 1)
    weighted_out = out_grad_full.astype(F32) * gain_full
    out_scale = lax.rsqrt(jnp.sum(out_total * out_total, axis=(0, 1, 2)) / D + EPSILON)
    out_inner = jnp.sum(weighted_out * out_total, axis=(0, 1, 2)) / D
    grad_full = (out_scale * weighted_out - out_scale**3 * out_total * out_inner).astype(BF)
    output_gradient = grad_full.reshape(D, count)
    out_mine = lax.dynamic_slice_in_dim(out_total.reshape(D, count), column_start, share, 0)
    post_mine = lax.dynamic_slice_in_dim(post_gain, column_start, share, 0)[:, None]
    mixed = (tokens_t.astype(F32) + out_mine * out_scale * post_mine).astype(BF)

    output_mixture = dot_f32(output_gradient, output_up, 0, 1).astype(BF)
    grad_mine = lax.dynamic_slice_in_dim(output_gradient, column_start, share, 0)
    output_up_gradient = ADAPTER_SCALE * dot_f32(output_lowrank, grad_mine, 0, 1)
    output_down_gradient = ADAPTER_SCALE * dot_f32(output_mixture, attended, 0, 1)
    attended_gradient = (
        dot_f32(output_matrix, output_gradient, 0, 0)
        + ADAPTER_SCALE * dot_f32(output_down, output_mixture, 1, 1)
    ).astype(BF)
    query_grad, *window_grad = attention_call(
        backward_kernel,
        first_key,
        [q_turned, attended_gradient],
        window,
        [jax.ShapeDtypeStruct((q_width, count), F32)]
        + [jax.ShapeDtypeStruct((count, 2 * kv_width), BF)] * steps
        + [jax.ShapeDtypeStruct((count, 2 * kv_width), F32)],
    )
    own = window_grad[steps]
    for s in range(steps, 0, -1):
        own = own + shifted(window_grad[steps - s], -s).astype(F32)
    query_grad = query_grad.T.reshape(count, q_heads_here, HEAD_SIZE)
    q_norm_grad = unrotate(query_grad, cosine, sine)
    k_norm_grad = unrotate(of_heads(own, 0).reshape(count, kv_heads_here, HEAD_SIZE), cosine, sine)
    query_back = head_norm_back(q_heads, q_scale, query_gain, q_norm_grad)
    query_back = query_back.reshape(count, q_width).astype(BF)
    into_query = [dot_f32(w[:, :q_width], query_back, 1, 1) for w in (own_matrix, other_matrix)]
    key_back = head_norm_back(key_head_rows, k_scale, key_gain, k_norm_grad)
    key_back = key_back.reshape(count, kv_width).astype(BF)
    value_back = of_heads(own, 1).astype(BF)

    inner_part = (
        jnp.sum(query_back.astype(F32) * query_rows, axis=1)
        + jnp.sum(key_back.astype(F32) * key, axis=1)
        + jnp.sum(value_back.astype(F32) * value_total, axis=1)
    )
    small = jnp.concatenate(
        [
            dot_f32(query_up, query_back, 1, 1),
            dot_f32(key_value_up[0], key_back, 1, 1),
            dot_f32(key_value_up[1], value_back, 1, 1),
            inner_part[None],
            jnp.zeros((7, count), F32),
        ]
    )
    small = jnp.sum(lax.all_gather(small, TP), axis=0)
    mixes = small[: 3 * rank].astype(BF)
    in_inner = small[3 * rank] / (row_scale * D)

    in_gain_mine = lax.dynamic_slice_in_dim(in_gain, column_start, share, 0)[:, None]
    tokens_wide = tokens_t.astype(F32)
    normed_mine = (tokens_wide * row_scale * in_gain_mine).astype(BF)
    down_gradients = ADAPTER_SCALE * dot_f32(mixes, normed_mine, 1, 1)
    up_gradients = ADAPTER_SCALE * jnp.concatenate(
        [
            dot_f32(query_lowrank, query_back, 0, 0),
            dot_f32(key_lowrank, key_back, 0, 0),
            dot_f32(value_lowrank, value_back, 0, 0),
        ],
        axis=1,
    )
    everything = jnp.concatenate(
        [
            down_gradients.reshape(-1),
            output_up_gradient.reshape(-1),
            up_gradients.reshape(-1),
            output_down_gradient.reshape(-1),
        ]
    )
    devices = lax.axis_size(CTX)
    parts = everything.reshape(devices, -1, 128)
    sums_arrived = lax.all_to_all(parts, CTX, 0, 0, tiled=True)

    heads = (count, kv_heads_here, HEAD_SIZE)
    kv_back = jnp.stack([key_back.reshape(heads), value_back.reshape(heads)], axis=2)
    kv_back = after(kv_back.reshape(count, -1), parts)
    into = [
        (part + dot_f32(w[:, q_width:], kv_back, 1, 1)).reshape(2, 2, share // 2, count)
        for part, w in zip(into_query, (own_matrix, other_matrix))
    ]

    def piece(a, far_xl, far_c):
        a = lax.dynamic_index_in_dim(a, 1 - xl if far_xl else xl, 0, False)
        return lax.dynamic_index_in_dim(a, 1 - c if far_c else c, 0, False)

    give = [
        jnp.concatenate([piece(a, far, True) for a in into]).astype(BF) for far in (True, False)
    ]
    arrived = [swap(g, "c").astype(F32) for g in give]
    to_chip = jnp.concatenate([piece(a, True, False) for a in into]) + arrived[0]
    far_into = swap(to_chip.astype(BF), "xl")
    into_mine = jnp.concatenate([piece(a, False, False) for a in into]) + arrived[1]
    into_mine = into_mine + far_into.astype(F32)
    halves = into_mine.reshape(2, nz, rows, count)
    first = jnp.where(xh == 0, halves[0], halves[1])
    last = jnp.where(xh == 0, halves[1], halves[0])
    into_mine = jnp.stack([first, last], axis=1).reshape(share, count)

    downs_mine = lax.dynamic_slice_in_dim(downs, column_start, share, 0)
    normalized_gradient = into_mine + ADAPTER_SCALE * dot_f32(downs_mine, mixes, 1, 0)
    weighted_in = normalized_gradient * in_gain_mine
    tokens_grad = (
        out_grad_t.astype(F32)
        + row_scale * weighted_in
        - row_scale**3 * tokens_wide * in_inner
    )
    in_projection = (float(D) ** 0.5 * row_scale * in_inner)[:, None]
    chunk = jnp.sum(sums_arrived, axis=0)
    spread = jnp.broadcast_to(chunk[None], (devices, *chunk.shape))
    summed = lax.all_to_all(spread, CTX, 0, 0, tiled=True).reshape(-1)
    cut = 4 * rank * share
    wide_sums = lax.all_gather(summed[:cut].reshape(4 * rank, share).astype(BF), TP)
    wide_sums = jnp.moveaxis(wide_sums, 0, 1).reshape(4 * rank, D).astype(F32)
    narrow = summed[cut : cut + up_gradients.size].reshape(up_gradients.shape)
    output_down_gradient = summed[cut + up_gradients.size :].reshape(rank, q_width).T

    return (
        mixed.T,
        tokens_grad.T,
        wide_sums[:rank].T,
        narrow[:, :q_width],
        jnp.stack([wide_sums[rank : 2 * rank].T, wide_sums[2 * rank : 3 * rank].T]),
        jnp.stack([narrow[:, q_width : q_width + kv_width], narrow[:, q_width + kv_width :]]),
        output_down_gradient,
        wide_sums[3 * rank :],
        in_projection,
    )


def solution(mesh):
    torus = Mesh(mesh.devices.reshape(4, 4, 2, 2, 2), (*CTX, *TP))

    return jax.shard_map(
        on_device,
        mesh=torus,
        in_specs=(
            P(CTX, TP),
            P(CTX, TP),
            P(),
            P(),
            P(),
            P(),
            P(CTX, TP),
            P(CTX, TP),
            P(None, TP),
            P(None, CTX, TP),
            P(None, CTX, TP),
            P(None, None, TP),
            P(CTX, TP),
            P(CTX, TP),
            P(None, TP),
            P(),
            P(None, TP),
            P(),
            P(None, None, TP),
            P(TP, None),
            P(),
        ),
        out_specs=(
            P(CTX, TP),
            P(CTX, TP),
            P(),
            P(None, TP),
            P(),
            P(None, None, TP),
            P(TP, None),
            P(),
            P(CTX, None),
        ),
        check_vma=False,
    )
```

```python
import jax
import jax.numpy as jnp
from jax import lax
from jax.experimental import pallas as pl
from jax.experimental.pallas import tpu as pltpu
from jax.sharding import Mesh
from jax.sharding import PartitionSpec as P

D = 5376
HEAD_SIZE = 128
WINDOW_TOKENS = 1024
QBLOCK = 64
QGROUP = 256
CTX = ("y", "z", "xh")
TP = ("xl", "c")
NORMAL_FLOAT = (
    -1.0,
    -0.6961928009986877,
    -0.5250730514526367,
    -0.39491748809814453,
    -0.28444138169288635,
    -0.18477343022823334,
    -0.09105003625154495,
    0.0,
    0.07958029955625534,
    0.16093020141124725,
    0.24611230194568634,
    0.33791524171829224,
    0.44070982933044434,
    0.5626170039176941,
    0.7229568362236023,
    1.0,
)
EPSILON = 1e-06
ADAPTER_SCALE = 2.0
SCORE_SCALE = 168.0 ** (-0.5)
ROPE_BASE = 10000.0
BF = jnp.bfloat16
F32 = jnp.float32


def swap(x, axis):
    return lax.ppermute(x, axis, [(0, 1), (1, 0)])


def after(arrays, *done):
    return lax.optimization_barrier((arrays, done))[0]


def shifted(x, by):
    n = lax.axis_size(CTX)
    return lax.ppermute(x, CTX, [(i, i + by) for i in range(n) if 0 <= i + by < n])


def dot_f32(a, b, ca, cb):
    return lax.dot_general(a, b, (((ca,), (cb,)), ((), ())), preferred_element_type=F32)


def levels_of(codes):
    bits = [(codes & (1 << b)) != 0 for b in range(4)]
    table = [F32(v) for v in NORMAL_FLOAT]
    for bit in bits:
        table = [jnp.where(bit, high, low) for low, high in zip(table[::2], table[1::2])]
    return table[0]


def scales_of(place, scodes, second):
    group = lax.broadcasted_iota(jnp.int32, second.shape, 1)
    first = jnp.sum(jnp.where(group == place[0], second, 0.0), axis=1, keepdims=True)
    last = jnp.sum(jnp.where(group == place[1], second, 0.0), axis=1, keepdims=True)
    row = lax.broadcasted_iota(jnp.int32, scodes.shape, 1)
    return jnp.where(row < place[2], first, last) * ((scodes.astype(F32) + 1.0) / 256.0)


def dequantize_kernel(place, q_ref, kv_ref, o_ref, qs, kvs, os, q2, kv2, o2, qkv_out, o_out):
    height, q_width = q_ref.shape
    kv_width = kv_ref.shape[2]
    parts = [
        scales_of(place, qs[...], q2[...]),
        scales_of(place, kvs[0], kv2[0]),
        scales_of(place, kvs[1], kv2[1]),
        scales_of(place, os[...], o2[...]),
    ]
    parts = [
        p if p.shape[0] % 8 == 0 else jnp.concatenate([p, jnp.zeros((8 - p.shape[0] % 8, height), F32)])
        for p in parts
    ]
    absmax = jnp.concatenate(parts)
    starts = [sum(p.shape[0] for p in parts[:n]) for n in range(4)]
    absmax = absmax.T
    lane = lax.broadcasted_iota(jnp.int32, (height, 128), 1)

    def scaled(codes, block):
        scale = jnp.where(lane < QBLOCK, absmax[:, block : block + 1], absmax[:, block + 1 : block + 2])
        return (levels_of(codes) * scale).astype(BF)

    for j in range(q_width // 128):
        at = slice(j * 128, (j + 1) * 128)
        qkv_out[:, at] = scaled(q_ref[:, at], 2 * j)
        o_out[:, at] = scaled(o_ref[:, at], starts[3] + 2 * j)
    for j in range(kv_width // 128):
        for part in range(2):
            to = q_width + (2 * j + part) * 128
            codes = kv_ref[part, :, j * 128 : (j + 1) * 128]
            qkv_out[:, to : to + 128] = scaled(codes, starts[1 + part] + 2 * j)


def dequantize(codes, scales, row_start):
    q_codes, kv_codes, _ = codes
    height, q_width = q_codes.shape
    kv_width = kv_codes.shape[2]
    group = row_start // QGROUP
    last = jnp.minimum(group + 1, scales[3].shape[1] - 1)
    place = jnp.stack([group, last, (group + 1) * QGROUP - row_start]).astype(jnp.int32)
    return pl.pallas_call(
        dequantize_kernel,
        out_shape=(
            jax.ShapeDtypeStruct((height, q_width + 2 * kv_width), BF),
            jax.ShapeDtypeStruct((height, q_width), BF),
        ),
        in_specs=[pl.BlockSpec(memory_space=pltpu.SMEM)]
        + [pl.BlockSpec(memory_space=pltpu.VMEM)] * 9,
        name="dequantize",
    )(place, *codes, *scales)


def rope_tables(positions):
    half = HEAD_SIZE // 2
    exponent = jnp.arange(half, dtype=F32) * (2.0 / HEAD_SIZE)
    frequency = jnp.power(F32(ROPE_BASE), -exponent)
    angle = positions.astype(F32)[:, None] * frequency[None, :]
    return (jnp.cos(angle), jnp.sin(angle))


def rotate(heads, cosine, sine):
    half = heads.shape[-1] // 2
    first = heads[..., :half]
    second = heads[..., half:]
    across = cosine[:, None, :]
    along = sine[:, None, :]
    return jnp.concatenate(
        [first * across - second * along, second * across + first * along], axis=-1
    )


def head_norm(heads, gain):
    scale = lax.rsqrt(jnp.mean(heads * heads, axis=-1, keepdims=True) + EPSILON)
    return (heads * scale * gain, scale)


def head_norm_back(heads, scale, gain, grad):
    weighted = grad * gain
    inner = jnp.mean(weighted * heads, axis=-1, keepdims=True)
    return scale * weighted - scale**3 * heads * inner


def mxu(a, b, ca, cb):
    return lax.dot_general(a, b, (((ca,), (cb,)), ((), ())), preferred_element_type=F32)


def side_by_side(ref):
    return jnp.concatenate([ref[:HEAD_SIZE, :], ref[HEAD_SIZE:, :]], axis=1)


def weights_of(first_key, blocks, queries):
    weights, total = [], None
    for b, block in enumerate(blocks):
        keys, count = block.shape[0], queries.shape[1] // 2
        scores = mxu(block[:, :HEAD_SIZE], queries, 1, 0) * SCORE_SCALE
        e = jnp.exp(scores)
        key = lax.broadcasted_iota(jnp.int32, e.shape, 0)
        query = lax.broadcasted_iota(jnp.int32, e.shape, 1) % count
        if b == 0:
            e = jnp.where((key > query) & (first_key <= 0), e, 0.0)
        elif b == len(blocks) - 1:
            e = jnp.where(key <= query, e, 0.0)
        else:
            e = jnp.where(key + b * keys >= first_key, e, 0.0)
        part = jnp.sum(e, axis=0, keepdims=True)
        total = part if total is None else total + part
        weights.append(e)
    return weights, total


def forward_kernel(first_key, q_ref, *refs):
    blocks, out = refs[:-1], refs[-1]
    queries = side_by_side(q_ref)
    count = q_ref.shape[1]
    weights, total = weights_of(first_key[0], blocks, queries)
    inverse = 1.0 / total
    mixed = None
    for block, e in zip(blocks, weights):
        term = mxu(block[:, HEAD_SIZE:], (e * inverse).astype(BF), 0, 0)
        mixed = term if mixed is None else mixed + term
    mixed = mixed.astype(BF)
    out[:HEAD_SIZE, :] = mixed[:, :count]
    out[HEAD_SIZE:, :] = mixed[:, count:]


def backward_kernel(first_key, q_ref, grad_ref, *refs):
    n = (len(refs) - 1) // 2
    blocks, q_out, outs = refs[:n], refs[n], refs[n + 1 :]
    queries, grads = side_by_side(q_ref), side_by_side(grad_ref)
    count = q_ref.shape[1]
    weights, total = weights_of(first_key[0], blocks, queries)
    inverse = 1.0 / total
    inner, from_values = None, []
    for block, e in zip(blocks, weights):
        g = mxu(block[:, HEAD_SIZE:], grads, 1, 0)
        part = jnp.sum(e * inverse * g, axis=0, keepdims=True)
        inner = part if inner is None else inner + part
        from_values.append(g)
    q_grad = None
    for block, e, g, out in zip(blocks, weights, from_values, outs):
        p = e * inverse
        score_grad = (p * (g - inner) * SCORE_SCALE).astype(BF)
        out[:, HEAD_SIZE:] = mxu(p.astype(BF), grads, 1, 1).astype(out.dtype)
        out[:, :HEAD_SIZE] = mxu(score_grad, queries, 1, 1).astype(out.dtype)
        term = mxu(block[:, :HEAD_SIZE], score_grad, 0, 0)
        q_grad = term if q_grad is None else q_grad + term
    q_out[:HEAD_SIZE, :] = q_grad[:, :count]
    q_out[HEAD_SIZE:, :] = q_grad[:, count:]


def attention_call(kernel, first_key, transposed, blocks, outs):
    count = transposed[0].shape[1]
    row = pl.BlockSpec((2 * HEAD_SIZE, count), lambda g: (g, 0))
    column = pl.BlockSpec((count, 2 * HEAD_SIZE), lambda g: (0, g))
    kinds = [row if o.shape[1] == count else column for o in outs]
    return pl.pallas_call(
        kernel,
        grid=(blocks[0].shape[1] // (2 * HEAD_SIZE),),
        out_shape=outs,
        in_specs=[pl.BlockSpec(memory_space=pltpu.SMEM)]
        + [row] * len(transposed)
        + [column] * len(blocks),
        out_specs=kinds,
    )(first_key, *transposed, *blocks)


def unrotated(grad, across, along):
    return grad * across + pltpu.roll(grad, HEAD_SIZE // 2, 1) * along


def query_back_kernel(grad, rows, across, along, gain, up, back, small):
    mix, products = None, None
    for h in range(rows.shape[1] // HEAD_SIZE):
        at = slice(h * HEAD_SIZE, (h + 1) * HEAD_SIZE)
        heads = rows[:, at]
        scale = lax.rsqrt(jnp.mean(heads * heads, axis=-1, keepdims=True) + EPSILON)
        g = unrotated(grad[at, :].T, across[...], along[...])
        b = head_norm_back(heads, scale, gain[...], g).astype(BF)
        back[:, at] = b
        m, p = mxu(up[:, at], b, 1, 1), b.astype(F32) * heads
        mix, products = (m, p) if mix is None else (mix + m, products + p)
    rank, count = mix.shape
    small[:rank, :] = mix
    small[rank:, :] = jnp.broadcast_to(jnp.sum(products.T, axis=0, keepdims=True), (8, count))


def key_value_back_kernel(*refs):
    own, arrived = refs[0], refs[1:-7]
    rows, across, along, gain, up, back, small = refs[-7:]
    mixes, products = [None, None], None
    for h in range(rows.shape[1] // HEAD_SIZE):
        at = slice(h * HEAD_SIZE, (h + 1) * HEAD_SIZE)
        g = own[:, at]
        for a in arrived:
            g = g + a[:, at].astype(F32)
        heads = rows[:, at]
        if h % 2 == 0:
            scale = lax.rsqrt(jnp.mean(heads * heads, axis=-1, keepdims=True) + EPSILON)
            g = unrotated(g, across[...], along[...])
            g = head_norm_back(heads, scale, gain[...], g)
        b = g.astype(BF)
        back[:, at] = b
        m, p = mxu(up[:, at], b, 1, 1), b.astype(F32) * heads
        mixes[h % 2] = m if mixes[h % 2] is None else mixes[h % 2] + m
        products = p if products is None else products + p
    rank, count = mixes[0].shape
    small[:rank, :] = mixes[0]
    small[rank : 2 * rank, :] = mixes[1]
    small[2 * rank :, :] = jnp.broadcast_to(jnp.sum(products.T, axis=0, keepdims=True), (8, count))


def adapter_kernel(smalls, normed, up_grad, q_up, down_grad, low, kv_back, out, mixes_out, inner_out, buf):
    rank = q_up.shape[0]
    total = smalls[0]
    for i in range(1, smalls.shape[0]):
        total = total + smalls[i]
    mixes = jnp.concatenate([total[:rank], total[rank + 8 : 3 * rank + 8]]).astype(BF)
    mixes_out[...] = mixes
    inner_out[...] = total[rank : rank + 8] + total[3 * rank + 8 :]
    buf[: 3 * rank, :] = ADAPTER_SCALE * mxu(mixes, normed[...], 1, 1)
    buf[3 * rank : 4 * rank, :] = up_grad[...]
    kv = ADAPTER_SCALE * mxu(low[rank:, :], kv_back[...], 1, 0)
    row, extra = slice(4 * rank, 5 * rank), slice(5 * rank, 6 * rank)
    at = q_up.shape[1]
    buf[row, :at] = q_up[...]
    for h in range(kv_back.shape[1] // HEAD_SIZE):
        here = slice(h * HEAD_SIZE, (h + 1) * HEAD_SIZE)
        which = h % 2
        buf[row, at : at + HEAD_SIZE] = kv[which * rank : (which + 1) * rank, here]
        at += HEAD_SIZE
    half = down_grad.shape[1] // 2
    buf[row, at : at + half] = down_grad[:, :half]
    buf[row, at + half :] = jnp.zeros((rank, buf.shape[1] - at - half), F32)
    buf[extra, :half] = down_grad[:, half:]
    buf[extra, half:] = jnp.zeros((rank, buf.shape[1] - half), F32)
    each = out.shape[1]
    for i in range(out.shape[0]):
        out[i] = buf[i * each : (i + 1) * each, :]


def whole(kernel, outs, arrays, scratch=()):
    return pl.pallas_call(
        kernel,
        out_shape=outs,
        in_specs=[pl.BlockSpec(memory_space=pltpu.VMEM)] * len(arrays),
        out_specs=[pl.BlockSpec(memory_space=pltpu.VMEM)] * len(outs),
        scratch_shapes=list(scratch),
    )(*arrays)


def into_kernel(piece, own, other, back, out):
    out[0] = mxu(own[...], back[...], 1, 1).astype(out.dtype)
    out[1] = mxu(other[...], back[...], 1, 1).astype(out.dtype)


def into_piece(own, other, back, piece, rows, dtype):
    half = own.shape[0] // 4
    steps = half // rows
    weight = pl.BlockSpec((rows, own.shape[1]), lambda i, p: (p[0] * steps + i, 0))
    count = back.shape[0]
    return pl.pallas_call(
        into_kernel,
        out_shape=jax.ShapeDtypeStruct((2, half, count), dtype),
        grid_spec=pltpu.PrefetchScalarGridSpec(
            num_scalar_prefetch=1,
            grid=(steps,),
            in_specs=[weight, weight, pl.BlockSpec(back.shape, lambda i, p: (0, 0))],
            out_specs=pl.BlockSpec((2, rows, count), lambda i, p: (0, i, 0)),
        ),
        name="into_piece",
    )(piece, own, other, back)


def out_kernel(piece, weight, up, attended, low, out):
    total = mxu(weight[...], attended[...], 1, 0)
    total = total + ADAPTER_SCALE * mxu(up[...], low[...], 1, 0)
    out[...] = total.astype(out.dtype)


def out_piece(matrix, up, attended, low, piece, dtype):
    steps = 4
    rows = matrix.shape[0] // (4 * steps)
    count = attended.shape[1]

    def rows_of(a):
        return pl.BlockSpec((rows, a.shape[1]), lambda i, p: (p[0] * steps + i, 0))

    def all_of(a):
        return pl.BlockSpec(a.shape, lambda i, p: (0, 0))

    return pl.pallas_call(
        out_kernel,
        out_shape=jax.ShapeDtypeStruct((rows * steps, count), dtype),
        grid_spec=pltpu.PrefetchScalarGridSpec(
            num_scalar_prefetch=1,
            grid=(steps,),
            in_specs=[rows_of(matrix), rows_of(up), all_of(attended), all_of(low)],
            out_specs=pl.BlockSpec((rows, count), lambda i, p: (i, 0)),
        ),
        name="out_piece",
    )(piece, matrix, up, attended, low)


def gathered_pieces(own, xl, c):
    other = swap(own, "xl")
    pair = jnp.stack([jnp.where(xl == 0, own, other), jnp.where(xl == 0, other, own)])
    far = swap(pair, "c")
    return jnp.stack([jnp.where(c == 0, pair, far), jnp.where(c == 0, far, pair)], axis=1)


def on_device(
    tokens,
    out_grad,
    in_gain,
    query_gain,
    key_gain,
    post_gain,
    q_codes,
    q_scodes,
    q_second,
    kv_codes,
    kv_scodes,
    kv_second,
    o_codes,
    o_scodes,
    o_second,
    q_down,
    query_up,
    kv_down,
    key_value_up,
    output_down,
    output_up,
):
    count, share = tokens.shape
    _, _, xh = (lax.axis_index(a) for a in CTX)
    xl, c = (lax.axis_index(a) for a in TP)
    ctx_rank = lax.axis_index(CTX)
    column_start = lax.axis_index(TP) * share
    rows = q_codes.shape[0]
    row_start = ctx_rank * rows
    blocks = share // rows
    ny, nz = lax.axis_size("y"), lax.axis_size("z")
    q_width = query_up.shape[1]
    kv_width = key_value_up.shape[2]
    q_heads_here = q_width // HEAD_SIZE
    kv_heads_here = kv_width // HEAD_SIZE

    turned = (0, 2, 1)
    scales = [q_scodes.T, kv_scodes.transpose(turned), o_scodes.T]
    scales += [q_second.T, kv_second.transpose(turned), o_second.T]
    qkv_part, o_part = dequantize([q_codes, kv_codes, o_codes], scales, row_start)
    own_matrix = lax.all_gather(qkv_part, ("y", "z"), axis=0, tiled=True)

    tokens_t = tokens.T
    mine = tokens_t.reshape(blocks // 2, 2, rows, count)
    keep = lax.dynamic_index_in_dim(mine, xh, 1, False)
    give = lax.dynamic_index_in_dim(mine, 1 - xh, 1, False)
    pair = jnp.concatenate([keep, swap(give, "xh")], axis=-1)
    wide = gathered_pieces(pair, xl, c).reshape(ny, nz, rows, 2 * count).astype(F32)
    partial_sum = jnp.sum(wide * wide, axis=(0, 1, 2))
    other_sum = swap(partial_sum.reshape(4, -1), "xh").reshape(-1)
    square_sum = partial_sum + jnp.roll(other_sum, count)
    pair_scale = lax.rsqrt(square_sum / D + EPSILON)

    def parity(a, which):
        return lax.dynamic_index_in_dim(a.reshape(ny, nz, 2, rows, -1), which, 2, False)

    normed = (wide * pair_scale * parity(in_gain, xh)).astype(BF).reshape(D // 2, -1)
    downs = jnp.concatenate([q_down, kv_down[0], kv_down[1]], axis=1)
    downs_parity = parity(downs, xh).reshape(D // 2, -1)
    low_pair = dot_f32(normed, downs_parity, 0, 0)
    low_sum = low_pair[:count] + swap(low_pair[count:], "xh")
    low = low_sum.astype(BF)
    rank = q_down.shape[1]
    query_lowrank, _, _ = (
        low[:, i * rank : (i + 1) * rank] for i in range(3)
    )
    row_scale = pair_scale[:count]
    qkv_pair = dot_f32(normed, own_matrix, 0, 0)
    far_kv = swap(qkv_pair[count:, q_width:].astype(BF), "xh")
    kv_sum = qkv_pair[:count, q_width:] + far_kv.astype(F32)
    far_q = swap(after(qkv_pair[count:, :q_width].astype(BF), far_kv), "xh")
    q_sum = qkv_pair[:count, :q_width] + far_q.astype(F32)

    def of_heads(both, which):
        return both.reshape(-1, kv_heads_here, 2, HEAD_SIZE)[:, :, which].reshape(-1, kv_width)

    def interleaved(first, second):
        heads = (-1, kv_heads_here, HEAD_SIZE)
        both = jnp.stack([first.reshape(heads), second.reshape(heads)], axis=2)
        return both.reshape(first.shape[0], 2 * kv_width)

    kv_up = interleaved(key_value_up[0], key_value_up[1])
    nothing = jnp.zeros_like(key_value_up[0])
    kv_up_apart = jnp.concatenate(
        [interleaved(key_value_up[0], nothing), interleaved(nothing, key_value_up[1])]
    )
    kv_total = kv_sum + ADAPTER_SCALE * dot_f32(low[:, rank:], kv_up_apart, 1, 0)
    key = of_heads(kv_total, 0)
    value_rows = of_heads(kv_total, 1).astype(BF)
    query_rows = q_sum + ADAPTER_SCALE * dot_f32(query_lowrank, query_up, 1, 0)

    query_pos = ctx_rank * count + jnp.arange(count, dtype=jnp.int32)
    cosine, sine = rope_tables(query_pos)
    key_head_rows = key.reshape(count, kv_heads_here, HEAD_SIZE)
    k_normed, _ = head_norm(key_head_rows, key_gain)
    k_rot = rotate(k_normed, cosine, sine).astype(BF)
    kv_rows = jnp.stack([k_rot, value_rows.reshape(k_rot.shape)], axis=2).reshape(count, -1)
    steps = WINDOW_TOKENS // count
    window = [shifted(kv_rows, s) for s in range(steps, 0, -1)] + [kv_rows]
    first_key = (WINDOW_TOKENS - ctx_rank * count).astype(jnp.int32).reshape(1)
    q_heads = query_rows.reshape(count, q_heads_here, HEAD_SIZE)
    q_normed, _ = head_norm(q_heads, query_gain)
    q_rot = rotate(q_normed, cosine, sine).astype(BF)

    q_turned = q_rot.reshape(count, q_width).T

    o_swapped, qkv_other = swap(after((o_part, qkv_part), low_pair), "xh")
    o_both = jnp.concatenate(
        [jnp.where(xh == 0, o_part, o_swapped), jnp.where(xh == 0, o_swapped, o_part)]
    )
    output_matrix = lax.all_gather(after(o_both, own_matrix), ("y", "z"), axis=0, tiled=True)
    other_matrix = lax.all_gather(after(qkv_other, output_matrix), ("y", "z"), axis=0, tiled=True)
    out_grad_t = out_grad.T
    out_grad_full = gathered_pieces(after(out_grad_t, far_q), xl, c)

    (attended,) = attention_call(
        forward_kernel, first_key, [q_turned], window, [jax.ShapeDtypeStruct((q_width, count), BF)]
    )

    low_out_part = dot_f32(output_down, attended, 0, 0).astype(BF)
    up_rows = output_up.T
    sums, low_total = [], None

    def number(a, b):
        return (a * 2 + b).astype(jnp.int32).reshape(1)

    for j in range(2):
        give = out_piece(output_matrix, up_rows, attended, low_out_part, number(j, 1 - c), BF)
        keep = out_piece(output_matrix, up_rows, attended, low_out_part, number(j, c), F32)
        if j == 0:
            keep = jnp.concatenate([keep, low_out_part.astype(F32)])
            give = jnp.concatenate([give, low_out_part])
        chip = (keep + swap(give.astype(BF), "c").astype(F32)).astype(BF)
        total = (chip.astype(F32) + swap(chip, "xl").astype(F32)).astype(BF)
        if j == 0:
            low_total = total[share:]
            total = total[:share]
        far = swap(total, "c")
        sums.append(jnp.stack([jnp.where(c == 0, total, far), jnp.where(c == 0, far, total)]))
    out_total = jnp.stack(sums).astype(F32)
    output_lowrank = low_total.T
    gain_full = post_gain.reshape(2, 2, share, 1)
    weighted_out = out_grad_full.astype(F32) * gain_full
    out_scale = lax.rsqrt(jnp.sum(out_total * out_total, axis=(0, 1, 2)) / D + EPSILON)
    out_inner = jnp.sum(weighted_out * out_total, axis=(0, 1, 2)) / D
    grad_full = (out_scale * weighted_out - out_scale**3 * out_total * out_inner).astype(BF)
    output_gradient = grad_full.reshape(D, count)
    out_mine = lax.dynamic_slice_in_dim(out_total.reshape(D, count), column_start, share, 0)
    post_mine = lax.dynamic_slice_in_dim(post_gain, column_start, share, 0)[:, None]
    mixed = (tokens_t.astype(F32) + out_mine * out_scale * post_mine).astype(BF)

    output_mixture = dot_f32(output_gradient, output_up, 0, 1).astype(BF)
    grad_mine = lax.dynamic_slice_in_dim(output_gradient, column_start, share, 0)
    output_up_gradient = ADAPTER_SCALE * dot_f32(output_lowrank, grad_mine, 0, 1)
    output_down_gradient = ADAPTER_SCALE * dot_f32(output_mixture, attended, 0, 1)
    attended_gradient = (
        dot_f32(output_matrix, output_gradient, 0, 0)
        + ADAPTER_SCALE * dot_f32(output_down, output_mixture, 1, 1)
    ).astype(BF)
    query_grad, *window_grad = attention_call(
        backward_kernel,
        first_key,
        [q_turned, attended_gradient],
        window,
        [jax.ShapeDtypeStruct((q_width, count), F32)]
        + [jax.ShapeDtypeStruct((count, 2 * kv_width), BF)] * steps
        + [jax.ShapeDtypeStruct((count, 2 * kv_width), F32)],
    )
    across = jnp.concatenate([cosine, cosine], axis=1)
    along = jnp.concatenate([sine, -sine], axis=1)
    query_back, small_q = whole(
        query_back_kernel,
        [
            jax.ShapeDtypeStruct((count, q_width), BF),
            jax.ShapeDtypeStruct((rank + 8, count), F32),
        ],
        [query_grad, query_rows, across, along, query_gain[None], query_up],
    )
    arrived = [shifted(window_grad[steps - s], -s) for s in range(steps, 0, -1)]
    kv_back, small_kv = whole(
        key_value_back_kernel,
        [
            jax.ShapeDtypeStruct((count, 2 * kv_width), BF),
            jax.ShapeDtypeStruct((2 * rank + 8, count), F32),
        ],
        [window_grad[steps], *arrived, kv_total, across, along, key_gain[None], kv_up],
    )
    smalls = lax.all_gather(jnp.concatenate([small_q, small_kv]), TP)

    in_gain_mine = lax.dynamic_slice_in_dim(in_gain, column_start, share, 0)[:, None]
    tokens_wide = tokens_t.astype(F32)
    normed_mine = (tokens_wide * row_scale * in_gain_mine).astype(BF)
    devices = lax.axis_size(CTX)
    each = 6 * rank // devices
    parts, mixes, inner = whole(
        adapter_kernel,
        [
            jax.ShapeDtypeStruct((devices, each, share), F32),
            jax.ShapeDtypeStruct((3 * rank, count), BF),
            jax.ShapeDtypeStruct((8, count), F32),
        ],
        [
            smalls,
            normed_mine,
            output_up_gradient,
            ADAPTER_SCALE * dot_f32(query_lowrank, query_back, 0, 0),
            output_down_gradient,
            low.T,
            kv_back,
        ],
        [pltpu.VMEM((6 * rank, share), F32)],
    )
    in_inner = inner[0] / (row_scale * D)
    sums_arrived = lax.all_to_all(parts, CTX, 0, 0, tiled=True)

    back = after(jnp.concatenate([query_back, kv_back], axis=1), parts)

    def into(a, b, dtype):
        return into_piece(own_matrix, other_matrix, back, number(a, b), rows, dtype)

    give_far = into(1 - xl, 1 - c, BF)
    give_near = into(xl, 1 - c, BF)
    keep_far = into(1 - xl, c, F32)
    keep_near = into(xl, c, F32)
    to_chip = (keep_far + swap(give_far, "c").astype(F32)).astype(BF)
    far_into = swap(to_chip, "xl")
    into_mine = keep_near + swap(give_near, "c").astype(F32) + far_into.astype(F32)
    halves = into_mine.reshape(2, nz, rows, count)
    first = jnp.where(xh == 0, halves[0], halves[1])
    last = jnp.where(xh == 0, halves[1], halves[0])
    into_mine = jnp.stack([first, last], axis=1).reshape(share, count)

    downs_mine = lax.dynamic_slice_in_dim(downs, column_start, share, 0)
    normalized_gradient = into_mine + ADAPTER_SCALE * dot_f32(downs_mine, mixes, 1, 0)
    weighted_in = normalized_gradient * in_gain_mine
    tokens_grad = (
        out_grad_t.astype(F32)
        + row_scale * weighted_in
        - row_scale**3 * tokens_wide * in_inner
    )
    in_projection = (float(D) ** 0.5 * row_scale * in_inner)[:, None]
    chunk = jnp.sum(sums_arrived, axis=0)
    spread = jnp.broadcast_to(chunk[None], (devices, *chunk.shape))
    summed = lax.all_to_all(spread, CTX, 0, 0, tiled=True).reshape(-1, share)
    cut = 4 * rank
    wide_sums = lax.all_gather(summed[:cut].astype(BF), TP)
    wide_sums = jnp.moveaxis(wide_sums, 0, 1).reshape(cut, D).astype(F32)
    narrow = summed[cut : 5 * rank]
    kv_end = q_width + 2 * kv_width
    kv_up_gradient = narrow[:, q_width:kv_end].reshape(rank, kv_heads_here, 2, HEAD_SIZE)
    kv_up_gradient = kv_up_gradient.transpose(2, 0, 1, 3).reshape(2, rank, kv_width)
    output_down_gradient = jnp.concatenate(
        [narrow[:, kv_end : kv_end + q_width // 2], summed[5 * rank :, : q_width // 2]], axis=1
    ).T
    return (
        mixed.T,
        tokens_grad.T,
        wide_sums[:rank].T,
        narrow[:, :q_width],
        jnp.stack([wide_sums[rank : 2 * rank].T, wide_sums[2 * rank : 3 * rank].T]),
        kv_up_gradient,
        output_down_gradient,
        wide_sums[3 * rank :],
        in_projection,
    )


def solution(mesh):
    torus = Mesh(mesh.devices.reshape(4, 4, 2, 2, 2), (*CTX, *TP))

    return jax.shard_map(
        on_device,
        mesh=torus,
        in_specs=(
            P(CTX, TP),
            P(CTX, TP),
            P(),
            P(),
            P(),
            P(),
            P(CTX, TP),
            P(CTX, TP),
            P(None, TP),
            P(None, CTX, TP),
            P(None, CTX, TP),
            P(None, None, TP),
            P(CTX, TP),
            P(CTX, TP),
            P(None, TP),
            P(),
            P(None, TP),
            P(),
            P(None, None, TP),
            P(TP, None),
            P(),
        ),
        out_specs=(
            P(CTX, TP),
            P(CTX, TP),
            P(),
            P(None, TP),
            P(),
            P(None, None, TP),
            P(TP, None),
            P(),
            P(CTX, None),
        ),
        check_vma=False,
    )
```

```python
import jax
import jax.numpy as jnp
from jax import lax
from jax.experimental import pallas as pl
from jax.experimental.pallas import tpu as pltpu
from jax.sharding import Mesh
from jax.sharding import PartitionSpec as P

D = 5376
HEAD_SIZE = 128
WINDOW_TOKENS = 1024
QBLOCK = 64
QGROUP = 256
CTX = ("y", "z", "xh")
TP = ("xl", "c")
NORMAL_FLOAT = (
    -1.0,
    -0.6961928009986877,
    -0.5250730514526367,
    -0.39491748809814453,
    -0.28444138169288635,
    -0.18477343022823334,
    -0.09105003625154495,
    0.0,
    0.07958029955625534,
    0.16093020141124725,
    0.24611230194568634,
    0.33791524171829224,
    0.44070982933044434,
    0.5626170039176941,
    0.7229568362236023,
    1.0,
)
EPSILON = 1e-06
ADAPTER_SCALE = 2.0
SCORE_SCALE = 168.0 ** (-0.5)
ROPE_BASE = 10000.0
BF = jnp.bfloat16
F32 = jnp.float32


def swap(x, axis):
    return lax.ppermute(x, axis, [(0, 1), (1, 0)])


def after(arrays, *done):
    return lax.optimization_barrier((arrays, done))[0]


def shifted(x, by):
    n = lax.axis_size(CTX)
    return lax.ppermute(x, CTX, [(i, i + by) for i in range(n) if 0 <= i + by < n])


def dot_f32(a, b, ca, cb):
    return lax.dot_general(a, b, (((ca,), (cb,)), ((), ())), preferred_element_type=F32)


def levels_of(codes):
    bits = [(codes & (1 << b)) != 0 for b in range(4)]
    table = [F32(v) for v in NORMAL_FLOAT]
    for bit in bits:
        table = [jnp.where(bit, high, low) for low, high in zip(table[::2], table[1::2])]
    return table[0]


def scales_of(place, scodes, second):
    group = lax.broadcasted_iota(jnp.int32, second.shape, 1)
    first = jnp.sum(jnp.where(group == place[0], second, 0.0), axis=1, keepdims=True)
    last = jnp.sum(jnp.where(group == place[1], second, 0.0), axis=1, keepdims=True)
    row = lax.broadcasted_iota(jnp.int32, scodes.shape, 1)
    return jnp.where(row < place[2], first, last) * ((scodes.astype(F32) + 1.0) / 256.0)


def dequantize_kernel(place, q_ref, kv_ref, o_ref, qs, kvs, os, q2, kv2, o2, qkv_out, o_out):
    height, q_width = q_ref.shape
    kv_width = kv_ref.shape[2]
    parts = [
        scales_of(place, qs[...], q2[...]),
        scales_of(place, kvs[0], kv2[0]),
        scales_of(place, kvs[1], kv2[1]),
        scales_of(place, os[...], o2[...]),
    ]
    parts = [
        p if p.shape[0] % 8 == 0 else jnp.concatenate([p, jnp.zeros((8 - p.shape[0] % 8, height), F32)])
        for p in parts
    ]
    absmax = jnp.concatenate(parts)
    starts = [sum(p.shape[0] for p in parts[:n]) for n in range(4)]
    absmax = absmax.T
    lane = lax.broadcasted_iota(jnp.int32, (height, 128), 1)

    def scaled(codes, block):
        scale = jnp.where(lane < QBLOCK, absmax[:, block : block + 1], absmax[:, block + 1 : block + 2])
        return (levels_of(codes) * scale).astype(BF)

    for j in range(q_width // 128):
        at = slice(j * 128, (j + 1) * 128)
        qkv_out[:, at] = scaled(q_ref[:, at], 2 * j)
        o_out[:, at] = scaled(o_ref[:, at], starts[3] + 2 * j)
    for j in range(kv_width // 128):
        for part in range(2):
            to = q_width + (2 * j + part) * 128
            codes = kv_ref[part, :, j * 128 : (j + 1) * 128]
            qkv_out[:, to : to + 128] = scaled(codes, starts[1 + part] + 2 * j)


def dequantize(codes, scales, row_start):
    q_codes, kv_codes, _ = codes
    height, q_width = q_codes.shape
    kv_width = kv_codes.shape[2]
    group = row_start // QGROUP
    last = jnp.minimum(group + 1, scales[3].shape[1] - 1)
    place = jnp.stack([group, last, (group + 1) * QGROUP - row_start]).astype(jnp.int32)
    return pl.pallas_call(
        dequantize_kernel,
        out_shape=(
            jax.ShapeDtypeStruct((height, q_width + 2 * kv_width), BF),
            jax.ShapeDtypeStruct((height, q_width), BF),
        ),
        in_specs=[pl.BlockSpec(memory_space=pltpu.SMEM)]
        + [pl.BlockSpec(memory_space=pltpu.VMEM)] * 9,
        name="dequantize",
    )(place, *codes, *scales)


def rope_tables(positions):
    half = HEAD_SIZE // 2
    exponent = jnp.arange(half, dtype=F32) * (2.0 / HEAD_SIZE)
    frequency = jnp.power(F32(ROPE_BASE), -exponent)
    angle = positions.astype(F32)[:, None] * frequency[None, :]
    return (jnp.cos(angle), jnp.sin(angle))


def rotate(heads, cosine, sine):
    half = heads.shape[-1] // 2
    first = heads[..., :half]
    second = heads[..., half:]
    across = cosine[:, None, :]
    along = sine[:, None, :]
    return jnp.concatenate(
        [first * across - second * along, second * across + first * along], axis=-1
    )


def head_norm(heads, gain):
    scale = lax.rsqrt(jnp.mean(heads * heads, axis=-1, keepdims=True) + EPSILON)
    return (heads * scale * gain, scale)


def head_norm_back(heads, scale, gain, grad):
    weighted = grad * gain
    inner = jnp.mean(weighted * heads, axis=-1, keepdims=True)
    return scale * weighted - scale**3 * heads * inner


def mxu(a, b, ca, cb):
    return lax.dot_general(a, b, (((ca,), (cb,)), ((), ())), preferred_element_type=F32)


def side_by_side(ref):
    return jnp.concatenate([ref[:HEAD_SIZE, :], ref[HEAD_SIZE:, :]], axis=1)


def weights_of(first_key, blocks, queries):
    weights, total = [], None
    for b, block in enumerate(blocks):
        keys, count = block.shape[0], queries.shape[1] // 2
        scores = mxu(block[:, :HEAD_SIZE], queries, 1, 0) * SCORE_SCALE
        e = jnp.exp(scores)
        key = lax.broadcasted_iota(jnp.int32, e.shape, 0)
        query = lax.broadcasted_iota(jnp.int32, e.shape, 1) % count
        if b == 0:
            e = jnp.where((key > query) & (first_key <= 0), e, 0.0)
        elif b == len(blocks) - 1:
            e = jnp.where(key <= query, e, 0.0)
        else:
            e = jnp.where(key + b * keys >= first_key, e, 0.0)
        part = jnp.sum(e, axis=0, keepdims=True)
        total = part if total is None else total + part
        weights.append(e)
    return weights, total


def forward_kernel(first_key, q_ref, *refs):
    blocks, out = refs[:-1], refs[-1]
    queries = side_by_side(q_ref)
    count = q_ref.shape[1]
    weights, total = weights_of(first_key[0], blocks, queries)
    inverse = 1.0 / total
    mixed = None
    for block, e in zip(blocks, weights):
        term = mxu(block[:, HEAD_SIZE:], (e * inverse).astype(BF), 0, 0)
        mixed = term if mixed is None else mixed + term
    mixed = mixed.astype(BF)
    out[:HEAD_SIZE, :] = mixed[:, :count]
    out[HEAD_SIZE:, :] = mixed[:, count:]


def backward_kernel(first_key, q_ref, grad_ref, *refs):
    n = (len(refs) - 1) // 2
    blocks, q_out, outs = refs[:n], refs[n], refs[n + 1 :]
    queries, grads = side_by_side(q_ref), side_by_side(grad_ref)
    count = q_ref.shape[1]
    weights, total = weights_of(first_key[0], blocks, queries)
    inverse = 1.0 / total
    inner, from_values = None, []
    for block, e in zip(blocks, weights):
        g = mxu(block[:, HEAD_SIZE:], grads, 1, 0)
        part = jnp.sum(e * inverse * g, axis=0, keepdims=True)
        inner = part if inner is None else inner + part
        from_values.append(g)
    q_grad = None
    for block, e, g, out in zip(blocks, weights, from_values, outs):
        p = e * inverse
        score_grad = (p * (g - inner) * SCORE_SCALE).astype(BF)
        out[:, HEAD_SIZE:] = mxu(p.astype(BF), grads, 1, 1).astype(out.dtype)
        out[:, :HEAD_SIZE] = mxu(score_grad, queries, 1, 1).astype(out.dtype)
        term = mxu(block[:, :HEAD_SIZE], score_grad, 0, 0)
        q_grad = term if q_grad is None else q_grad + term
    q_out[:HEAD_SIZE, :] = q_grad[:, :count]
    q_out[HEAD_SIZE:, :] = q_grad[:, count:]


def attention_call(kernel, first_key, transposed, blocks, outs):
    count = transposed[0].shape[1]
    row = pl.BlockSpec((2 * HEAD_SIZE, count), lambda g: (g, 0))
    column = pl.BlockSpec((count, 2 * HEAD_SIZE), lambda g: (0, g))
    kinds = [row if o.shape[1] == count else column for o in outs]
    return pl.pallas_call(
        kernel,
        grid=(blocks[0].shape[1] // (2 * HEAD_SIZE),),
        out_shape=outs,
        in_specs=[pl.BlockSpec(memory_space=pltpu.SMEM)]
        + [row] * len(transposed)
        + [column] * len(blocks),
        out_specs=kinds,
    )(first_key, *transposed, *blocks)


def unrotated(grad, across, along):
    return grad * across + pltpu.roll(grad, HEAD_SIZE // 2, 1) * along


def query_back_kernel(grad, rows, across, along, gain, up, back, small):
    mix, products = None, None
    for h in range(rows.shape[1] // HEAD_SIZE):
        at = slice(h * HEAD_SIZE, (h + 1) * HEAD_SIZE)
        heads = rows[:, at]
        scale = lax.rsqrt(jnp.mean(heads * heads, axis=-1, keepdims=True) + EPSILON)
        g = unrotated(grad[at, :].T, across[...], along[...])
        b = head_norm_back(heads, scale, gain[...], g).astype(BF)
        back[:, at] = b
        m, p = mxu(up[:, at], b, 1, 1), b.astype(F32) * heads
        mix, products = (m, p) if mix is None else (mix + m, products + p)
    rank, count = mix.shape
    small[:rank, :] = mix
    small[rank:, :] = jnp.broadcast_to(jnp.sum(products.T, axis=0, keepdims=True), (8, count))


def key_value_back_kernel(*refs):
    own, arrived = refs[0], refs[1:-7]
    rows, across, along, gain, up, back, small = refs[-7:]
    mixes, products = [None, None], None
    for h in range(rows.shape[1] // HEAD_SIZE):
        at = slice(h * HEAD_SIZE, (h + 1) * HEAD_SIZE)
        g = own[:, at]
        for a in arrived:
            g = g + a[:, at].astype(F32)
        heads = rows[:, at]
        if h % 2 == 0:
            scale = lax.rsqrt(jnp.mean(heads * heads, axis=-1, keepdims=True) + EPSILON)
            g = unrotated(g, across[...], along[...])
            g = head_norm_back(heads, scale, gain[...], g)
        b = g.astype(BF)
        back[:, at] = b
        m, p = mxu(up[:, at], b, 1, 1), b.astype(F32) * heads
        mixes[h % 2] = m if mixes[h % 2] is None else mixes[h % 2] + m
        products = p if products is None else products + p
    rank, count = mixes[0].shape
    small[:rank, :] = mixes[0]
    small[rank : 2 * rank, :] = mixes[1]
    small[2 * rank :, :] = jnp.broadcast_to(jnp.sum(products.T, axis=0, keepdims=True), (8, count))


def adapter_kernel(smalls, normed, up_grad, q_up, down_grad, low, kv_back, out, mixes_out, inner_out, buf):
    rank = q_up.shape[0]
    total = smalls[0]
    for i in range(1, smalls.shape[0]):
        total = total + smalls[i]
    mixes = jnp.concatenate([total[:rank], total[rank + 8 : 3 * rank + 8]]).astype(BF)
    mixes_out[...] = mixes
    inner_out[...] = total[rank : rank + 8] + total[3 * rank + 8 :]
    buf[: 3 * rank, :] = ADAPTER_SCALE * mxu(mixes, normed[...], 1, 1)
    buf[3 * rank : 4 * rank, :] = up_grad[...]
    kv = ADAPTER_SCALE * mxu(low[rank:, :], kv_back[...], 1, 0)
    row, extra = slice(4 * rank, 5 * rank), slice(5 * rank, 6 * rank)
    at = q_up.shape[1]
    buf[row, :at] = q_up[...]
    for h in range(kv_back.shape[1] // HEAD_SIZE):
        here = slice(h * HEAD_SIZE, (h + 1) * HEAD_SIZE)
        which = h % 2
        buf[row, at : at + HEAD_SIZE] = kv[which * rank : (which + 1) * rank, here]
        at += HEAD_SIZE
    half = down_grad.shape[1] // 2
    buf[row, at : at + half] = down_grad[:, :half]
    buf[row, at + half :] = jnp.zeros((rank, buf.shape[1] - at - half), F32)
    buf[extra, :half] = down_grad[:, half:]
    buf[extra, half:] = jnp.zeros((rank, buf.shape[1] - half), F32)
    each = out.shape[1]
    for i in range(out.shape[0]):
        out[i] = buf[i * each : (i + 1) * each, :]


def whole(kernel, outs, arrays, scratch=()):
    return pl.pallas_call(
        kernel,
        out_shape=outs,
        in_specs=[pl.BlockSpec(memory_space=pltpu.VMEM)] * len(arrays),
        out_specs=[pl.BlockSpec(memory_space=pltpu.VMEM)] * len(outs),
        scratch_shapes=list(scratch),
    )(*arrays)


def into_kernel(piece, own, other, back, out):
    out[0] = mxu(own[...], back[...], 1, 1).astype(out.dtype)
    out[1] = mxu(other[...], back[...], 1, 1).astype(out.dtype)


def into_piece(own, other, back, piece, rows, dtype):
    half = own.shape[0] // 4
    steps = half // rows
    weight = pl.BlockSpec((rows, own.shape[1]), lambda i, p: (p[0] * steps + i, 0))
    count = back.shape[0]
    return pl.pallas_call(
        into_kernel,
        out_shape=jax.ShapeDtypeStruct((2, half, count), dtype),
        grid_spec=pltpu.PrefetchScalarGridSpec(
            num_scalar_prefetch=1,
            grid=(steps,),
            in_specs=[weight, weight, pl.BlockSpec(back.shape, lambda i, p: (0, 0))],
            out_specs=pl.BlockSpec((2, rows, count), lambda i, p: (0, i, 0)),
        ),
        name="into_piece",
    )(piece, own, other, back)


def gathered_pieces(own, xl, c):
    other = swap(own, "xl")
    pair = jnp.stack([jnp.where(xl == 0, own, other), jnp.where(xl == 0, other, own)])
    far = swap(pair, "c")
    return jnp.stack([jnp.where(c == 0, pair, far), jnp.where(c == 0, far, pair)], axis=1)


def on_device(
    tokens,
    out_grad,
    in_gain,
    query_gain,
    key_gain,
    post_gain,
    q_codes,
    q_scodes,
    q_second,
    kv_codes,
    kv_scodes,
    kv_second,
    o_codes,
    o_scodes,
    o_second,
    q_down,
    query_up,
    kv_down,
    key_value_up,
    output_down,
    output_up,
):
    count, share = tokens.shape
    _, _, xh = (lax.axis_index(a) for a in CTX)
    xl, c = (lax.axis_index(a) for a in TP)
    ctx_rank = lax.axis_index(CTX)
    column_start = lax.axis_index(TP) * share
    rows = q_codes.shape[0]
    row_start = ctx_rank * rows
    blocks = share // rows
    ny, nz = lax.axis_size("y"), lax.axis_size("z")
    q_width = query_up.shape[1]
    kv_width = key_value_up.shape[2]
    q_heads_here = q_width // HEAD_SIZE
    kv_heads_here = kv_width // HEAD_SIZE

    turned = (0, 2, 1)
    scales = [q_scodes.T, kv_scodes.transpose(turned), o_scodes.T]
    scales += [q_second.T, kv_second.transpose(turned), o_second.T]
    qkv_part, o_part = dequantize([q_codes, kv_codes, o_codes], scales, row_start)
    own_matrix = lax.all_gather(qkv_part, ("y", "z"), axis=0, tiled=True)

    tokens_t = tokens.T
    mine = tokens_t.reshape(blocks // 2, 2, rows, count)
    keep = lax.dynamic_index_in_dim(mine, xh, 1, False)
    give = lax.dynamic_index_in_dim(mine, 1 - xh, 1, False)
    pair = jnp.concatenate([keep, swap(give, "xh")], axis=-1)
    wide = gathered_pieces(pair, xl, c).reshape(ny, nz, rows, 2 * count).astype(F32)
    partial_sum = jnp.sum(wide * wide, axis=(0, 1, 2))
    other_sum = swap(partial_sum.reshape(4, -1), "xh").reshape(-1)
    square_sum = partial_sum + jnp.roll(other_sum, count)
    pair_scale = lax.rsqrt(square_sum / D + EPSILON)

    def parity(a, which):
        return lax.dynamic_index_in_dim(a.reshape(ny, nz, 2, rows, -1), which, 2, False)

    normed = (wide * pair_scale * parity(in_gain, xh)).astype(BF).reshape(D // 2, -1)
    downs = jnp.concatenate([q_down, kv_down[0], kv_down[1]], axis=1)
    downs_parity = parity(downs, xh).reshape(D // 2, -1)
    low_pair = dot_f32(normed, downs_parity, 0, 0)
    low_sum = low_pair[:count] + swap(low_pair[count:], "xh")
    low = low_sum.astype(BF)
    rank = q_down.shape[1]
    query_lowrank, _, _ = (
        low[:, i * rank : (i + 1) * rank] for i in range(3)
    )
    row_scale = pair_scale[:count]
    qkv_pair = dot_f32(normed, own_matrix, 0, 0)
    far_kv = swap(qkv_pair[count:, q_width:].astype(BF), "xh")
    kv_sum = qkv_pair[:count, q_width:] + far_kv.astype(F32)
    far_q = swap(after(qkv_pair[count:, :q_width].astype(BF), far_kv), "xh")
    q_sum = qkv_pair[:count, :q_width] + far_q.astype(F32)

    def of_heads(both, which):
        return both.reshape(-1, kv_heads_here, 2, HEAD_SIZE)[:, :, which].reshape(-1, kv_width)

    def interleaved(first, second):
        heads = (-1, kv_heads_here, HEAD_SIZE)
        both = jnp.stack([first.reshape(heads), second.reshape(heads)], axis=2)
        return both.reshape(first.shape[0], 2 * kv_width)

    kv_up = interleaved(key_value_up[0], key_value_up[1])
    nothing = jnp.zeros_like(key_value_up[0])
    kv_up_apart = jnp.concatenate(
        [interleaved(key_value_up[0], nothing), interleaved(nothing, key_value_up[1])]
    )
    kv_total = kv_sum + ADAPTER_SCALE * dot_f32(low[:, rank:], kv_up_apart, 1, 0)
    key = of_heads(kv_total, 0)
    value_rows = of_heads(kv_total, 1).astype(BF)
    query_rows = q_sum + ADAPTER_SCALE * dot_f32(query_lowrank, query_up, 1, 0)

    query_pos = ctx_rank * count + jnp.arange(count, dtype=jnp.int32)
    cosine, sine = rope_tables(query_pos)
    key_head_rows = key.reshape(count, kv_heads_here, HEAD_SIZE)
    k_normed, _ = head_norm(key_head_rows, key_gain)
    k_rot = rotate(k_normed, cosine, sine).astype(BF)
    kv_rows = jnp.stack([k_rot, value_rows.reshape(k_rot.shape)], axis=2).reshape(count, -1)
    steps = WINDOW_TOKENS // count
    window = []
    for s in range(steps, 0, -1):
        window.append(shifted(kv_rows, s))
    window.append(kv_rows)
    first_key = (WINDOW_TOKENS - ctx_rank * count).astype(jnp.int32).reshape(1)
    q_heads = query_rows.reshape(count, q_heads_here, HEAD_SIZE)
    q_normed, _ = head_norm(q_heads, query_gain)
    q_rot = rotate(q_normed, cosine, sine).astype(BF)

    q_turned = q_rot.reshape(count, q_width).T

    o_swapped = swap(after(o_part, low), "xh")
    qkv_other = swap(after(qkv_part, far_kv), "xh")
    o_both = jnp.concatenate(
        [jnp.where(xh == 0, o_part, o_swapped), jnp.where(xh == 0, o_swapped, o_part)]
    )
    output_matrix = lax.all_gather(after(o_both, own_matrix), ("y", "z"), axis=0, tiled=True)
    other_matrix = lax.all_gather(after(qkv_other, output_matrix), ("y", "z"), axis=0, tiled=True)
    out_grad_t = out_grad.T
    out_grad_full = gathered_pieces(after(out_grad_t, partial_sum), xl, c)

    (attended,) = attention_call(
        forward_kernel, first_key, [q_turned], window, [jax.ShapeDtypeStruct((q_width, count), BF)]
    )

    low_out_part = dot_f32(output_down, attended, 0, 0).astype(BF)
    out_rows = output_matrix.reshape(2, 2 * share, q_width)
    up_rows = output_up.T.reshape(2, 2 * share, rank)
    sums, low_total = [], None

    def number(a, b):
        return (a * 2 + b).astype(jnp.int32).reshape(1)

    for j in range(2):
        part = dot_f32(out_rows[j], attended, 1, 0) + ADAPTER_SCALE * dot_f32(
            up_rows[j], low_out_part, 1, 0
        )
        part = part.reshape(2, share, count)
        keep = lax.dynamic_index_in_dim(part, c, 0, False)
        give = lax.dynamic_index_in_dim(part, 1 - c, 0, False)
        if j == 0:
            keep = jnp.concatenate([keep, low_out_part.astype(F32)])
            give = jnp.concatenate([give, low_out_part.astype(F32)])
        chip = (keep + swap(give.astype(BF), "c").astype(F32)).astype(BF)
        total = (chip.astype(F32) + swap(chip, "xl").astype(F32)).astype(BF)
        if j == 0:
            low_total = total[share:]
            total = total[:share]
        far = swap(total, "c")
        sums.append(jnp.stack([jnp.where(c == 0, total, far), jnp.where(c == 0, far, total)]))
    out_total = jnp.stack(sums).astype(F32)
    output_lowrank = low_total.T
    gain_full = post_gain.reshape(2, 2, share, 1)
    weighted_out = out_grad_full.astype(F32) * gain_full
    out_scale = lax.rsqrt(jnp.sum(out_total * out_total, axis=(0, 1, 2)) / D + EPSILON)
    out_inner = jnp.sum(weighted_out * out_total, axis=(0, 1, 2)) / D
    grad_full = (out_scale * weighted_out - out_scale**3 * out_total * out_inner).astype(BF)
    output_gradient = grad_full.reshape(D, count)
    out_mine = lax.dynamic_slice_in_dim(out_total.reshape(D, count), column_start, share, 0)
    post_mine = lax.dynamic_slice_in_dim(post_gain, column_start, share, 0)[:, None]
    mixed = (tokens_t.astype(F32) + out_mine * out_scale * post_mine).astype(BF)

    output_mixture = dot_f32(output_gradient, output_up, 0, 1).astype(BF)
    grad_mine = lax.dynamic_slice_in_dim(output_gradient, column_start, share, 0)
    output_up_gradient = ADAPTER_SCALE * dot_f32(output_lowrank, grad_mine, 0, 1)
    output_down_gradient = ADAPTER_SCALE * dot_f32(output_mixture, attended, 0, 1)
    attended_gradient = (
        dot_f32(output_matrix, output_gradient, 0, 0)
        + ADAPTER_SCALE * dot_f32(output_down, output_mixture, 1, 1)
    ).astype(BF)
    query_grad, *window_grad = attention_call(
        backward_kernel,
        first_key,
        [q_turned, attended_gradient],
        window,
        [jax.ShapeDtypeStruct((q_width, count), F32)]
        + [jax.ShapeDtypeStruct((count, 2 * kv_width), BF)] * steps
        + [jax.ShapeDtypeStruct((count, 2 * kv_width), F32)],
    )
    across = jnp.concatenate([cosine, cosine], axis=1)
    along = jnp.concatenate([sine, -sine], axis=1)
    query_back, small_q = whole(
        query_back_kernel,
        [
            jax.ShapeDtypeStruct((count, q_width), BF),
            jax.ShapeDtypeStruct((rank + 8, count), F32),
        ],
        [query_grad, query_rows, across, along, query_gain[None], query_up],
    )
    arrived = [shifted(window_grad[steps - s], -s) for s in range(steps, 0, -1)]
    kv_back, small_kv = whole(
        key_value_back_kernel,
        [
            jax.ShapeDtypeStruct((count, 2 * kv_width), BF),
            jax.ShapeDtypeStruct((2 * rank + 8, count), F32),
        ],
        [window_grad[steps], *arrived, kv_total, across, along, key_gain[None], kv_up],
    )
    smalls = lax.all_gather(jnp.concatenate([small_q, small_kv]), TP)

    in_gain_mine = lax.dynamic_slice_in_dim(in_gain, column_start, share, 0)[:, None]
    tokens_wide = tokens_t.astype(F32)
    normed_mine = (tokens_wide * row_scale * in_gain_mine).astype(BF)
    devices = lax.axis_size(CTX)
    each = 6 * rank // devices
    parts, mixes, inner = whole(
        adapter_kernel,
        [
            jax.ShapeDtypeStruct((devices, each, share), F32),
            jax.ShapeDtypeStruct((3 * rank, count), BF),
            jax.ShapeDtypeStruct((8, count), F32),
        ],
        [
            smalls,
            normed_mine,
            output_up_gradient,
            ADAPTER_SCALE * dot_f32(query_lowrank, query_back, 0, 0),
            output_down_gradient,
            low.T,
            kv_back,
        ],
        [pltpu.VMEM((6 * rank, share), F32)],
    )
    in_inner = inner[0] / (row_scale * D)
    sums_arrived = lax.all_to_all(parts, CTX, 0, 0, tiled=True)

    back = after(jnp.concatenate([query_back, kv_back], axis=1), parts)

    def into(a, b, dtype):
        return into_piece(own_matrix, other_matrix, back, number(a, b), 2 * rows, dtype)

    give_far = into(1 - xl, 1 - c, BF)
    give_near = into(xl, 1 - c, BF)
    keep_far = into(1 - xl, c, F32)
    keep_near = into(xl, c, F32)
    to_chip = (keep_far + swap(give_far, "c").astype(F32)).astype(BF)
    far_into = swap(to_chip, "xl")
    into_mine = keep_near + swap(give_near, "c").astype(F32) + far_into.astype(F32)
    halves = into_mine.reshape(2, nz, rows, count)
    first = jnp.where(xh == 0, halves[0], halves[1])
    last = jnp.where(xh == 0, halves[1], halves[0])
    into_mine = jnp.stack([first, last], axis=1).reshape(share, count)

    downs_mine = lax.dynamic_slice_in_dim(downs, column_start, share, 0)
    normalized_gradient = into_mine + ADAPTER_SCALE * dot_f32(downs_mine, mixes, 1, 0)
    weighted_in = normalized_gradient * in_gain_mine
    tokens_grad = (
        out_grad_t.astype(F32)
        + row_scale * weighted_in
        - row_scale**3 * tokens_wide * in_inner
    )
    in_projection = (float(D) ** 0.5 * row_scale * in_inner)[:, None]
    chunk = jnp.sum(sums_arrived, axis=0)
    spread = jnp.broadcast_to(chunk[None], (devices, *chunk.shape))
    summed = lax.all_to_all(spread, CTX, 0, 0, tiled=True).reshape(-1, share)
    cut = 4 * rank
    wide_sums = lax.all_gather(summed[:cut].astype(BF), TP)
    wide_sums = jnp.moveaxis(wide_sums, 0, 1).reshape(cut, D).astype(F32)
    narrow = summed[cut : 5 * rank]
    kv_end = q_width + 2 * kv_width
    kv_up_gradient = narrow[:, q_width:kv_end].reshape(rank, kv_heads_here, 2, HEAD_SIZE)
    kv_up_gradient = kv_up_gradient.transpose(2, 0, 1, 3).reshape(2, rank, kv_width)
    output_down_gradient = jnp.concatenate(
        [narrow[:, kv_end : kv_end + q_width // 2], summed[5 * rank :, : q_width // 2]], axis=1
    ).T
    return (
        mixed.T,
        tokens_grad.T,
        wide_sums[:rank].T,
        narrow[:, :q_width],
        jnp.stack([wide_sums[rank : 2 * rank].T, wide_sums[2 * rank : 3 * rank].T]),
        kv_up_gradient,
        output_down_gradient,
        wide_sums[3 * rank :],
        in_projection,
    )


def solution(mesh):
    torus = Mesh(mesh.devices.reshape(4, 4, 2, 2, 2), (*CTX, *TP))

    return jax.shard_map(
        on_device,
        mesh=torus,
        in_specs=(
            P(CTX, TP),
            P(CTX, TP),
            P(),
            P(),
            P(),
            P(),
            P(CTX, TP),
            P(CTX, TP),
            P(None, TP),
            P(None, CTX, TP),
            P(None, CTX, TP),
            P(None, None, TP),
            P(CTX, TP),
            P(CTX, TP),
            P(None, TP),
            P(),
            P(None, TP),
            P(),
            P(None, None, TP),
            P(TP, None),
            P(),
        ),
        out_specs=(
            P(CTX, TP),
            P(CTX, TP),
            P(),
            P(None, TP),
            P(),
            P(None, None, TP),
            P(TP, None),
            P(),
            P(CTX, None),
        ),
        check_vma=False,
    )
```

```python
import jax
import jax.numpy as jnp
from jax import lax
from jax.experimental import pallas as pl
from jax.experimental.pallas import tpu as pltpu
from jax.sharding import Mesh
from jax.sharding import PartitionSpec as P

D = 5376
HEAD_SIZE = 128
WINDOW_TOKENS = 1024
QBLOCK = 64
QGROUP = 256
CTX = ("y", "z", "xh")
TP = ("xl", "c")
NORMAL_FLOAT = (
    -1.0,
    -0.6961928009986877,
    -0.5250730514526367,
    -0.39491748809814453,
    -0.28444138169288635,
    -0.18477343022823334,
    -0.09105003625154495,
    0.0,
    0.07958029955625534,
    0.16093020141124725,
    0.24611230194568634,
    0.33791524171829224,
    0.44070982933044434,
    0.5626170039176941,
    0.7229568362236023,
    1.0,
)
EPSILON = 1e-06
ADAPTER_SCALE = 2.0
SCORE_SCALE = 168.0 ** (-0.5)
ROPE_BASE = 10000.0
BF = jnp.bfloat16
F32 = jnp.float32


def swap(x, axis):
    return lax.ppermute(x, axis, [(0, 1), (1, 0)])


def after(arrays, *done):
    return lax.optimization_barrier((arrays, done))[0]


def shifted(x, by):
    n = lax.axis_size(CTX)
    return lax.ppermute(x, CTX, [(i, i + by) for i in range(n) if 0 <= i + by < n])


def dot_f32(a, b, ca, cb):
    return lax.dot_general(a, b, (((ca,), (cb,)), ((), ())), preferred_element_type=F32)


def levels_of(codes):
    bits = [(codes & (1 << b)) != 0 for b in range(4)]
    table = [F32(v) for v in NORMAL_FLOAT]
    for bit in bits:
        table = [jnp.where(bit, high, low) for low, high in zip(table[::2], table[1::2])]
    return table[0]


def scales_of(place, scodes, second):
    group = lax.broadcasted_iota(jnp.int32, second.shape, 1)
    first = jnp.sum(jnp.where(group == place[0], second, 0.0), axis=1, keepdims=True)
    last = jnp.sum(jnp.where(group == place[1], second, 0.0), axis=1, keepdims=True)
    row = lax.broadcasted_iota(jnp.int32, scodes.shape, 1)
    return jnp.where(row < place[2], first, last) * ((scodes.astype(F32) + 1.0) / 256.0)


def dequantize_kernel(place, q_ref, kv_ref, o_ref, qs, kvs, os, q2, kv2, o2, qkv_out, o_out):
    height, q_width = q_ref.shape
    kv_width = kv_ref.shape[2]
    parts = [
        scales_of(place, qs[...], q2[...]),
        scales_of(place, kvs[0], kv2[0]),
        scales_of(place, kvs[1], kv2[1]),
        scales_of(place, os[...], o2[...]),
    ]
    parts = [
        p if p.shape[0] % 8 == 0 else jnp.concatenate([p, jnp.zeros((8 - p.shape[0] % 8, height), F32)])
        for p in parts
    ]
    absmax = jnp.concatenate(parts)
    starts = [sum(p.shape[0] for p in parts[:n]) for n in range(4)]
    absmax = absmax.T
    lane = lax.broadcasted_iota(jnp.int32, (height, 128), 1)

    def scaled(codes, block):
        scale = jnp.where(lane < QBLOCK, absmax[:, block : block + 1], absmax[:, block + 1 : block + 2])
        return (levels_of(codes) * scale).astype(BF)

    for j in range(q_width // 128):
        at = slice(j * 128, (j + 1) * 128)
        qkv_out[:, at] = scaled(q_ref[:, at], 2 * j)
        o_out[:, at] = scaled(o_ref[:, at], starts[3] + 2 * j)
    for j in range(kv_width // 128):
        for part in range(2):
            to = q_width + (2 * j + part) * 128
            codes = kv_ref[part, :, j * 128 : (j + 1) * 128]
            qkv_out[:, to : to + 128] = scaled(codes, starts[1 + part] + 2 * j)


def dequantize(codes, scales, row_start):
    q_codes, kv_codes, _ = codes
    height, q_width = q_codes.shape
    kv_width = kv_codes.shape[2]
    group = row_start // QGROUP
    last = jnp.minimum(group + 1, scales[3].shape[1] - 1)
    place = jnp.stack([group, last, (group + 1) * QGROUP - row_start]).astype(jnp.int32)
    return pl.pallas_call(
        dequantize_kernel,
        out_shape=(
            jax.ShapeDtypeStruct((height, q_width + 2 * kv_width), BF),
            jax.ShapeDtypeStruct((height, q_width), BF),
        ),
        in_specs=[pl.BlockSpec(memory_space=pltpu.SMEM)]
        + [pl.BlockSpec(memory_space=pltpu.VMEM)] * 9,
        name="dequantize",
    )(place, *codes, *scales)


def rope_tables(positions):
    half = HEAD_SIZE // 2
    exponent = jnp.arange(half, dtype=F32) * (2.0 / HEAD_SIZE)
    frequency = jnp.power(F32(ROPE_BASE), -exponent)
    angle = positions.astype(F32)[:, None] * frequency[None, :]
    return (jnp.cos(angle), jnp.sin(angle))


def rotate(heads, cosine, sine):
    half = heads.shape[-1] // 2
    first = heads[..., :half]
    second = heads[..., half:]
    across = cosine[:, None, :]
    along = sine[:, None, :]
    return jnp.concatenate(
        [first * across - second * along, second * across + first * along], axis=-1
    )


def head_norm(heads, gain):
    scale = lax.rsqrt(jnp.mean(heads * heads, axis=-1, keepdims=True) + EPSILON)
    return (heads * scale * gain, scale)


def head_norm_back(heads, scale, gain, grad):
    weighted = grad * gain
    inner = jnp.mean(weighted * heads, axis=-1, keepdims=True)
    return scale * weighted - scale**3 * heads * inner


def mxu(a, b, ca, cb):
    return lax.dot_general(a, b, (((ca,), (cb,)), ((), ())), preferred_element_type=F32)


def side_by_side(ref):
    return jnp.concatenate([ref[:HEAD_SIZE, :], ref[HEAD_SIZE:, :]], axis=1)


def weights_of(first_key, blocks, queries):
    weights, total = [], None
    for b, block in enumerate(blocks):
        keys, count = block.shape[0], queries.shape[1] // 2
        scores = mxu(block[:, :HEAD_SIZE], queries, 1, 0) * SCORE_SCALE
        e = jnp.exp(scores)
        key = lax.broadcasted_iota(jnp.int32, e.shape, 0)
        query = lax.broadcasted_iota(jnp.int32, e.shape, 1) % count
        if b == 0:
            e = jnp.where((key > query) & (first_key <= 0), e, 0.0)
        elif b == len(blocks) - 1:
            e = jnp.where(key <= query, e, 0.0)
        else:
            e = jnp.where(key + b * keys >= first_key, e, 0.0)
        part = jnp.sum(e, axis=0, keepdims=True)
        total = part if total is None else total + part
        weights.append(e)
    return weights, total


def forward_kernel(first_key, q_ref, *refs):
    blocks, out = refs[:-1], refs[-1]
    queries = side_by_side(q_ref)
    count = q_ref.shape[1]
    weights, total = weights_of(first_key[0], blocks, queries)
    inverse = 1.0 / total
    mixed = None
    for block, e in zip(blocks, weights):
        term = mxu(block[:, HEAD_SIZE:], (e * inverse).astype(BF), 0, 0)
        mixed = term if mixed is None else mixed + term
    mixed = mixed.astype(BF)
    out[:HEAD_SIZE, :] = mixed[:, :count]
    out[HEAD_SIZE:, :] = mixed[:, count:]


def backward_kernel(first_key, q_ref, grad_ref, *refs):
    n = (len(refs) - 1) // 2
    blocks, q_out, outs = refs[:n], refs[n], refs[n + 1 :]
    queries, grads = side_by_side(q_ref), side_by_side(grad_ref)
    count = q_ref.shape[1]
    weights, total = weights_of(first_key[0], blocks, queries)
    inverse = 1.0 / total
    inner, from_values = None, []
    for block, e in zip(blocks, weights):
        g = mxu(block[:, HEAD_SIZE:], grads, 1, 0)
        part = jnp.sum(e * inverse * g, axis=0, keepdims=True)
        inner = part if inner is None else inner + part
        from_values.append(g)
    q_grad = None
    for block, e, g, out in zip(blocks, weights, from_values, outs):
        p = e * inverse
        score_grad = (p * (g - inner) * SCORE_SCALE).astype(BF)
        out[:, HEAD_SIZE:] = mxu(p.astype(BF), grads, 1, 1).astype(out.dtype)
        out[:, :HEAD_SIZE] = mxu(score_grad, queries, 1, 1).astype(out.dtype)
        term = mxu(block[:, :HEAD_SIZE], score_grad, 0, 0)
        q_grad = term if q_grad is None else q_grad + term
    q_out[:HEAD_SIZE, :] = q_grad[:, :count]
    q_out[HEAD_SIZE:, :] = q_grad[:, count:]


def attention_call(kernel, first_key, transposed, blocks, outs):
    count = transposed[0].shape[1]
    row = pl.BlockSpec((2 * HEAD_SIZE, count), lambda g: (g, 0))
    column = pl.BlockSpec((count, 2 * HEAD_SIZE), lambda g: (0, g))
    kinds = [row if o.shape[1] == count else column for o in outs]
    return pl.pallas_call(
        kernel,
        grid=(blocks[0].shape[1] // (2 * HEAD_SIZE),),
        out_shape=outs,
        in_specs=[pl.BlockSpec(memory_space=pltpu.SMEM)]
        + [row] * len(transposed)
        + [column] * len(blocks),
        out_specs=kinds,
    )(first_key, *transposed, *blocks)


def unrotated(grad, across, along):
    return grad * across + pltpu.roll(grad, HEAD_SIZE // 2, 1) * along


def query_back_kernel(grad, rows, across, along, gain, up, back, small):
    mix, products = None, None
    for h in range(rows.shape[1] // HEAD_SIZE):
        at = slice(h * HEAD_SIZE, (h + 1) * HEAD_SIZE)
        heads = rows[:, at]
        scale = lax.rsqrt(jnp.mean(heads * heads, axis=-1, keepdims=True) + EPSILON)
        g = unrotated(grad[at, :].T, across[...], along[...])
        b = head_norm_back(heads, scale, gain[...], g).astype(BF)
        back[:, at] = b
        m, p = mxu(up[:, at], b, 1, 1), b.astype(F32) * heads
        mix, products = (m, p) if mix is None else (mix + m, products + p)
    rank, count = mix.shape
    small[:rank, :] = mix
    small[rank:, :] = jnp.broadcast_to(jnp.sum(products.T, axis=0, keepdims=True), (8, count))


def key_value_back_kernel(*refs):
    own, arrived = refs[0], refs[1:-7]
    rows, across, along, gain, up, back, small = refs[-7:]
    mixes, products = [None, None], None
    for h in range(rows.shape[1] // HEAD_SIZE):
        at = slice(h * HEAD_SIZE, (h + 1) * HEAD_SIZE)
        g = own[:, at]
        for a in arrived:
            g = g + a[:, at].astype(F32)
        heads = rows[:, at]
        if h % 2 == 0:
            scale = lax.rsqrt(jnp.mean(heads * heads, axis=-1, keepdims=True) + EPSILON)
            g = unrotated(g, across[...], along[...])
            g = head_norm_back(heads, scale, gain[...], g)
        b = g.astype(BF)
        back[:, at] = b
        m, p = mxu(up[:, at], b, 1, 1), b.astype(F32) * heads
        mixes[h % 2] = m if mixes[h % 2] is None else mixes[h % 2] + m
        products = p if products is None else products + p
    rank, count = mixes[0].shape
    small[:rank, :] = mixes[0]
    small[rank : 2 * rank, :] = mixes[1]
    small[2 * rank :, :] = jnp.broadcast_to(jnp.sum(products.T, axis=0, keepdims=True), (8, count))


def adapter_kernel(smalls, normed, up_grad, q_up, down_grad, low, kv_back, out, mixes_out, inner_out, buf):
    rank = q_up.shape[0]
    total = smalls[0]
    for i in range(1, smalls.shape[0]):
        total = total + smalls[i]
    mixes = jnp.concatenate([total[:rank], total[rank + 8 : 3 * rank + 8]]).astype(BF)
    mixes_out[...] = mixes
    inner_out[...] = total[rank : rank + 8] + total[3 * rank + 8 :]
    buf[: 3 * rank, :] = ADAPTER_SCALE * mxu(mixes, normed[...], 1, 1)
    buf[3 * rank : 4 * rank, :] = up_grad[...]
    kv = ADAPTER_SCALE * mxu(low[rank:, :], kv_back[...], 1, 0)
    row, extra = slice(4 * rank, 5 * rank), slice(5 * rank, 6 * rank)
    at = q_up.shape[1]
    buf[row, :at] = q_up[...]
    for h in range(kv_back.shape[1] // HEAD_SIZE):
        here = slice(h * HEAD_SIZE, (h + 1) * HEAD_SIZE)
        which = h % 2
        buf[row, at : at + HEAD_SIZE] = kv[which * rank : (which + 1) * rank, here]
        at += HEAD_SIZE
    half = down_grad.shape[1] // 2
    buf[row, at : at + half] = down_grad[:, :half]
    buf[row, at + half :] = jnp.zeros((rank, buf.shape[1] - at - half), F32)
    buf[extra, :half] = down_grad[:, half:]
    buf[extra, half:] = jnp.zeros((rank, buf.shape[1] - half), F32)
    each = out.shape[1]
    for i in range(out.shape[0]):
        out[i] = buf[i * each : (i + 1) * each, :]


def whole(kernel, outs, arrays, scratch=()):
    return pl.pallas_call(
        kernel,
        out_shape=outs,
        in_specs=[pl.BlockSpec(memory_space=pltpu.VMEM)] * len(arrays),
        out_specs=[pl.BlockSpec(memory_space=pltpu.VMEM)] * len(outs),
        scratch_shapes=list(scratch),
    )(*arrays)


def into_kernel(piece, own, other, back, out):
    out[0] = mxu(own[...], back[...], 1, 1).astype(out.dtype)
    out[1] = mxu(other[...], back[...], 1, 1).astype(out.dtype)


def into_piece(own, other, back, piece, rows, dtype):
    half = own.shape[0] // 4
    steps = half // rows
    weight = pl.BlockSpec((rows, own.shape[1]), lambda i, p: (p[0] * steps + i, 0))
    count = back.shape[0]
    return pl.pallas_call(
        into_kernel,
        out_shape=jax.ShapeDtypeStruct((2, half, count), dtype),
        grid_spec=pltpu.PrefetchScalarGridSpec(
            num_scalar_prefetch=1,
            grid=(steps,),
            in_specs=[weight, weight, pl.BlockSpec(back.shape, lambda i, p: (0, 0))],
            out_specs=pl.BlockSpec((2, rows, count), lambda i, p: (0, i, 0)),
        ),
        name="into_piece",
    )(piece, own, other, back)


def gathered_pieces(own, xl, c):
    other = swap(own, "xl")
    pair = jnp.stack([jnp.where(xl == 0, own, other), jnp.where(xl == 0, other, own)])
    far = swap(pair, "c")
    return jnp.stack([jnp.where(c == 0, pair, far), jnp.where(c == 0, far, pair)], axis=1)


def on_device(
    tokens,
    out_grad,
    in_gain,
    query_gain,
    key_gain,
    post_gain,
    q_codes,
    q_scodes,
    q_second,
    kv_codes,
    kv_scodes,
    kv_second,
    o_codes,
    o_scodes,
    o_second,
    q_down,
    query_up,
    kv_down,
    key_value_up,
    output_down,
    output_up,
):
    count, share = tokens.shape
    _, _, xh = (lax.axis_index(a) for a in CTX)
    xl, c = (lax.axis_index(a) for a in TP)
    ctx_rank = lax.axis_index(CTX)
    column_start = lax.axis_index(TP) * share
    rows = q_codes.shape[0]
    row_start = ctx_rank * rows
    blocks = share // rows
    ny, nz = lax.axis_size("y"), lax.axis_size("z")
    q_width = query_up.shape[1]
    kv_width = key_value_up.shape[2]
    q_heads_here = q_width // HEAD_SIZE
    kv_heads_here = kv_width // HEAD_SIZE

    turned = (0, 2, 1)
    scales = [q_scodes.T, kv_scodes.transpose(turned), o_scodes.T]
    scales += [q_second.T, kv_second.transpose(turned), o_second.T]
    qkv_part, o_part = dequantize([q_codes, kv_codes, o_codes], scales, row_start)
    own_matrix = lax.all_gather(qkv_part, ("y", "z"), axis=0, tiled=True)

    tokens_t = tokens.T
    mine = tokens_t.reshape(blocks // 2, 2, rows, count)
    keep = lax.dynamic_index_in_dim(mine, xh, 1, False)
    give = lax.dynamic_index_in_dim(mine, 1 - xh, 1, False)
    pair = jnp.concatenate([keep, swap(give, "xh")], axis=-1)
    wide = gathered_pieces(pair, xl, c).reshape(ny, nz, rows, 2 * count).astype(F32)
    partial_sum = jnp.sum(wide * wide, axis=(0, 1, 2))
    other_sum = swap(partial_sum.reshape(4, -1), "xh").reshape(-1)
    square_sum = partial_sum + jnp.roll(other_sum, count)
    pair_scale = lax.rsqrt(square_sum / D + EPSILON)

    def parity(a, which):
        return lax.dynamic_index_in_dim(a.reshape(ny, nz, 2, rows, -1), which, 2, False)

    normed = (wide * pair_scale * parity(in_gain, xh)).astype(BF).reshape(D // 2, -1)
    downs = jnp.concatenate([q_down, kv_down[0], kv_down[1]], axis=1)
    downs_parity = parity(downs, xh).reshape(D // 2, -1)
    low_pair = dot_f32(normed, downs_parity, 0, 0)
    far_low = swap(low_pair[count:], "xh")
    low_sum = low_pair[:count] + far_low
    low = low_sum.astype(BF)
    rank = q_down.shape[1]
    query_lowrank, _, _ = (
        low[:, i * rank : (i + 1) * rank] for i in range(3)
    )
    row_scale = pair_scale[:count]
    qkv_pair = dot_f32(normed, own_matrix, 0, 0)
    far_kv = swap(qkv_pair[count:, q_width:].astype(BF), "xh")
    kv_sum = qkv_pair[:count, q_width:] + far_kv.astype(F32)
    far_q = swap(after(qkv_pair[count:, :q_width].astype(BF), far_kv), "xh")
    q_sum = qkv_pair[:count, :q_width] + far_q.astype(F32)

    def of_heads(both, which):
        return both.reshape(-1, kv_heads_here, 2, HEAD_SIZE)[:, :, which].reshape(-1, kv_width)

    def interleaved(first, second):
        heads = (-1, kv_heads_here, HEAD_SIZE)
        both = jnp.stack([first.reshape(heads), second.reshape(heads)], axis=2)
        return both.reshape(first.shape[0], 2 * kv_width)

    kv_up = interleaved(key_value_up[0], key_value_up[1])
    nothing = jnp.zeros_like(key_value_up[0])
    kv_up_apart = jnp.concatenate(
        [interleaved(key_value_up[0], nothing), interleaved(nothing, key_value_up[1])]
    )
    kv_total = kv_sum + ADAPTER_SCALE * dot_f32(low[:, rank:], kv_up_apart, 1, 0)
    key = of_heads(kv_total, 0)
    value_rows = of_heads(kv_total, 1).astype(BF)
    query_rows = q_sum + ADAPTER_SCALE * dot_f32(query_lowrank, query_up, 1, 0)

    query_pos = ctx_rank * count + jnp.arange(count, dtype=jnp.int32)
    cosine, sine = rope_tables(query_pos)
    key_head_rows = key.reshape(count, kv_heads_here, HEAD_SIZE)
    k_normed, _ = head_norm(key_head_rows, key_gain)
    k_rot = rotate(k_normed, cosine, sine).astype(BF)
    kv_rows = jnp.stack([k_rot, value_rows.reshape(k_rot.shape)], axis=2).reshape(count, -1)
    steps = WINDOW_TOKENS // count
    window = []
    for s in range(steps, 0, -1):
        window.append(shifted(kv_rows, s))
    window.append(kv_rows)
    first_key = (WINDOW_TOKENS - ctx_rank * count).astype(jnp.int32).reshape(1)
    q_heads = query_rows.reshape(count, q_heads_here, HEAD_SIZE)
    q_normed, _ = head_norm(q_heads, query_gain)
    q_rot = rotate(q_normed, cosine, sine).astype(BF)

    q_turned = q_rot.reshape(count, q_width).T

    o_swapped = swap(after(o_part, low_pair), "xh")
    qkv_other = swap(after(qkv_part, far_kv), "xh")
    o_both = jnp.concatenate(
        [jnp.where(xh == 0, o_part, o_swapped), jnp.where(xh == 0, o_swapped, o_part)]
    )
    output_matrix = lax.all_gather(after(o_both, own_matrix), ("y", "z"), axis=0, tiled=True)
    other_matrix = lax.all_gather(after(qkv_other, output_matrix), ("y", "z"), axis=0, tiled=True)
    out_grad_t = out_grad.T
    out_grad_full = gathered_pieces(after(out_grad_t, partial_sum), xl, c)

    (attended,) = attention_call(
        forward_kernel, first_key, [q_turned], window, [jax.ShapeDtypeStruct((q_width, count), BF)]
    )

    low_out_part = dot_f32(output_down, attended, 0, 0).astype(BF)
    out_rows = output_matrix.reshape(2, 2 * share, q_width)
    up_rows = output_up.T.reshape(2, 2 * share, rank)
    sums, low_total = [], None

    def number(a, b):
        return (a * 2 + b).astype(jnp.int32).reshape(1)

    for j in range(2):
        part = dot_f32(out_rows[j], attended, 1, 0) + ADAPTER_SCALE * dot_f32(
            up_rows[j], low_out_part, 1, 0
        )
        part = part.reshape(2, share, count)
        keep = lax.dynamic_index_in_dim(part, c, 0, False)
        give = lax.dynamic_index_in_dim(part, 1 - c, 0, False)
        if j == 0:
            keep = jnp.concatenate([keep, low_out_part.astype(F32)])
            give = jnp.concatenate([give, low_out_part.astype(F32)])
        chip = (keep + swap(give.astype(BF), "c").astype(F32)).astype(BF)
        total = (chip.astype(F32) + swap(chip, "xl").astype(F32)).astype(BF)
        if j == 0:
            low_total = total[share:]
            total = total[:share]
        far = swap(total, "c")
        sums.append(jnp.stack([jnp.where(c == 0, total, far), jnp.where(c == 0, far, total)]))
    out_total = jnp.stack(sums).astype(F32)
    output_lowrank = low_total.T
    gain_full = post_gain.reshape(2, 2, share, 1)
    weighted_out = out_grad_full.astype(F32) * gain_full
    out_scale = lax.rsqrt(jnp.sum(out_total * out_total, axis=(0, 1, 2)) / D + EPSILON)
    out_inner = jnp.sum(weighted_out * out_total, axis=(0, 1, 2)) / D
    grad_full = (out_scale * weighted_out - out_scale**3 * out_total * out_inner).astype(BF)
    output_gradient = grad_full.reshape(D, count)
    out_mine = lax.dynamic_slice_in_dim(out_total.reshape(D, count), column_start, share, 0)
    post_mine = lax.dynamic_slice_in_dim(post_gain, column_start, share, 0)[:, None]
    mixed = (tokens_t.astype(F32) + out_mine * out_scale * post_mine).astype(BF)

    output_mixture = dot_f32(output_gradient, output_up, 0, 1).astype(BF)
    grad_mine = lax.dynamic_slice_in_dim(output_gradient, column_start, share, 0)
    output_up_gradient = ADAPTER_SCALE * dot_f32(output_lowrank, grad_mine, 0, 1)
    output_down_gradient = ADAPTER_SCALE * dot_f32(output_mixture, attended, 0, 1)
    attended_gradient = (
        dot_f32(output_matrix, output_gradient, 0, 0)
        + ADAPTER_SCALE * dot_f32(output_down, output_mixture, 1, 1)
    ).astype(BF)
    query_grad, *window_grad = attention_call(
        backward_kernel,
        first_key,
        [q_turned, attended_gradient],
        window,
        [jax.ShapeDtypeStruct((q_width, count), F32)]
        + [jax.ShapeDtypeStruct((count, 2 * kv_width), BF)] * steps
        + [jax.ShapeDtypeStruct((count, 2 * kv_width), F32)],
    )
    across = jnp.concatenate([cosine, cosine], axis=1)
    along = jnp.concatenate([sine, -sine], axis=1)
    query_back, small_q = whole(
        query_back_kernel,
        [
            jax.ShapeDtypeStruct((count, q_width), BF),
            jax.ShapeDtypeStruct((rank + 8, count), F32),
        ],
        [query_grad, query_rows, across, along, query_gain[None], query_up],
    )
    arrived = [shifted(window_grad[steps - s], -s) for s in range(steps, 0, -1)]
    kv_back, small_kv = whole(
        key_value_back_kernel,
        [
            jax.ShapeDtypeStruct((count, 2 * kv_width), BF),
            jax.ShapeDtypeStruct((2 * rank + 8, count), F32),
        ],
        [window_grad[steps], *arrived, kv_total, across, along, key_gain[None], kv_up],
    )
    smalls = lax.all_gather(jnp.concatenate([small_q, small_kv]), TP)

    in_gain_mine = lax.dynamic_slice_in_dim(in_gain, column_start, share, 0)[:, None]
    tokens_wide = tokens_t.astype(F32)
    normed_mine = (tokens_wide * row_scale * in_gain_mine).astype(BF)
    devices = lax.axis_size(CTX)
    each = 6 * rank // devices
    parts, mixes, inner = whole(
        adapter_kernel,
        [
            jax.ShapeDtypeStruct((devices, each, share), F32),
            jax.ShapeDtypeStruct((3 * rank, count), BF),
            jax.ShapeDtypeStruct((8, count), F32),
        ],
        [
            smalls,
            normed_mine,
            output_up_gradient,
            ADAPTER_SCALE * dot_f32(query_lowrank, query_back, 0, 0),
            output_down_gradient,
            low.T,
            kv_back,
        ],
        [pltpu.VMEM((6 * rank, share), F32)],
    )
    in_inner = inner[0] / (row_scale * D)
    sums_arrived = lax.all_to_all(parts, CTX, 0, 0, tiled=True)

    back = after(jnp.concatenate([query_back, kv_back], axis=1), parts)

    def into(a, b, dtype):
        return into_piece(own_matrix, other_matrix, back, number(a, b), 2 * rows, dtype)

    give_far = into(1 - xl, 1 - c, BF)
    give_near = into(xl, 1 - c, BF)
    keep_far = into(1 - xl, c, F32)
    keep_near = into(xl, c, F32)
    to_chip = (keep_far + swap(give_far, "c").astype(F32)).astype(BF)
    far_into = swap(to_chip, "xl")
    into_mine = keep_near + swap(give_near, "c").astype(F32) + far_into.astype(F32)
    halves = into_mine.reshape(2, nz, rows, count)
    first = jnp.where(xh == 0, halves[0], halves[1])
    last = jnp.where(xh == 0, halves[1], halves[0])
    into_mine = jnp.stack([first, last], axis=1).reshape(share, count)

    downs_mine = lax.dynamic_slice_in_dim(downs, column_start, share, 0)
    normalized_gradient = into_mine + ADAPTER_SCALE * dot_f32(downs_mine, mixes, 1, 0)
    weighted_in = normalized_gradient * in_gain_mine
    tokens_grad = (
        out_grad_t.astype(F32)
        + row_scale * weighted_in
        - row_scale**3 * tokens_wide * in_inner
    )
    in_projection = (float(D) ** 0.5 * row_scale * in_inner)[:, None]
    chunk = jnp.sum(sums_arrived, axis=0)
    spread = jnp.broadcast_to(chunk[None], (devices, *chunk.shape))
    summed = lax.all_to_all(spread, CTX, 0, 0, tiled=True).reshape(-1, share)
    cut = 4 * rank
    wide_sums = lax.all_gather(summed[:cut].astype(BF), TP)
    wide_sums = jnp.moveaxis(wide_sums, 0, 1).reshape(cut, D).astype(F32)
    narrow = summed[cut : 5 * rank]
    kv_end = q_width + 2 * kv_width
    kv_up_gradient = narrow[:, q_width:kv_end].reshape(rank, kv_heads_here, 2, HEAD_SIZE)
    kv_up_gradient = kv_up_gradient.transpose(2, 0, 1, 3).reshape(2, rank, kv_width)
    output_down_gradient = jnp.concatenate(
        [narrow[:, kv_end : kv_end + q_width // 2], summed[5 * rank :, : q_width // 2]], axis=1
    ).T
    return (
        mixed.T,
        tokens_grad.T,
        wide_sums[:rank].T,
        narrow[:, :q_width],
        jnp.stack([wide_sums[rank : 2 * rank].T, wide_sums[2 * rank : 3 * rank].T]),
        kv_up_gradient,
        output_down_gradient,
        wide_sums[3 * rank :],
        in_projection,
    )


def solution(mesh):
    torus = Mesh(mesh.devices.reshape(4, 4, 2, 2, 2), (*CTX, *TP))

    return jax.shard_map(
        on_device,
        mesh=torus,
        in_specs=(
            P(CTX, TP),
            P(CTX, TP),
            P(),
            P(),
            P(),
            P(),
            P(CTX, TP),
            P(CTX, TP),
            P(None, TP),
            P(None, CTX, TP),
            P(None, CTX, TP),
            P(None, None, TP),
            P(CTX, TP),
            P(CTX, TP),
            P(None, TP),
            P(),
            P(None, TP),
            P(),
            P(None, None, TP),
            P(TP, None),
            P(),
        ),
        out_specs=(
            P(CTX, TP),
            P(CTX, TP),
            P(),
            P(None, TP),
            P(),
            P(None, None, TP),
            P(TP, None),
            P(),
            P(CTX, None),
        ),
        check_vma=False,
    )
```
